128 devices in a mesh: neg: 16 (over x, y), qry: 8 (over z, core).
Axes of the slice: x: 4, y: 4, z: 4, core: 2. Of those that a mesh axis runs over, the one named last changes fastest.
Arguments:
- items_table: bfloat16 [131072, 512], P('neg'), may hold values from -6 to 6
- fetch_rows: int32 [2048, 640], P(('neg', 'qry')), may hold values from 0 to 8191, as said below
- neighbour_slots: int32 [65536, 40], P(('neg', 'qry')), may hold values from 0 to 10239, as said below
- neighbour_count: int32 [65536], P(('neg', 'qry')), may hold values from 20 to 40
- self_slot: int32 [65536], P(('neg', 'qry')), may hold values from 0 to 10239
- negative_count: int32 [65536], P('neg'), may hold values from 1 to 999
- message_weight: bfloat16 [512, 512], replicated, may hold values from -0.25 to 0.25
- message_bias: float32 [512], replicated, may hold values from -3 to 3
- self_weight: bfloat16 [512, 512], replicated, may hold values from -0.25 to 0.25
- neighbour_weight: bfloat16 [512, 512], replicated, may hold values from -0.25 to 0.25
- output_bias: float32 [512], replicated, may hold values from -3 to 3
- queries: bfloat16 [8192, 512], P('qry'), may hold values from -8 to 8
Outputs:
- negative_embed: bfloat16 [65536, 512], P(('neg', 'qry'))
- query_lse: float32 [8192], P('qry')
The draws below stay inside these ranges and needn't reach their ends.
Inputs may be any that keep to these rules, and one draw needn't show every extreme that they name: Within one row of fetch_rows (one device's list for one partition) no item appears twice. `neighbour_slots`: every one of a device's 16 * 640 fetched rows is named by at least one live neighbour of that device's negatives.
All inputs are finite; a program needn't handle non-finite values.
Results may differ from the reference program's by a relative error of at most 0.0055.
Values may be sent and summed in bfloat16 or wider, within the bound.
A program may use at most 128 MiB of HBM per device.

```python
import math
import jax
import jax.numpy as jnp
from jax import lax

D = 512
K = 40
ITEM_DEV = 8192
NEG_DEV = 512
CAP = 640
NEG = 65536
QRY = 8192
ITEMS = 131072
N_NEG = 16
N_QRY = 8


def draw_queries(key, part):
    values = jnp.clip(jax.random.normal(key, (QRY, D), jnp.float32), -5.5, 5.5)
    return values.astype(jnp.bfloat16)


def draw_fetch_rows(key, part):
    row_keys = jax.random.split(jax.random.fold_in(key, 7), N_NEG * N_QRY * N_NEG)

    def one_row(row_key):
        return jax.random.permutation(row_key, ITEM_DEV)[:CAP].astype(jnp.int32)
    return jax.vmap(one_row)(row_keys).astype(jnp.int32)


def neighbour_draw(key):
    count_key = jax.random.fold_in(key, 11)
    counts = jax.random.randint(count_key, (NEG,), K // 2, K + 1, dtype=jnp.int32)
    slot_total = N_NEG * CAP
    device_keys = jax.random.split(jax.random.fold_in(key, 13), N_NEG * N_QRY)
    count_blocks = counts.reshape(N_NEG * N_QRY, NEG_DEV)

    def one_device(device_key, count_block):
        order_key = jax.random.fold_in(device_key, 1)
        filler_key = jax.random.fold_in(device_key, 2)
        live_mask = jnp.arange(K, dtype=jnp.int32)[None, :] < count_block[:, None]
        priority = jax.random.randint(order_key, (NEG_DEV * K,), 0, 1 << 20, dtype=jnp.int32)
        priority = priority + jnp.where(live_mask.reshape(-1), 0, 1 << 21).astype(jnp.int32)
        order = jnp.argsort(priority, stable=True).astype(jnp.int32)
        ranked = jnp.argsort(order, stable=True).astype(jnp.int32)
        filler = jax.random.randint(filler_key, (NEG_DEV * K,), 0, slot_total, dtype=jnp.int32)
        slots = jnp.where(ranked < slot_total, ranked, filler)
        return slots.reshape(NEG_DEV, K).astype(jnp.int32)
    slots = jax.vmap(one_device)(device_keys, count_blocks).reshape(NEG, K)
    return (counts, slots)


def draw_neighbour_count(key, part):
    return neighbour_draw(key)[0].astype(jnp.int32)


def draw_neighbour_slots(key, part):
    return neighbour_draw(key)[1].astype(jnp.int32)


def place_ends(drawn, stream_key, smallest, largest):
    longest = drawn.shape.index(max(drawn.shape))
    spots = []
    for shift in (0, 1):
        where = [jax.random.randint(jax.random.fold_in(stream_key, axis), (), 0, length) for axis, length in enumerate(drawn.shape)]
        where[longest] = (where[longest] + shift) % drawn.shape[longest]
        spots.append(tuple(where))
    return drawn.at[spots[0]].set(smallest).at[spots[1]].set(largest)


def shard_levels(own_key, shape, cuts, least, high):
    factor_of = 1.0
    for dim, parts in cuts:
        draws = jax.random.uniform(jax.random.fold_in(jax.random.fold_in(own_key, 6), dim), (parts,), jnp.float32, least / len(cuts), high / len(cuts))
        factor_of = factor_of * jnp.repeat(jnp.exp(draws), shape[dim] // parts).reshape((-1,) + (1,) * (len(shape) - 1 - dim))
    return factor_of


def gaussian(key, shape, deviation, limit, pieces=(), kind=jnp.bfloat16):
    factor_of = shard_levels(key, shape, pieces, -0.22, 0.18) if pieces else 1.0
    values = jax.random.normal(key, shape, jnp.float32) * deviation * factor_of
    return jnp.minimum(jnp.maximum(values, -limit), limit).astype(kind)


def setup_inputs(seed: int = 0) -> dict:
    seeds = jax.random.split(jax.random.key(seed), 13)
    items_table = gaussian(seeds[0], (ITEMS, D), 1.0, 6.0, ((0, 16),))
    fetch_rows = draw_fetch_rows(jax.random.fold_in(seeds[12], 71), 0)
    neighbour_slots = draw_neighbour_slots(jax.random.fold_in(seeds[12], 71), 0)
    neighbour_count = draw_neighbour_count(jax.random.fold_in(seeds[12], 71), 0)
    self_slot = place_ends(jax.random.randint(seeds[4], (NEG,), 0, N_NEG * CAP), jax.random.fold_in(seeds[4], 1), 0, (N_NEG * CAP) - 1).astype(jnp.int32)
    negative_count = place_ends(jax.random.randint(seeds[5], (NEG,), 1, 1000), jax.random.fold_in(seeds[5], 1), 1, 999).astype(jnp.int32)
    message_weight = gaussian(seeds[6], (D, D), D ** -0.5, 0.25)
    message_bias = gaussian(seeds[7], (D,), 0.5, 3.0, (), jnp.float32)
    self_weight = gaussian(seeds[8], (D, D), D ** -0.5, 0.25)
    neighbour_weight = gaussian(seeds[9], (D, D), D ** -0.5, 0.25)
    output_bias = gaussian(seeds[10], (D,), 0.5, 3.0, (), jnp.float32)
    queries = draw_queries(jax.random.fold_in(seeds[12], 71), 0)
    return {"items_table": items_table, "fetch_rows": fetch_rows, "neighbour_slots": neighbour_slots, "neighbour_count": neighbour_count, "self_slot": self_slot, "negative_count": negative_count, "message_weight": message_weight, "message_bias": message_bias, "self_weight": self_weight, "neighbour_weight": neighbour_weight, "output_bias": output_bias, "queries": queries}


def embed_device(items_table, fetch_block, slot_block, count_block, self_block, message_weight, message_bias, self_weight, neighbour_weight, output_bias):
    owners = jnp.arange(N_NEG, dtype=jnp.int32)[:, None] * ITEM_DEV
    global_rows = (fetch_block.astype(jnp.int32) + owners).reshape(-1)
    fetched = items_table[global_rows]
    message = jax.nn.relu(jnp.dot(fetched, message_weight, preferred_element_type=jnp.float32) + message_bias).astype(jnp.bfloat16)
    gathered = message[slot_block].astype(jnp.float32)
    live_mask = jnp.arange(K, dtype=jnp.int32)[None, :] < count_block[:, None]
    summed = lax.optimization_barrier(jnp.sum(jnp.where(live_mask[:, :, None], gathered, jnp.float32(0.0)), axis=1))
    neighbour_mean = (summed / count_block.astype(jnp.float32)[:, None]).astype(jnp.bfloat16)
    self_rows = fetched[self_block]
    hidden = jnp.dot(self_rows, self_weight, preferred_element_type=jnp.float32)
    hidden = hidden + jnp.dot(neighbour_mean, neighbour_weight, preferred_element_type=jnp.float32) + output_bias
    hidden = jax.nn.relu(hidden)
    scale_inv = lax.rsqrt(lax.optimization_barrier(jnp.mean(hidden * hidden, axis=-1, keepdims=True)) + 0.25)
    return (hidden * scale_inv).astype(jnp.bfloat16)

def reference(items_table, fetch_rows, neighbour_slots, neighbour_count, self_slot, negative_count, message_weight, message_bias, self_weight, neighbour_weight, output_bias, queries):
    devices_all = N_NEG * N_QRY
    fetch_all = fetch_rows.reshape(devices_all, N_NEG, -1)
    slots_all = neighbour_slots.reshape(devices_all, -1, K)
    counts_all = neighbour_count.reshape(devices_all, -1)
    selves_all = self_slot.reshape(devices_all, -1)

    def one_device(inputs):
        return embed_device(items_table, inputs[0], inputs[1], inputs[2], inputs[3], message_weight, message_bias, self_weight, neighbour_weight, output_bias)
    embedded = lax.map(one_device, (fetch_all, slots_all, counts_all, selves_all))
    negative_embed = embedded.reshape(-1, D)
    log_count = jnp.log(negative_count.astype(jnp.float32))
    query_blocks = queries.reshape(N_QRY, -1, D)

    def one_block(query_block):
        scores = 0.25 * jnp.dot(query_block, negative_embed.T, preferred_element_type=jnp.float32) - log_count[None, :]
        peak = lax.optimization_barrier(jnp.max(scores, axis=1))
        totals = lax.optimization_barrier(jnp.sum(jnp.exp(scores - peak[:, None]), axis=1))
        return peak + jnp.log(totals) - math.log(NEG)
    query_lse = lax.map(one_block, query_blocks).reshape(-1)
    return (negative_embed, query_lse)
```

```python
import functools
import math

import jax
import jax.numpy as jnp
from jax import lax
from jax.experimental import pallas as pl
from jax.experimental.pallas import tpu as pltpu
from jax.sharding import PartitionSpec as P


LANES = 128
ROWS = 128
DEAD = 32767
SIDE = 4
NT = (((1,), (1,)), ((), ()))
MESH = pl.DeviceIdType.MESH
ORDER = (
    (2, 2), (2, 1), (2, 3), (1, 2), (3, 2), (2, 0), (0, 2), (1, 1),
    (1, 3), (3, 1), (3, 3), (1, 0), (3, 0), (0, 1), (0, 3), (0, 0),
)


def sort_pairs(count):
    full = 1
    while full < count:
        full *= 2
    pairs = []
    p = 1
    while p < full:
        k = p
        while k >= 1:
            for j in range(k % p, full - k, 2 * k):
                for i in range(min(k, full - j - k)):
                    if (i + j) // (2 * p) == (i + j + k) // (2 * p):
                        if i + j + k < count:
                            pairs.append((i + j, i + j + k))
            k //= 2
        p *= 2
    return pairs


def place():
    neg, qry = lax.axis_index("neg"), lax.axis_index("qry")
    return neg // SIDE, neg % SIDE, qry // 2, qry % 2


def device(x, y, z, core):
    wrap = lambda v: lax.rem(v + 2 * SIDE, SIDE)
    return (wrap(x) * SIDE + wrap(y), wrap(z) * 2 + core)


def remote(src, dst, send, recv, target):
    return pltpu.make_async_remote_copy(
        src_ref=src, dst_ref=dst, send_sem=send, recv_sem=recv,
        device_id=target, device_id_type=MESH,
    )


def greet(peers):
    barrier = pltpu.get_barrier_semaphore()
    for peer in peers:
        pl.semaphore_signal(barrier, inc=1, device_id=peer, device_id_type=MESH)
    pl.semaphore_wait(barrier, len(peers))


def exchange_kernel(lists_ref, fetch_ref, all_lists, all_fetch, sends, recvs):
    x, y, z, core = place()
    others = ORDER[:-1]
    greet([device(x - dx, y - dy, z, core) for dx, dy in others])
    copies = []
    for j, (dx, dy) in enumerate(others):
        target = device(x - dx, y - dy, z, core)
        copies.append(
            remote(fetch_ref.at[target[0]], all_fetch.at[j], sends.at[0, j], recvs.at[0, j], target)
        )
        copies.append(remote(lists_ref, all_lists.at[j], sends.at[1, j], recvs.at[1, j], target))
    for copy in copies:
        copy.start()
    last = len(others)
    all_fetch[last] = fetch_ref[x * SIDE + y]
    all_lists[last] = lists_ref[...]
    for copy in copies:
        copy.wait()


def exchange_lists(lists, fetch):
    peers = fetch.shape[0]
    vmem = pl.BlockSpec(memory_space=pltpu.VMEM)
    return pl.pallas_call(
        exchange_kernel,
        out_shape=(
            jax.ShapeDtypeStruct((peers,) + lists.shape, lists.dtype),
            jax.ShapeDtypeStruct(fetch.shape, fetch.dtype),
        ),
        in_specs=[vmem, vmem],
        out_specs=(vmem, vmem),
        scratch_shapes=[
            pltpu.SemaphoreType.DMA((2, peers - 1)),
            pltpu.SemaphoreType.DMA((2, peers - 1)),
        ],
        compiler_params=pltpu.CompilerParams(collective_id=0, has_side_effects=True),
    )(lists, fetch)


def count_kernel(
    neighbours, cap, base_ref, index_ref, lists_ref, table_ref,
    counts_ref, inverse_ref, own_ref, rows_ref,
    order_ref, times_ref, mine_ref, live_ref, self_ref, wide_ref, picked_ref,
):
    j = pl.program_id(0)
    rows, width = table_ref.shape
    pieces = width // LANES

    @pl.when(j == 0)
    def _():
        @pl.loop(0, rows // ROWS)
        def _(t):
            span = pl.ds(pl.multiple_of(t * ROWS, ROWS), ROWS)
            for c in range(pieces):
                wide_ref[pl.ds(t * ROWS * pieces + c, ROWS, stride=pieces), :] = table_ref[
                    span, c * LANES : (c + 1) * LANES
                ].astype(jnp.float32)

    groups = counts_ref.shape[2] // LANES
    half = neighbours // 2
    packed = 16
    tall = 8
    batch = tall // groups
    big = jnp.int32(DEAD)

    @pl.when(lax.rem(j, batch) == 0)
    def _():
        base = base_ref[0]
        live = jnp.zeros((tall, LANES), jnp.int32)
        mine = jnp.zeros((tall, LANES), jnp.int32)

        def rows_of(k):
            return jnp.concatenate(
                [lists_ref[j + i, k * groups : (k + 1) * groups, :] for i in range(batch)]
            )

        words = [rows_of(k) for k in range(half)]
        places = []
        for k in range(neighbours):
            slot = words[k] & DEAD if k < half else words[k - half] >> 16
            local = slot - base
            inside = (local >= 0) & (local < cap)
            live = live + jnp.where(slot < DEAD, 1, 0)
            mine = mine + jnp.where(inside, 1, 0)
            places.append(jnp.where(inside, local, big).astype(jnp.float32))
        for a, b in sort_pairs(neighbours):
            low, high = jnp.minimum(places[a], places[b]), jnp.maximum(places[a], places[b])
            places[a], places[b] = low, high
        rows = pl.ds(pl.multiple_of(j * groups, tall), tall)
        run = jnp.ones((tall, LANES), jnp.float32)
        for k in range(neighbours):
            if k:
                run = jnp.where(places[k] == places[k - 1], run + 1.0, 1.0)
            order_ref[k, rows, :] = places[k].astype(jnp.int32)
            times_ref[k, rows, :] = run
        mine_ref[rows, :] = mine
        live_ref[rows, :] = 1.0 / live.astype(jnp.float32)
        own = rows_of(half) - base
        self_ref[rows, :] = jnp.where((own >= 0) & (own < cap), own, big)

    chunk = 320 if cap % 320 == 0 else ROWS
    tiles = chunk // packed
    unroll = 2
    iota = lax.broadcasted_iota(jnp.int32, (packed, LANES), 0)
    for g in range(groups):
        lanes = pl.ds(g * LANES, LANES)
        row = pl.ds(j * groups + g, 1)
        inverse_ref[0, :, lanes] = live_ref[row, :]
        own_ref[0, :, lanes] = self_ref[row, :]
        steps = (jnp.max(mine_ref[row, :]) + unroll - 1) // unroll

        @pl.loop(0, cap // chunk)
        def _(c):
            first = c * chunk
            here = [(iota + (first + packed * i)).astype(jnp.int16) for i in range(tiles)]

            def step(i, totals):
                for u in range(unroll):
                    k = unroll * i + u
                    tile = (packed, LANES)
                    slot = jnp.broadcast_to(order_ref[k, row, :], tile).astype(jnp.int16)
                    times = jnp.broadcast_to(times_ref[k, row, :], tile).astype(jnp.bfloat16)
                    totals = tuple(
                        jnp.where(here[t] == slot, times, totals[t]) for t in range(tiles)
                    )
                return totals

            zero = jnp.zeros((packed, LANES), jnp.bfloat16)
            totals = lax.fori_loop(0, steps, step, (zero,) * tiles)
            for t in range(tiles):
                span = pl.ds(pl.multiple_of(first + packed * t, packed), packed)
                counts_ref[0, span, lanes] = totals[t]

    burst = 32

    @pl.loop(0, cap // burst)
    def _(i):
        first = j * cap + i * burst
        start = pl.multiple_of(i * (burst * pieces), burst * pieces)
        places = [pl.multiple_of(index_ref[first + u], pieces) for u in range(burst)]
        for u in range(burst):
            picked_ref[pl.ds(start + u * pieces, pieces), :] = wide_ref[pl.ds(places[u], pieces), :]

    @pl.loop(0, cap // ROWS)
    def _(t):
        span = pl.ds(pl.multiple_of(t * ROWS, ROWS), ROWS)
        for c in range(pieces):
            rows_ref[0, span, c * LANES : (c + 1) * LANES] = picked_ref[
                pl.ds(t * ROWS * pieces + c, ROWS, stride=pieces), :
            ].astype(jnp.bfloat16)


def pick_and_count(base, index, lists, table, neighbours, cap):
    peers = lists.shape[0]
    groups = lists.shape[1] // (neighbours // 2 + 1)
    negatives = groups * LANES
    rows = peers * groups
    width = table.shape[1]
    pieces = width // LANES
    return pl.pallas_call(
        functools.partial(count_kernel, neighbours, cap),
        grid=(peers,),
        out_shape=(
            jax.ShapeDtypeStruct((peers, cap, negatives), jnp.bfloat16),
            jax.ShapeDtypeStruct((peers, 1, negatives), jnp.float32),
            jax.ShapeDtypeStruct((peers, 1, negatives), jnp.int32),
            jax.ShapeDtypeStruct((peers, cap, width), jnp.bfloat16),
        ),
        in_specs=[
            pl.BlockSpec(memory_space=pltpu.SMEM),
            pl.BlockSpec(memory_space=pltpu.SMEM),
            pl.BlockSpec(memory_space=pltpu.VMEM),
            pl.BlockSpec(memory_space=pltpu.VMEM),
        ],
        out_specs=(
            pl.BlockSpec((1, cap, negatives), lambda j: (j, 0, 0)),
            pl.BlockSpec((1, 1, negatives), lambda j: (j, 0, 0)),
            pl.BlockSpec((1, 1, negatives), lambda j: (j, 0, 0)),
            pl.BlockSpec((1, cap, width), lambda j: (j, 0, 0)),
        ),
        scratch_shapes=[
            pltpu.VMEM((neighbours, rows, LANES), jnp.int32),
            pltpu.VMEM((neighbours, rows, LANES), jnp.float32),
            pltpu.VMEM((rows, LANES), jnp.int32),
            pltpu.VMEM((rows, LANES), jnp.float32),
            pltpu.VMEM((rows, LANES), jnp.int32),
            pltpu.VMEM((table.shape[0] * pieces, LANES), jnp.float32),
            pltpu.VMEM((cap * pieces, LANES), jnp.float32),
        ],
        compiler_params=pltpu.CompilerParams(vmem_limit_bytes=48 << 20),
    )(base, index * pieces, lists, table)


def reduce_kernel(
    rows_ref, counts_ref, inverse_ref, own_ref, wm_ref, mb_ref, ws_ref, wn_ref,
    queries_ref, hidden_ref, around_ref,
    hot_ref, turned_ref, wnt_ref, total_ref, part_ref,
    relay1, full1, relay2, full2, mid_ref,
    s_relay1, r_relay1, s_full1, r_full1, s_relay2, r_relay2, s_full2, r_full2, s_query, r_query,
):
    step = pl.program_id(0)
    x, y, z, core = place()
    _, cap, width = rows_ref.shape
    negatives = counts_ref.shape[2]
    groups = negatives // LANES
    half, quarter = width // 2, width // 4
    packed = 16

    def neighbour(axis, sign):
        if axis == 0:
            return device(x + sign, y, z, core)
        return device(x, y + sign, z, core)

    up, down, sibling = device(x, y, z + 1, core), device(x, y, z - 1, core), device(x, y, z, 1 - core)
    upper = pl.ds(0, queries_ref.shape[0] // 2)
    lower = pl.ds(queries_ref.shape[0] // 2, queries_ref.shape[0] // 2)

    def query_copy(which):
        sem = (s_query.at[which], r_query.at[which])
        if which == 0:
            return remote(queries_ref, around_ref.at[6], *sem, up)
        if which == 1:
            return remote(queries_ref, around_ref.at[2], *sem, down)
        if which == 2:
            return remote(queries_ref, around_ref.at[1], *sem, sibling)
        if which == 3:
            return remote(around_ref.at[6, upper], around_ref.at[4, upper], *sem, up)
        if which == 4:
            return remote(around_ref.at[2, lower], around_ref.at[4, lower], *sem, down)
        slot = {5: 6, 6: 2, 7: 4}[which]
        return remote(around_ref.at[slot], around_ref.at[slot + 1], *sem, sibling)

    @pl.when(step == 0)
    def _():
        greet(
            [neighbour(0, 1), neighbour(0, -1), neighbour(1, 1), neighbour(1, -1), up, down, sibling]
        )
        for which in range(3):
            query_copy(which).start()
        turned_ref[:width, :] = wm_ref[...].T
        turned_ref[width:, :] = ws_ref[...].T
        wnt_ref[...] = wn_ref[...].T

    @pl.when(step == 7)
    def _():
        for which in (0, 1):
            query_copy(which).wait_recv()
        for which in (3, 4, 5, 6):
            query_copy(which).start()

    @pl.when(step == 12)
    def _():
        for which in (3, 4):
            query_copy(which).wait_recv()
        query_copy(7).start()

    iota = lax.broadcasted_iota(jnp.int32, (packed, LANES), 0)
    zero = jnp.zeros((packed, LANES), jnp.bfloat16)
    one = jnp.ones((packed, LANES), jnp.bfloat16)
    for g in range(groups):
        lanes = pl.ds(g * LANES, LANES)
        own = jnp.broadcast_to(own_ref[0, :, lanes], (packed, LANES))

        @pl.loop(0, cap // ROWS)
        def _(t):
            for i in range(ROWS // packed):
                first = t * ROWS + i * packed
                span = pl.ds(pl.multiple_of(first, packed), packed)
                same = (iota + first).astype(jnp.int16) == own.astype(jnp.int16)
                hot_ref[span, lanes] = jnp.where(same, one, zero)

    both = lax.dot_general(turned_ref[...], rows_ref[0], NT, preferred_element_type=jnp.float32)
    message = jax.nn.relu(both[:width] + mb_ref[...]).astype(jnp.bfloat16)
    own_part = both[width:].astype(jnp.bfloat16)
    summed = jnp.dot(message, counts_ref[0], preferred_element_type=jnp.float32)
    mid_ref[...] = (summed * inverse_ref[0]).astype(jnp.bfloat16)
    total_ref[...] = jnp.dot(
        own_part, hot_ref[...], preferred_element_type=jnp.float32
    ) + jnp.dot(wnt_ref[...], mid_ref[...], preferred_element_type=jnp.float32)

    block = 32

    def combine(first, count, sources):
        @pl.loop(0, count // block)
        def _(i):
            span = pl.ds(pl.multiple_of(first + i * block, block), block)
            value = total_ref[span, :]
            for source, begin in sources:
                value = value + source[
                    pl.ds(pl.multiple_of(begin + i * block, block), block), :
                ].astype(jnp.float32)
            total_ref[span, :] = value

    def pack(j, first):
        @pl.loop(0, half // block)
        def _(i):
            span = pl.ds(pl.multiple_of(first + i * block, block), block)
            part_ref[j, span, :] = total_ref[span, :].astype(jnp.bfloat16)

    def relay_copy(j, first, axis, side, relay, send, recv, at):
        return remote(
            part_ref.at[j, pl.ds(first + side * quarter, quarter)],
            relay.at[(*at, side)], send.at[(*at, side)], recv.at[(*at, side)],
            neighbour(axis, 1 - 2 * side),
        )

    def full_copy(j, first, axis, side, full, send, recv, at):
        return remote(
            part_ref.at[j, pl.ds(first, half)],
            full.at[(*at, side)], send.at[(*at, side)], recv.at[(*at, side)],
            neighbour(axis, 1 - 2 * side),
        )

    def ring(j, first, axis, offset, bufs, at):
        relay, full, s_relay, r_relay, s_full, r_full = bufs
        if offset == 2:
            pack(j, first)
            for side in (0, 1):
                relay_copy(j, first, axis, side, relay, s_relay, r_relay, at).start()
        elif offset in (1, 3):
            side = 0 if offset == 1 else 1
            relay_copy(j, first, axis, side, relay, s_relay, r_relay, at).wait_recv()
            combine(first + side * quarter, quarter, [(relay.at[(*at, side)], 0)])
            pack(j, first)
            full_copy(j, first, axis, side, full, s_full, r_full, at).start()
        else:
            for side in (0, 1):
                full_copy(j, first, axis, side, full, s_full, r_full, at).wait_recv()
            combine(first, half, [(full.at[(*at, side)], 0) for side in (0, 1)])

    stage1 = (relay1, full1, s_relay1, r_relay1, s_full1, r_full1)
    stage2 = (relay2, full2, s_relay2, r_relay2, s_full2, r_full2)
    for j, offsets in enumerate(ORDER):

        @pl.when(step == j)
        def _(j=j, offsets=offsets):
            for h in (0, 1):
                first = h * half
                near, far = offsets[h], offsets[1 - h]
                ring(j, first, h, near, stage1, (h, far))
                if near == 0:
                    ring(j, first, 1 - h, far, stage2, (h,))

    @pl.when(step == len(ORDER) - 1)
    def _():
        hidden_ref[...] = total_ref[...]
        for j, offsets in enumerate(ORDER):
            for h in (0, 1):
                first = h * half
                near, far = offsets[h], offsets[1 - h]
                stages = [(near, h, stage1, (h, far))]
                if near == 0:
                    stages.append((far, 1 - h, stage2, (h,)))
                for offset, axis, bufs, at in stages:
                    relay, full, s_relay, r_relay, s_full, r_full = bufs
                    if offset == 2:
                        for side in (0, 1):
                            relay_copy(j, first, axis, side, relay, s_relay, r_relay, at).wait_send()
                    elif offset in (1, 3):
                        side = 0 if offset == 1 else 1
                        full_copy(j, first, axis, side, full, s_full, r_full, at).wait_send()
        for which in (2, 5, 6, 7):
            query_copy(which).wait_recv()
        for which in range(8):
            query_copy(which).wait_send()


def reduce_parts(picked, counts, inverse, own, wm, mb, ws, wn, queries):
    peers, cap, negatives = counts.shape
    width = picked.shape[2]
    half, quarter = width // 2, width // 4
    vmem = pl.BlockSpec(memory_space=pltpu.VMEM)
    hbm = pl.BlockSpec(memory_space=pl.ANY)
    dma = pltpu.SemaphoreType.DMA
    bf16, f32 = jnp.bfloat16, jnp.float32
    return pl.pallas_call(
        reduce_kernel,
        grid=(peers,),
        out_shape=(
            jax.ShapeDtypeStruct((width, negatives), f32),
            jax.ShapeDtypeStruct((8,) + queries.shape, queries.dtype),
        ),
        in_specs=[
            pl.BlockSpec((1, cap, width), lambda j: (j, 0, 0)),
            pl.BlockSpec((1, cap, negatives), lambda j: (j, 0, 0)),
            pl.BlockSpec((1, 1, negatives), lambda j: (j, 0, 0)),
            pl.BlockSpec((1, 1, negatives), lambda j: (j, 0, 0)),
            vmem, vmem, vmem, vmem,
            hbm,
        ],
        out_specs=(vmem, hbm),
        scratch_shapes=[
            pltpu.VMEM((cap, negatives), bf16),
            pltpu.VMEM((2 * width, width), bf16),
            pltpu.VMEM((width, width), bf16),
            pltpu.VMEM((width, negatives), f32),
            pltpu.VMEM((peers, width, negatives), bf16),
            pltpu.VMEM((2, SIDE, 2, quarter, negatives), bf16),
            pltpu.VMEM((2, SIDE, 2, half, negatives), bf16),
            pltpu.VMEM((2, 2, quarter, negatives), bf16),
            pltpu.VMEM((2, 2, half, negatives), bf16),
            pltpu.VMEM((width, negatives), bf16),
            dma((2, SIDE, 2)), dma((2, SIDE, 2)), dma((2, SIDE, 2)), dma((2, SIDE, 2)),
            dma((2, 2)), dma((2, 2)), dma((2, 2)), dma((2, 2)),
            dma((8,)), dma((8,)),
        ],
        compiler_params=pltpu.CompilerParams(
            collective_id=1, has_side_effects=True, vmem_limit_bytes=62 << 20
        ),
    )(picked, counts, inverse, own, wm, mb, ws, wn, queries)


def score_kernel(
    total_negatives, hidden_ref, queries_ref, around_ref, bias_ref, count_ref,
    embed_ref, lse_ref,
    log_ref, block_ref, mine_ref, slots_ref, merged_ref, all_ref,
    s_load, s_send1, r_send1, s_send2, r_send2,
):
    x, y, z, core = place()
    others = ORDER[:-1]
    near = [(dz, c) for dz in range(SIDE) for c in (0, 1)][1:]
    greet(
        [device(x, y, z - dz, core if c == 0 else 1 - core) for dz, c in near]
        + [device(x - dx, y - dy, z, core) for dx, dy in others]
    )

    def load(slot):
        buffer = block_ref.at[slot % 2]
        return pltpu.make_async_copy(around_ref.at[slot], buffer, s_load.at[slot % 2])

    load(1).start()
    hidden = jax.nn.relu(hidden_ref[...] + bias_ref[...])
    scale = lax.rsqrt(jnp.mean(hidden * hidden, axis=0, keepdims=True) + 0.25)
    embed_ref[...] = (hidden * scale).T.astype(jnp.bfloat16)
    log_ref[...] = jnp.broadcast_to(jnp.log(count_ref[...].astype(jnp.float32)), log_ref.shape)
    tile = LANES

    def score(slot, ref):
        @pl.loop(0, queries_ref.shape[0] // tile)
        def _(t):
            span = pl.ds(pl.multiple_of(t * tile, tile), tile)
            scores = (
                0.25
                * lax.dot_general(
                    embed_ref[...], ref[span, :], NT, preferred_element_type=jnp.float32
                )
                - log_ref[...]
            )
            peak = jnp.max(scores, axis=0, keepdims=True)
            total = jnp.sum(jnp.exp(scores - peak), axis=0, keepdims=True)
            mine_ref[slot, :, span] = peak + jnp.log(total)

    def exchange1(slot):
        dz, c = slot // 2, slot % 2
        return remote(
            mine_ref.at[slot], slots_ref.at[slot], s_send1.at[slot], r_send1.at[slot],
            device(x, y, z + dz, core if c == 0 else 1 - core),
        )

    for slot in range(1, 8):
        if slot < 7:
            load(slot + 1).start()
        load(slot).wait()
        score(slot, block_ref.at[slot % 2])
        exchange1(slot).start()
    score(0, queries_ref)
    slots_ref[0] = mine_ref[0]
    for slot in range(1, 8):
        exchange1(slot).wait_recv()

    def merge(ref, count):
        values = [ref[i] for i in range(count)]
        top = functools.reduce(jnp.maximum, values)
        return top + jnp.log(sum(jnp.exp(v - top) for v in values))

    merged_ref[...] = merge(slots_ref, 8)

    def exchange2(j):
        dx, dy = others[j]
        return remote(
            merged_ref, all_ref.at[j], s_send2.at[j], r_send2.at[j], device(x - dx, y - dy, z, core)
        )

    for j in range(len(others)):
        exchange2(j).start()
    all_ref[len(others)] = merged_ref[...]
    for j in range(len(others)):
        exchange2(j).wait_recv()
    lse_ref[...] = merge(all_ref, len(others) + 1) - math.log(total_negatives)
    for slot in range(1, 8):
        exchange1(slot).wait_send()
    for j in range(len(others)):
        exchange2(j).wait_send()


def embed_and_score(hidden, queries, around, bias, count, total_negatives):
    width, negatives = hidden.shape
    rows = queries.shape[0]
    vmem = pl.BlockSpec(memory_space=pltpu.VMEM)
    dma = pltpu.SemaphoreType.DMA
    f32 = jnp.float32
    return pl.pallas_call(
        functools.partial(score_kernel, total_negatives),
        out_shape=(
            jax.ShapeDtypeStruct((negatives, width), jnp.bfloat16),
            jax.ShapeDtypeStruct((1, rows), f32),
        ),
        in_specs=[vmem, vmem, pl.BlockSpec(memory_space=pl.ANY), vmem, vmem],
        out_specs=(vmem, vmem),
        scratch_shapes=[
            pltpu.VMEM((negatives, LANES), f32),
            pltpu.VMEM((2, rows, width), jnp.bfloat16),
            pltpu.VMEM((8, 1, rows), f32),
            pltpu.VMEM((8, 1, rows), f32),
            pltpu.VMEM((1, rows), f32),
            pltpu.VMEM((16, 1, rows), f32),
            dma((2,)), dma((8,)), dma((8,)), dma((15,)), dma((15,)),
        ],
        compiler_params=pltpu.CompilerParams(collective_id=2, has_side_effects=True),
    )(hidden, queries, around, bias, count)


def per_device(
    items_table,
    fetch_rows,
    neighbour_slots,
    neighbour_count,
    self_slot,
    negative_count,
    message_weight,
    message_bias,
    self_weight,
    neighbour_weight,
    output_bias,
    queries,
):
    n_neg, n_qry = lax.axis_size("neg"), lax.axis_size("qry")
    own_neg, own_qry = lax.axis_index("neg"), lax.axis_index("qry")
    cap = fetch_rows.shape[1]
    negatives, neighbours = neighbour_slots.shape

    assert n_neg * cap < DEAD and neighbours % 4 == 0 and n_neg == SIDE * SIDE and n_qry == 8
    live = jnp.arange(neighbours, dtype=jnp.int32)[None, :] < neighbour_count[:, None]
    slots = jnp.where(live, neighbour_slots, DEAD).T
    half = neighbours // 2
    words = slots[:half] | (slots[half:] << 16)
    lists = jnp.concatenate([words.reshape(-1, LANES), self_slot.reshape(-1, LANES)])
    all_lists, all_fetch = exchange_lists(lists, fetch_rows.reshape(n_neg, cap // LANES, LANES))
    base = (own_neg * cap).astype(jnp.int32).reshape(1)
    counts, inverse, own, picked = pick_and_count(
        base, all_fetch.reshape(n_neg * cap), all_lists, items_table, neighbours, cap
    )
    hidden, around = reduce_parts(
        picked, counts, inverse, own,
        message_weight, message_bias[:, None], self_weight, neighbour_weight, queries,
    )
    count = lax.dynamic_slice_in_dim(negative_count, own_qry * negatives, negatives)
    negative_embed, query_lse = embed_and_score(
        hidden, queries, around, output_bias[:, None], count[:, None],
        negatives * n_neg * n_qry,
    )
    return (negative_embed, query_lse.reshape(-1))


def solution(mesh):
    in_specs = (
        P("neg", None),
        P(("neg", "qry"), None),
        P(("neg", "qry"), None),
        P(("neg", "qry")),
        P(("neg", "qry")),
        P("neg"),
        P(),
        P(),
        P(),
        P(),
        P(),
        P("qry", None),
    )
    out_specs = (P(("neg", "qry"), None), P("qry"))
    return jax.shard_map(
        per_device, mesh=mesh, in_specs=in_specs, out_specs=out_specs, check_vma=False
    )
```

```python
import functools
import math

import jax
import jax.numpy as jnp
from jax import lax
from jax.experimental import pallas as pl
from jax.experimental.pallas import tpu as pltpu
from jax.sharding import PartitionSpec as P


LANES = 128
ROWS = 128
DEAD = 32767
SIDE = 4
NT = (((1,), (1,)), ((), ()))
SURE = 10
LOG2E = math.log2(math.e)
MESH = pl.DeviceIdType.MESH
ORDER = (
    (2, 2), (2, 1), (2, 3), (1, 2), (3, 2), (2, 0), (0, 2), (1, 1),
    (1, 3), (3, 1), (3, 3), (1, 0), (3, 0), (0, 1), (0, 3), (0, 0),
)


def sort_pairs(count):
    full = 1
    while full < count:
        full *= 2
    pairs = []
    p = 1
    while p < full:
        k = p
        while k >= 1:
            for j in range(k % p, full - k, 2 * k):
                for i in range(min(k, full - j - k)):
                    if (i + j) // (2 * p) == (i + j + k) // (2 * p):
                        if i + j + k < count:
                            pairs.append((i + j, i + j + k))
            k //= 2
        p *= 2
    return pairs


def place():
    neg, qry = lax.axis_index("neg"), lax.axis_index("qry")
    return neg // SIDE, neg % SIDE, qry // 2, qry % 2


def device(x, y, z, core):
    wrap = lambda v: lax.rem(v + 2 * SIDE, SIDE)
    return (wrap(x) * SIDE + wrap(y), wrap(z) * 2 + core)


def remote(src, dst, send, recv, target):
    return pltpu.make_async_remote_copy(
        src_ref=src, dst_ref=dst, send_sem=send, recv_sem=recv,
        device_id=target, device_id_type=MESH,
    )


def greet(peers):
    barrier = pltpu.get_barrier_semaphore()
    for peer in peers:
        pl.semaphore_signal(barrier, inc=1, device_id=peer, device_id_type=MESH)
    pl.semaphore_wait(barrier, len(peers))


def exchange_kernel(lists_ref, fetch_ref, all_lists, all_fetch, sends, recvs):
    x, y, z, core = place()
    others = ORDER[:-1]
    greet([device(x - dx, y - dy, z, core) for dx, dy in others])
    copies = []
    for j, (dx, dy) in enumerate(others):
        target = device(x - dx, y - dy, z, core)
        copies.append(
            remote(fetch_ref.at[target[0]], all_fetch.at[j], sends.at[0, j], recvs.at[0, j], target)
        )
        copies.append(remote(lists_ref, all_lists.at[j], sends.at[1, j], recvs.at[1, j], target))
    for copy in copies:
        copy.start()
    last = len(others)
    all_fetch[last] = fetch_ref[x * SIDE + y]
    all_lists[last] = lists_ref[...]
    for copy in copies:
        copy.wait()


def exchange_lists(lists, fetch):
    peers = fetch.shape[0]
    vmem = pl.BlockSpec(memory_space=pltpu.VMEM)
    return pl.pallas_call(
        exchange_kernel,
        out_shape=(
            jax.ShapeDtypeStruct((peers,) + lists.shape, lists.dtype),
            jax.ShapeDtypeStruct(fetch.shape, fetch.dtype),
        ),
        in_specs=[vmem, vmem],
        out_specs=(vmem, vmem),
        scratch_shapes=[
            pltpu.SemaphoreType.DMA((2, peers - 1)),
            pltpu.SemaphoreType.DMA((2, peers - 1)),
        ],
        compiler_params=pltpu.CompilerParams(collective_id=0, has_side_effects=True),
    )(lists, fetch)


def count_kernel(
    neighbours, cap, base_ref, index_ref, lists_ref, table_ref,
    counts_ref, live_ref, own_ref, rows_ref,
    order_ref, times_ref, mine_ref, most_ref, alive_ref, self_ref, wide_ref, picked_ref,
):
    j = pl.program_id(0)
    rows, width = table_ref.shape
    pieces = width // LANES

    @pl.when(j == 0)
    def _():
        @pl.loop(0, rows // ROWS)
        def _(t):
            span = pl.ds(pl.multiple_of(t * ROWS, ROWS), ROWS)
            for c in range(pieces):
                wide_ref[pl.ds(t * ROWS * pieces + c, ROWS, stride=pieces), :] = table_ref[
                    span, c * LANES : (c + 1) * LANES
                ].astype(jnp.float32)

    groups = counts_ref.shape[2] // LANES
    half = neighbours // 2
    packed = 16
    tall = 8
    batch = tall // groups
    big = jnp.int32(DEAD)

    @pl.when(lax.rem(j, batch) == 0)
    def _():
        base = base_ref[0]
        live = jnp.zeros((tall, LANES), jnp.int32)
        mine = jnp.zeros((tall, LANES), jnp.int32)

        def rows_of(k):
            return jnp.concatenate(
                [lists_ref[j + i, k * groups : (k + 1) * groups, :] for i in range(batch)]
            )

        words = [rows_of(k) for k in range(half)]
        places = []
        for k in range(neighbours):
            slot = words[k] & DEAD if k < half else words[k - half] >> 16
            local = slot - base
            inside = (local >= 0) & (local < cap)
            live = live + jnp.where(slot < DEAD, 1, 0)
            mine = mine + jnp.where(inside, 1, 0)
            places.append(jnp.where(inside, local, big).astype(jnp.float32))
        for a, b in sort_pairs(neighbours):
            low, high = jnp.minimum(places[a], places[b]), jnp.maximum(places[a], places[b])
            places[a], places[b] = low, high
        rows = pl.ds(pl.multiple_of(j * groups, tall), tall)
        run = jnp.ones((tall, LANES), jnp.float32)
        for k in range(neighbours):
            if k:
                run = jnp.where(places[k] == places[k - 1], run + 1.0, 1.0)
            order_ref[k, rows, :] = places[k].astype(jnp.int32)
            times_ref[k, rows, :] = run
        mine_ref[rows, :] = mine
        for i in range(batch):
            most_ref[j + i] = jnp.max(mine[i * groups : (i + 1) * groups])
        alive_ref[rows, :] = live
        own = rows_of(half) - base
        self_ref[rows, :] = jnp.where((own >= 0) & (own < cap), own, big)

    chunk = 320 if cap % 320 == 0 else ROWS
    tiles = chunk // packed
    tile = (packed, LANES)
    iota = lax.broadcasted_iota(jnp.int32, tile, 0)

    def entry(k, row):
        slot = jnp.broadcast_to(order_ref[k, row, :], tile)
        return slot, jnp.broadcast_to(times_ref[k, row, :], tile).astype(jnp.bfloat16)

    def mark(totals, slot, times, first):
        local = (slot - first).astype(jnp.int16)
        return tuple(
            jnp.where((iota + packed * t).astype(jnp.int16) == local, times, totals[t])
            for t in range(tiles)
        )

    def spans(first):
        return [pl.ds(pl.multiple_of(first + packed * t, packed), packed) for t in range(tiles)]

    for g in range(groups):
        lanes = pl.ds(g * LANES, LANES)
        row = pl.ds(j * groups + g, 1)
        live_ref[0, :, lanes] = alive_ref[row, :]
        own_ref[0, :, lanes] = self_ref[row, :]
        entries = [entry(k, row) for k in range(SURE)]

        @pl.loop(0, cap // chunk)
        def _(c):
            totals = (jnp.zeros(tile, jnp.bfloat16),) * tiles
            for slot, times in entries:
                totals = mark(totals, slot, times, c * chunk)
            for span, total in zip(spans(c * chunk), totals):
                counts_ref[0, span, lanes] = total

    @pl.when(most_ref[j] > SURE)
    def _():
        for g in range(groups):
            lanes = pl.ds(g * LANES, LANES)
            row = pl.ds(j * groups + g, 1)
            most = jnp.max(mine_ref[row, :])

            @pl.when(most > SURE)
            def _():
                @pl.loop(0, cap // chunk)
                def _(c):
                    totals = tuple(counts_ref[0, span, lanes] for span in spans(c * chunk))
                    totals = lax.fori_loop(
                        SURE, most, lambda k, t: mark(t, *entry(k, row), c * chunk), totals
                    )
                    for span, total in zip(spans(c * chunk), totals):
                        counts_ref[0, span, lanes] = total

    burst = 32

    @pl.loop(0, cap // burst)
    def _(i):
        first = j * cap + i * burst
        start = pl.multiple_of(i * (burst * pieces), burst * pieces)
        places = [pl.multiple_of(index_ref[first + u], pieces) for u in range(burst)]
        for u in range(burst):
            picked_ref[pl.ds(start + u * pieces, pieces), :] = wide_ref[pl.ds(places[u], pieces), :]

    @pl.loop(0, cap // ROWS)
    def _(t):
        span = pl.ds(pl.multiple_of(t * ROWS, ROWS), ROWS)
        for c in range(pieces):
            rows_ref[0, span, c * LANES : (c + 1) * LANES] = picked_ref[
                pl.ds(t * ROWS * pieces + c, ROWS, stride=pieces), :
            ].astype(jnp.bfloat16)


def pick_and_count(base, index, lists, table, neighbours, cap):
    peers = lists.shape[0]
    groups = lists.shape[1] // (neighbours // 2 + 1)
    negatives = groups * LANES
    rows = peers * groups
    width = table.shape[1]
    pieces = width // LANES
    return pl.pallas_call(
        functools.partial(count_kernel, neighbours, cap),
        grid=(peers,),
        out_shape=(
            jax.ShapeDtypeStruct((peers, cap, negatives), jnp.bfloat16),
            jax.ShapeDtypeStruct((peers, 1, negatives), jnp.int32),
            jax.ShapeDtypeStruct((peers, 1, negatives), jnp.int32),
            jax.ShapeDtypeStruct((peers, cap, width), jnp.bfloat16),
        ),
        in_specs=[
            pl.BlockSpec(memory_space=pltpu.SMEM),
            pl.BlockSpec(memory_space=pltpu.SMEM),
            pl.BlockSpec(memory_space=pltpu.VMEM),
            pl.BlockSpec(memory_space=pltpu.VMEM),
        ],
        out_specs=(
            pl.BlockSpec((1, cap, negatives), lambda j: (j, 0, 0)),
            pl.BlockSpec((1, 1, negatives), lambda j: (j, 0, 0)),
            pl.BlockSpec((1, 1, negatives), lambda j: (j, 0, 0)),
            pl.BlockSpec((1, cap, width), lambda j: (j, 0, 0)),
        ),
        scratch_shapes=[
            pltpu.VMEM((neighbours, rows, LANES), jnp.int32),
            pltpu.VMEM((neighbours, rows, LANES), jnp.float32),
            pltpu.VMEM((rows, LANES), jnp.int32),
            pltpu.SMEM((peers,), jnp.int32),
            pltpu.VMEM((rows, LANES), jnp.int32),
            pltpu.VMEM((rows, LANES), jnp.int32),
            pltpu.VMEM((table.shape[0] * pieces, LANES), jnp.float32),
            pltpu.VMEM((cap * pieces, LANES), jnp.float32),
        ],
        compiler_params=pltpu.CompilerParams(vmem_limit_bytes=48 << 20),
    )(base, index * pieces, lists, table)


def reduce_kernel(
    rows_ref, counts_ref, live_ref, own_ref, wm_ref, mb_ref, ws_ref, wn_ref,
    queries_ref, hidden_ref, around_ref,
    hot_ref, message_ref, from_ref, into_ref, total_ref, part_ref,
    relay1, full1, relay2, full2,
    s_relay1, r_relay1, s_full1, r_full1, s_relay2, r_relay2, s_full2, r_full2, s_query, r_query,
):
    step = pl.program_id(0)
    x, y, z, core = place()
    _, cap, width = rows_ref.shape
    negatives = counts_ref.shape[2]
    groups = negatives // LANES
    half, quarter = negatives // 2, negatives // 4
    packed = 16

    def neighbour(axis, sign):
        if axis == 0:
            return device(x + sign, y, z, core)
        return device(x, y + sign, z, core)

    up, down, sibling = device(x, y, z + 1, core), device(x, y, z - 1, core), device(x, y, z, 1 - core)
    upper = pl.ds(0, queries_ref.shape[0] // 2)
    lower = pl.ds(queries_ref.shape[0] // 2, queries_ref.shape[0] // 2)

    def query_copy(which):
        sem = (s_query.at[which], r_query.at[which])
        if which == 0:
            return remote(queries_ref, around_ref.at[6], *sem, up)
        if which == 1:
            return remote(queries_ref, around_ref.at[2], *sem, down)
        if which == 2:
            return remote(queries_ref, around_ref.at[1], *sem, sibling)
        if which == 3:
            return remote(around_ref.at[6, upper], around_ref.at[4, upper], *sem, up)
        if which == 4:
            return remote(around_ref.at[2, lower], around_ref.at[4, lower], *sem, down)
        slot = {5: 6, 6: 2, 7: 4}[which]
        return remote(around_ref.at[slot], around_ref.at[slot + 1], *sem, sibling)

    @pl.when(step == 0)
    def _():
        greet(
            [neighbour(0, 1), neighbour(0, -1), neighbour(1, 1), neighbour(1, -1), up, down, sibling]
        )
        for which in range(3):
            query_copy(which).start()

    @pl.when(step == 7)
    def _():
        for which in (0, 1):
            query_copy(which).wait_recv()
        for which in (3, 4, 5, 6):
            query_copy(which).start()

    @pl.when(step == 12)
    def _():
        for which in (3, 4):
            query_copy(which).wait_recv()
        query_copy(7).start()

    tile = (packed, LANES)
    iota = lax.broadcasted_iota(jnp.int32, tile, 0)
    heres = [(iota + i * packed).astype(jnp.int16) for i in range(cap // packed)]
    zero = jnp.zeros(tile, jnp.bfloat16)
    for g in range(groups):
        lanes = pl.ds(g * LANES, LANES)
        own = jnp.broadcast_to(own_ref[0, :, lanes], tile).astype(jnp.int16)
        live = jnp.broadcast_to(live_ref[0, :, lanes].astype(jnp.float32), tile).astype(jnp.bfloat16)
        for i, here in enumerate(heres):
            hot_ref[i * packed : (i + 1) * packed, lanes] = jnp.where(here == own, live, zero)

    columns = [slice(c, c + width // 2) for c in (0, width // 2)]
    into_ref[:, :cap] = counts_ref[0].T
    into_ref[:, cap:] = hot_ref[...].T

    def dot(a, b):
        return jnp.dot(a, b, preferred_element_type=jnp.float32)

    for s in columns:
        message_ref[:, s] = jax.nn.relu(dot(rows_ref[0], wm_ref[:, s]) + mb_ref[:, s]).astype(
            jnp.bfloat16
        )
        from_ref[cap:, s] = dot(rows_ref[0], ws_ref[:, s]).astype(jnp.bfloat16)
    for s in columns:
        from_ref[:cap, s] = dot(message_ref[...], wn_ref[:, s]).astype(jnp.bfloat16)
    for s in columns:
        total_ref[:, s] = dot(into_ref[...], from_ref[:, s])

    block = 32

    def combine(first, count, sources):
        @pl.loop(0, count // block)
        def _(i):
            span = pl.ds(pl.multiple_of(first + i * block, block), block)
            value = total_ref[span, :]
            for source, begin in sources:
                value = value + source[
                    pl.ds(pl.multiple_of(begin + i * block, block), block), :
                ].astype(jnp.float32)
            total_ref[span, :] = value

    def pack(j, first):
        @pl.loop(0, half // block)
        def _(i):
            span = pl.ds(pl.multiple_of(first + i * block, block), block)
            part_ref[j, span, :] = total_ref[span, :].astype(jnp.bfloat16)

    def relay_copy(j, first, axis, side, relay, send, recv, at):
        return remote(
            part_ref.at[j, pl.ds(first + side * quarter, quarter)],
            relay.at[(*at, side)], send.at[(*at, side)], recv.at[(*at, side)],
            neighbour(axis, 1 - 2 * side),
        )

    def full_copy(j, first, axis, side, full, send, recv, at):
        return remote(
            part_ref.at[j, pl.ds(first, half)],
            full.at[(*at, side)], send.at[(*at, side)], recv.at[(*at, side)],
            neighbour(axis, 1 - 2 * side),
        )

    def ring(j, first, axis, offset, bufs, at):
        relay, full, s_relay, r_relay, s_full, r_full = bufs
        if offset == 2:
            pack(j, first)
            for side in (0, 1):
                relay_copy(j, first, axis, side, relay, s_relay, r_relay, at).start()
        elif offset in (1, 3):
            side = 0 if offset == 1 else 1
            relay_copy(j, first, axis, side, relay, s_relay, r_relay, at).wait_recv()
            combine(first + side * quarter, quarter, [(relay.at[(*at, side)], 0)])
            pack(j, first)
            full_copy(j, first, axis, side, full, s_full, r_full, at).start()
        else:
            for side in (0, 1):
                full_copy(j, first, axis, side, full, s_full, r_full, at).wait_recv()
            combine(first, half, [(full.at[(*at, side)], 0) for side in (0, 1)])

    stage1 = (relay1, full1, s_relay1, r_relay1, s_full1, r_full1)
    stage2 = (relay2, full2, s_relay2, r_relay2, s_full2, r_full2)
    for j, offsets in enumerate(ORDER):

        @pl.when(step == j)
        def _(j=j, offsets=offsets):
            for h in (0, 1):
                first = h * half
                near, far = offsets[h], offsets[1 - h]
                ring(j, first, h, near, stage1, (h, far))
                if near == 0:
                    ring(j, first, 1 - h, far, stage2, (h,))

    @pl.when(step == len(ORDER) - 1)
    def _():
        hidden_ref[...] = total_ref[...]
        for j, offsets in enumerate(ORDER):
            for h in (0, 1):
                first = h * half
                near, far = offsets[h], offsets[1 - h]
                stages = [(near, h, stage1, (h, far))]
                if near == 0:
                    stages.append((far, 1 - h, stage2, (h,)))
                for offset, axis, bufs, at in stages:
                    relay, full, s_relay, r_relay, s_full, r_full = bufs
                    if offset == 2:
                        for side in (0, 1):
                            relay_copy(j, first, axis, side, relay, s_relay, r_relay, at).wait_send()
                    elif offset in (1, 3):
                        side = 0 if offset == 1 else 1
                        full_copy(j, first, axis, side, full, s_full, r_full, at).wait_send()
        for which in (2, 5, 6, 7):
            query_copy(which).wait_recv()
        for which in range(8):
            query_copy(which).wait_send()


def reduce_parts(picked, counts, live, own, wm, mb, ws, wn, queries):
    peers, cap, negatives = counts.shape
    width = picked.shape[2]
    half, quarter = negatives // 2, negatives // 4
    vmem = pl.BlockSpec(memory_space=pltpu.VMEM)
    hbm = pl.BlockSpec(memory_space=pl.ANY)
    dma = pltpu.SemaphoreType.DMA
    bf16, f32 = jnp.bfloat16, jnp.float32
    return pl.pallas_call(
        reduce_kernel,
        grid=(peers,),
        out_shape=(
            jax.ShapeDtypeStruct((negatives, width), f32),
            jax.ShapeDtypeStruct((8,) + queries.shape, queries.dtype),
        ),
        in_specs=[
            pl.BlockSpec((1, cap, width), lambda j: (j, 0, 0)),
            pl.BlockSpec((1, cap, negatives), lambda j: (j, 0, 0)),
            pl.BlockSpec((1, 1, negatives), lambda j: (j, 0, 0)),
            pl.BlockSpec((1, 1, negatives), lambda j: (j, 0, 0)),
            vmem, vmem, vmem, vmem,
            hbm,
        ],
        out_specs=(vmem, hbm),
        scratch_shapes=[
            pltpu.VMEM((cap, negatives), bf16),
            pltpu.VMEM((cap, width), bf16),
            pltpu.VMEM((2 * cap, width), bf16),
            pltpu.VMEM((negatives, 2 * cap), bf16),
            pltpu.VMEM((negatives, width), f32),
            pltpu.VMEM((peers, negatives, width), bf16),
            pltpu.VMEM((2, SIDE, 2, quarter, width), bf16),
            pltpu.VMEM((2, SIDE, 2, half, width), bf16),
            pltpu.VMEM((2, 2, quarter, width), bf16),
            pltpu.VMEM((2, 2, half, width), bf16),
            dma((2, SIDE, 2)), dma((2, SIDE, 2)), dma((2, SIDE, 2)), dma((2, SIDE, 2)),
            dma((2, 2)), dma((2, 2)), dma((2, 2)), dma((2, 2)),
            dma((8,)), dma((8,)),
        ],
        compiler_params=pltpu.CompilerParams(
            collective_id=1, has_side_effects=True, vmem_limit_bytes=62 << 20
        ),
    )(picked, counts, live, own, wm, mb, ws, wn, queries)


def score_kernel(
    total_negatives, hidden_ref, queries_ref, around_ref, bias_ref, count_ref, live_ref,
    embed_ref, lse_ref,
    log_ref, block_ref, mine_ref, slots_ref, merged_ref, all_ref,
    s_load, s_send1, r_send1, s_send2, r_send2,
):
    x, y, z, core = place()
    others = ORDER[:-1]
    near = [(dz, c) for dz in range(SIDE) for c in (0, 1)][1:]
    greet(
        [device(x, y, z - dz, core if c == 0 else 1 - core) for dz, c in near]
        + [device(x - dx, y - dy, z, core) for dx, dy in others]
    )

    def load(slot):
        buffer = 1 + lax.rem(slot, 2)
        return pltpu.make_async_copy(around_ref.at[slot], block_ref.at[buffer], s_load.at[buffer])

    own_load = pltpu.make_async_copy(queries_ref, block_ref.at[0], s_load.at[0])
    own_load.start()

    load(1).start()
    negatives = hidden_ref.shape[0]

    def column(row_ref):
        row = row_ref[...].astype(jnp.float32)
        return jnp.broadcast_to(row, (LANES, negatives)).T

    log_ref[...] = LOG2E * jnp.log(column(count_ref))
    inverse = 1.0 / column(live_ref)[:, :1]
    hidden = jax.nn.relu(hidden_ref[...] * inverse + bias_ref[...])
    scale = lax.rsqrt(jnp.mean(hidden * hidden, axis=1, keepdims=True) + 0.25)
    embed_ref[...] = (hidden * scale).astype(jnp.bfloat16)
    tile = 256

    def score(slot, ref):
        for t in range(queries_ref.shape[0] // tile):
            span = pl.ds(t * tile, tile)
            product = lax.dot_general(
                embed_ref[...], ref[span, :], NT, preferred_element_type=jnp.float32
            )
            logs = jnp.concatenate([log_ref[...]] * (tile // LANES), axis=1)
            scores = (0.25 * LOG2E) * product - logs
            peak = jnp.max(scores, axis=0, keepdims=True)
            total = jnp.sum(jnp.exp2(scores - peak), axis=0, keepdims=True)
            mine_ref[slot, :, span] = (peak + jnp.log2(total)) * (1 / LOG2E)

    def exchange1(slot):
        dz, c = lax.div(slot, 2), lax.rem(slot, 2)
        return remote(
            mine_ref.at[slot], slots_ref.at[slot], s_send1.at[slot], r_send1.at[slot],
            device(x, y, z + dz, lax.rem(core + c, 2)),
        )

    @pl.loop(0, 8)
    def _(turn):
        slot = lax.rem(turn + 1, 8)

        @pl.when(turn < 6)
        def _():
            load(slot + 1).start()

        @pl.when(turn < 7)
        def _():
            load(slot).wait()

        @pl.when(turn == 7)
        def _():
            own_load.wait()

        score(slot, block_ref.at[lax.select(slot == 0, 0, 1 + lax.rem(slot, 2))])

        @pl.when(turn < 7)
        def _():
            exchange1(slot).start()

    slots_ref[0] = mine_ref[0]
    for slot in range(1, 8):
        exchange1(slot).wait_recv()

    def merge(ref, count):
        values = [ref[i] for i in range(count)]
        top = functools.reduce(jnp.maximum, values)
        return top + jnp.log(sum(jnp.exp(v - top) for v in values))

    merged_ref[...] = merge(slots_ref, 8)

    def exchange2(j):
        dx, dy = others[j]
        return remote(
            merged_ref, all_ref.at[j], s_send2.at[j], r_send2.at[j], device(x - dx, y - dy, z, core)
        )

    for j in range(len(others)):
        exchange2(j).start()
    all_ref[len(others)] = merged_ref[...]
    for j in range(len(others)):
        exchange2(j).wait_recv()
    lse_ref[...] = merge(all_ref, len(others) + 1) - math.log(total_negatives)
    for slot in range(1, 8):
        exchange1(slot).wait_send()
    for j in range(len(others)):
        exchange2(j).wait_send()


def embed_and_score(hidden, queries, around, bias, count, live, total_negatives):
    negatives, width = hidden.shape
    rows = queries.shape[0]
    vmem = pl.BlockSpec(memory_space=pltpu.VMEM)
    hbm = pl.BlockSpec(memory_space=pl.ANY)
    dma = pltpu.SemaphoreType.DMA
    f32 = jnp.float32
    return pl.pallas_call(
        functools.partial(score_kernel, total_negatives),
        out_shape=(
            jax.ShapeDtypeStruct((negatives, width), jnp.bfloat16),
            jax.ShapeDtypeStruct((1, rows), f32),
        ),
        in_specs=[vmem, hbm, hbm, vmem, vmem, vmem],
        out_specs=(vmem, vmem),
        scratch_shapes=[
            pltpu.VMEM((negatives, LANES), f32),
            pltpu.VMEM((3, rows, width), jnp.bfloat16),
            pltpu.VMEM((8, 1, rows), f32),
            pltpu.VMEM((8, 1, rows), f32),
            pltpu.VMEM((1, rows), f32),
            pltpu.VMEM((16, 1, rows), f32),
            dma((3,)), dma((8,)), dma((8,)), dma((15,)), dma((15,)),
        ],
        compiler_params=pltpu.CompilerParams(collective_id=2, has_side_effects=True),
    )(hidden, queries, around, bias, count, live)


def per_device(
    items_table,
    fetch_rows,
    neighbour_slots,
    neighbour_count,
    self_slot,
    negative_count,
    message_weight,
    message_bias,
    self_weight,
    neighbour_weight,
    output_bias,
    queries,
):
    n_neg, n_qry = lax.axis_size("neg"), lax.axis_size("qry")
    own_neg, own_qry = lax.axis_index("neg"), lax.axis_index("qry")
    cap = fetch_rows.shape[1]
    negatives, neighbours = neighbour_slots.shape

    assert n_neg * cap < DEAD and neighbours % 4 == 0 and n_neg == SIDE * SIDE and n_qry == 8
    live = jnp.arange(neighbours, dtype=jnp.int32)[None, :] < neighbour_count[:, None]
    slots = jnp.where(live, neighbour_slots, DEAD).T
    half = neighbours // 2
    words = slots[:half] | (slots[half:] << 16)
    lists = jnp.concatenate([words.reshape(-1, LANES), self_slot.reshape(-1, LANES)])
    all_lists, all_fetch = exchange_lists(lists, fetch_rows.reshape(n_neg, cap // LANES, LANES))
    base = (own_neg * cap).astype(jnp.int32).reshape(1)
    counts, lives, own, picked = pick_and_count(
        base, all_fetch.reshape(n_neg * cap), all_lists, items_table, neighbours, cap
    )
    hidden, around = reduce_parts(
        picked, counts, lives, own,
        message_weight, message_bias[None, :], self_weight, neighbour_weight, queries,
    )
    count = lax.dynamic_slice_in_dim(negative_count, own_qry * negatives, negatives)
    negative_embed, query_lse = embed_and_score(
        hidden, queries, around, output_bias[None, :], count[None, :], neighbour_count[None, :],
        negatives * n_neg * n_qry,
    )
    return (negative_embed, query_lse.reshape(-1))


def solution(mesh):
    in_specs = (
        P("neg", None),
        P(("neg", "qry"), None),
        P(("neg", "qry"), None),
        P(("neg", "qry")),
        P(("neg", "qry")),
        P("neg"),
        P(),
        P(),
        P(),
        P(),
        P(),
        P("qry", None),
    )
    out_specs = (P(("neg", "qry"), None), P("qry"))
    return jax.shard_map(
        per_device, mesh=mesh, in_specs=in_specs, out_specs=out_specs, check_vma=False
    )
```

```python
import functools
import math

import jax
import jax.numpy as jnp
from jax import lax
from jax.experimental import pallas as pl
from jax.experimental.pallas import tpu as pltpu
from jax.sharding import PartitionSpec as P


LANES = 128
ROWS = 128
DEAD = 32767
SIDE = 4
NT = (((1,), (1,)), ((), ()))
SURE = 10
LOG2E = math.log2(math.e)
MESH = pl.DeviceIdType.MESH
ORDER = (
    (2, 2), (2, 1), (2, 3), (1, 2), (3, 2), (2, 0), (0, 2), (1, 1),
    (1, 3), (3, 1), (3, 3), (1, 0), (3, 0), (0, 1), (0, 3), (0, 0),
)


def sort_pairs(count):
    full = 1
    while full < count:
        full *= 2
    pairs = []
    p = 1
    while p < full:
        k = p
        while k >= 1:
            for j in range(k % p, full - k, 2 * k):
                for i in range(min(k, full - j - k)):
                    if (i + j) // (2 * p) == (i + j + k) // (2 * p):
                        if i + j + k < count:
                            pairs.append((i + j, i + j + k))
            k //= 2
        p *= 2
    return pairs


def place():
    neg, qry = lax.axis_index("neg"), lax.axis_index("qry")
    return neg // SIDE, neg % SIDE, qry // 2, qry % 2


def device(x, y, z, core):
    wrap = lambda v: lax.rem(v + 2 * SIDE, SIDE)
    return (wrap(x) * SIDE + wrap(y), wrap(z) * 2 + core)


def remote(src, dst, send, recv, target):
    return pltpu.make_async_remote_copy(
        src_ref=src, dst_ref=dst, send_sem=send, recv_sem=recv,
        device_id=target, device_id_type=MESH,
    )


def greet(peers):
    barrier = pltpu.get_barrier_semaphore()
    for peer in peers:
        pl.semaphore_signal(barrier, inc=1, device_id=peer, device_id_type=MESH)
    pl.semaphore_wait(barrier, len(peers))


def exchange_kernel(pieces, lists_ref, fetch_ref, all_lists, all_fetch, asked_ref, sends, recvs):
    x, y, z, core = place()
    others = ORDER[:-1]
    for p in range(SIDE * SIDE):
        asked_ref[p] = fetch_ref[p : p + 1, :] * pieces
    greet([device(x - dx, y - dy, z, core) for dx, dy in others])
    copies = []
    for j, (dx, dy) in enumerate(others):
        target = device(x - dx, y - dy, z, core)
        copies.append(
            remote(asked_ref.at[target[0]], all_fetch.at[j], sends.at[0, j], recvs.at[0, j], target)
        )
        copies.append(remote(lists_ref, all_lists.at[j], sends.at[1, j], recvs.at[1, j], target))
    for copy in copies:
        copy.start()
    last = len(others)
    all_fetch[last] = asked_ref[x * SIDE + y]
    all_lists[last] = lists_ref[...]
    for copy in copies:
        copy.wait()


def exchange_lists(lists, fetch, pieces):
    peers, cap = fetch.shape
    vmem = pl.BlockSpec(memory_space=pltpu.VMEM)
    return pl.pallas_call(
        functools.partial(exchange_kernel, pieces),
        out_shape=(
            jax.ShapeDtypeStruct((peers,) + lists.shape, lists.dtype),
            jax.ShapeDtypeStruct((peers, 1, cap), fetch.dtype),
        ),
        in_specs=[vmem, vmem],
        out_specs=(vmem, vmem),
        scratch_shapes=[
            pltpu.VMEM((peers, 1, cap), fetch.dtype),
            pltpu.SemaphoreType.DMA((2, peers - 1)),
            pltpu.SemaphoreType.DMA((2, peers - 1)),
        ],
        compiler_params=pltpu.CompilerParams(collective_id=0, has_side_effects=True),
    )(lists, fetch)


def count_kernel(
    neighbours, cap, base_ref, index_ref, lists_ref, table_ref,
    counts_ref, live_ref, own_ref, rows_ref,
    order_ref, times_ref, mine_ref, most_ref, alive_ref, self_ref, wide_ref, picked_ref,
):
    j = pl.program_id(0)
    rows, width = table_ref.shape
    pieces = width // LANES

    @pl.when(j == 0)
    def _():
        @pl.loop(0, rows // ROWS)
        def _(t):
            span = pl.ds(pl.multiple_of(t * ROWS, ROWS), ROWS)
            for c in range(pieces):
                wide_ref[pl.ds(t * ROWS * pieces + c, ROWS, stride=pieces), :] = table_ref[
                    span, c * LANES : (c + 1) * LANES
                ].astype(jnp.float32)

    groups = counts_ref.shape[2] // LANES
    half = neighbours // 2
    packed = 16
    tall = 8
    batch = tall // groups
    big = jnp.int32(DEAD)

    @pl.when(lax.rem(j, batch) == 0)
    def _():
        base = base_ref[0]
        live = jnp.zeros((tall, LANES), jnp.int32)
        mine = jnp.zeros((tall, LANES), jnp.int32)

        def rows_of(k):
            return jnp.concatenate(
                [lists_ref[j + i, k * groups : (k + 1) * groups, :] for i in range(batch)]
            )

        words = [rows_of(k) for k in range(half)]
        places = []
        for k in range(neighbours):
            slot = words[k] & DEAD if k < half else words[k - half] >> 16
            local = slot - base
            inside = (local >= 0) & (local < cap)
            live = live + jnp.where(slot < DEAD, 1, 0)
            mine = mine + jnp.where(inside, 1, 0)
            places.append(jnp.where(inside, local, big).astype(jnp.float32))
        for a, b in sort_pairs(neighbours):
            low, high = jnp.minimum(places[a], places[b]), jnp.maximum(places[a], places[b])
            places[a], places[b] = low, high
        rows = pl.ds(pl.multiple_of(j * groups, tall), tall)
        run = jnp.ones((tall, LANES), jnp.float32)
        for k in range(neighbours):
            if k:
                run = jnp.where(places[k] == places[k - 1], run + 1.0, 1.0)
            order_ref[k, rows, :] = places[k].astype(jnp.int32)
            times_ref[k, rows, :] = run
        mine_ref[rows, :] = mine
        for i in range(batch):
            most_ref[j + i] = jnp.max(mine[i * groups : (i + 1) * groups])
        alive_ref[rows, :] = live
        own = rows_of(half) - base
        self_ref[rows, :] = jnp.where((own >= 0) & (own < cap), own, big)

    chunk = 320 if cap % 320 == 0 else ROWS
    tiles = chunk // packed
    tile = (packed, LANES)
    iota = lax.broadcasted_iota(jnp.int32, tile, 0)

    def entry(k, row):
        slot = jnp.broadcast_to(order_ref[k, row, :], tile)
        return slot, jnp.broadcast_to(times_ref[k, row, :], tile).astype(jnp.bfloat16)

    def mark(totals, slot, times, first):
        local = (slot - first).astype(jnp.int16)
        return tuple(
            jnp.where((iota + packed * t).astype(jnp.int16) == local, times, totals[t])
            for t in range(tiles)
        )

    def spans(first):
        return [pl.ds(pl.multiple_of(first + packed * t, packed), packed) for t in range(tiles)]

    for g in range(groups):
        lanes = pl.ds(g * LANES, LANES)
        live_ref[0, :, lanes] = alive_ref[pl.ds(j * groups + g, 1), :]
        own_ref[0, :, lanes] = self_ref[pl.ds(j * groups + g, 1), :]

    parts = cap // chunk
    turns = groups * parts
    share = cap // turns

    burst = share // SURE
    casts = [(p, i) for i in range(share // packed) for p in range(pieces)]

    def cast(buffer, target, p, i):
        rows_ref[
            0,
            pl.ds(pl.multiple_of(target + i * packed, packed), packed),
            p * LANES : (p + 1) * LANES,
        ] = picked_ref[
            buffer, i * packed * pieces + p : (i + 1) * packed * pieces : pieces, :
        ].astype(jnp.bfloat16)

    @pl.loop(0, groups)
    def _(g):
        lanes = pl.ds(pl.multiple_of(g * LANES, LANES), LANES)
        row = pl.ds(j * groups + g, 1)
        for c in range(parts):
            turn = g * parts + c
            first = j * cap + turn * share
            here, there = c % 2, 1 - c % 2
            before = lax.max(turn - 1, 0) * share
            totals = (jnp.zeros(tile, jnp.bfloat16),) * tiles
            for k in range(SURE):
                places = [
                    pl.multiple_of(index_ref[first + k * burst + u], pieces) for u in range(burst)
                ]
                for u in range(burst):
                    into = (k * burst + u) * pieces
                    picked_ref[here, into : into + pieces, :] = wide_ref[pl.ds(places[u], pieces), :]
                totals = mark(totals, *entry(k, row), c * chunk)
                for p, i in casts[k * len(casts) // SURE : (k + 1) * len(casts) // SURE]:
                    cast(there, before, p, i)
            for span, total in zip(spans(c * chunk), totals):
                counts_ref[0, span, lanes] = total

    for p, i in casts:
        cast((turns - 1) % 2, (turns - 1) * share, p, i)

    @pl.when(most_ref[j] > SURE)
    def _():
        for g in range(groups):
            lanes = pl.ds(g * LANES, LANES)
            row = pl.ds(j * groups + g, 1)
            most = jnp.max(mine_ref[row, :])

            @pl.when(most > SURE)
            def _():
                @pl.loop(0, cap // chunk)
                def _(c):
                    totals = tuple(counts_ref[0, span, lanes] for span in spans(c * chunk))
                    totals = lax.fori_loop(
                        SURE, most, lambda k, t: mark(t, *entry(k, row), c * chunk), totals
                    )
                    for span, total in zip(spans(c * chunk), totals):
                        counts_ref[0, span, lanes] = total


def pick_and_count(base, index, lists, table, neighbours, cap):
    peers = lists.shape[0]
    groups = lists.shape[1] // (neighbours // 2 + 1)
    negatives = groups * LANES
    rows = peers * groups
    width = table.shape[1]
    pieces = width // LANES
    return pl.pallas_call(
        functools.partial(count_kernel, neighbours, cap),
        grid=(peers,),
        out_shape=(
            jax.ShapeDtypeStruct((peers, cap, negatives), jnp.bfloat16),
            jax.ShapeDtypeStruct((peers, 1, negatives), jnp.int32),
            jax.ShapeDtypeStruct((peers, 1, negatives), jnp.int32),
            jax.ShapeDtypeStruct((peers, cap, width), jnp.bfloat16),
        ),
        in_specs=[
            pl.BlockSpec(memory_space=pltpu.SMEM),
            pl.BlockSpec(memory_space=pltpu.SMEM),
            pl.BlockSpec(memory_space=pltpu.VMEM),
            pl.BlockSpec(memory_space=pltpu.VMEM),
        ],
        out_specs=(
            pl.BlockSpec((1, cap, negatives), lambda j: (j, 0, 0)),
            pl.BlockSpec((1, 1, negatives), lambda j: (j, 0, 0)),
            pl.BlockSpec((1, 1, negatives), lambda j: (j, 0, 0)),
            pl.BlockSpec((1, cap, width), lambda j: (j, 0, 0)),
        ),
        scratch_shapes=[
            pltpu.VMEM((neighbours, rows, LANES), jnp.int32),
            pltpu.VMEM((neighbours, rows, LANES), jnp.float32),
            pltpu.VMEM((rows, LANES), jnp.int32),
            pltpu.SMEM((peers,), jnp.int32),
            pltpu.VMEM((rows, LANES), jnp.int32),
            pltpu.VMEM((rows, LANES), jnp.int32),
            pltpu.VMEM((table.shape[0] * pieces, LANES), jnp.float32),
            pltpu.VMEM((2, cap * pieces // 8, LANES), jnp.float32),
        ],
        compiler_params=pltpu.CompilerParams(vmem_limit_bytes=48 << 20),
    )(base, index, lists, table)


def reduce_kernel(
    rows_ref, counts_ref, live_ref, own_ref, wm_ref, mb_ref, ws_ref, wn_ref,
    queries_ref, hidden_ref, around_ref,
    hot_ref, message_ref, from_ref, into_ref, total_ref, part_ref,
    relay1, full1, relay2, full2,
    s_relay1, r_relay1, s_full1, r_full1, s_relay2, r_relay2, s_full2, r_full2, s_query, r_query,
):
    step = pl.program_id(0)
    x, y, z, core = place()
    _, cap, width = rows_ref.shape
    negatives = counts_ref.shape[2]
    groups = negatives // LANES
    half, quarter = negatives // 2, negatives // 4
    packed = 16

    def neighbour(axis, sign):
        if axis == 0:
            return device(x + sign, y, z, core)
        return device(x, y + sign, z, core)

    up, down, sibling = device(x, y, z + 1, core), device(x, y, z - 1, core), device(x, y, z, 1 - core)
    upper = pl.ds(0, queries_ref.shape[0] // 2)
    lower = pl.ds(queries_ref.shape[0] // 2, queries_ref.shape[0] // 2)

    def query_copy(which):
        sem = (s_query.at[which], r_query.at[which])
        if which == 0:
            return remote(queries_ref, around_ref.at[6], *sem, up)
        if which == 1:
            return remote(queries_ref, around_ref.at[2], *sem, down)
        if which == 2:
            return remote(queries_ref, around_ref.at[1], *sem, sibling)
        if which == 3:
            return remote(around_ref.at[6, upper], around_ref.at[4, upper], *sem, up)
        if which == 4:
            return remote(around_ref.at[2, lower], around_ref.at[4, lower], *sem, down)
        slot = {5: 6, 6: 2, 7: 4}[which]
        return remote(around_ref.at[slot], around_ref.at[slot + 1], *sem, sibling)

    @pl.when(step == 0)
    def _():
        greet(
            [neighbour(0, 1), neighbour(0, -1), neighbour(1, 1), neighbour(1, -1), up, down, sibling]
        )
        for which in range(3):
            query_copy(which).start()

    @pl.when(step == 10)
    def _():
        for which in (0, 1):
            query_copy(which).wait_recv()
        for which in (3, 4, 5, 6):
            query_copy(which).start()

    @pl.when(step == 15)
    def _():
        for which in (3, 4):
            query_copy(which).wait_recv()
        query_copy(7).start()

    tile = (packed, LANES)
    iota = lax.broadcasted_iota(jnp.int32, tile, 0)
    heres = [(iota + i * packed).astype(jnp.int16) for i in range(cap // packed)]
    zero = jnp.zeros(tile, jnp.bfloat16)
    for g in range(groups):
        lanes = pl.ds(g * LANES, LANES)
        own = jnp.broadcast_to(own_ref[0, :, lanes], tile).astype(jnp.int16)
        live = jnp.broadcast_to(live_ref[0, :, lanes].astype(jnp.float32), tile).astype(jnp.bfloat16)
        for i, here in enumerate(heres):
            hot_ref[i * packed : (i + 1) * packed, lanes] = jnp.where(here == own, live, zero)

    columns = [slice(c, c + width // 2) for c in (0, width // 2)]
    into_ref[:, :cap] = counts_ref[0].T
    into_ref[:, cap:] = hot_ref[...].T

    def dot(a, b):
        return jnp.dot(a, b, preferred_element_type=jnp.float32)

    for s in columns:
        message_ref[:, s] = jax.nn.relu(dot(rows_ref[0], wm_ref[:, s]) + mb_ref[:, s]).astype(
            jnp.bfloat16
        )
        from_ref[cap:, s] = dot(rows_ref[0], ws_ref[:, s]).astype(jnp.bfloat16)
    for s in columns:
        from_ref[:cap, s] = dot(message_ref[...], wn_ref[:, s]).astype(jnp.bfloat16)
    for s in columns:
        total_ref[:, s] = dot(into_ref[...], from_ref[:, s])

    block = 32

    def combine(first, count, sources):
        @pl.loop(0, count // block)
        def _(i):
            span = pl.ds(pl.multiple_of(first + i * block, block), block)
            value = total_ref[span, :]
            for source, begin in sources:
                value = value + source[
                    pl.ds(pl.multiple_of(begin + i * block, block), block), :
                ].astype(jnp.float32)
            total_ref[span, :] = value

    def pack(j, first):
        @pl.loop(0, half // block)
        def _(i):
            span = pl.ds(pl.multiple_of(first + i * block, block), block)
            part_ref[j, span, :] = total_ref[span, :].astype(jnp.bfloat16)

    def relay_copy(j, first, axis, side, relay, send, recv, at):
        return remote(
            part_ref.at[j, pl.ds(first + side * quarter, quarter)],
            relay.at[(*at, side)], send.at[(*at, side)], recv.at[(*at, side)],
            neighbour(axis, 1 - 2 * side),
        )

    def full_copy(j, first, axis, side, full, send, recv, at):
        return remote(
            part_ref.at[j, pl.ds(first, half)],
            full.at[(*at, side)], send.at[(*at, side)], recv.at[(*at, side)],
            neighbour(axis, 1 - 2 * side),
        )

    def ring(j, first, axis, offset, bufs, at):
        relay, full, s_relay, r_relay, s_full, r_full = bufs
        if offset == 2:
            pack(j, first)
            for side in (0, 1):
                relay_copy(j, first, axis, side, relay, s_relay, r_relay, at).start()
        elif offset in (1, 3):
            side = 0 if offset == 1 else 1
            relay_copy(j, first, axis, side, relay, s_relay, r_relay, at).wait_recv()
            combine(first + side * quarter, quarter, [(relay.at[(*at, side)], 0)])
            pack(j, first)
            full_copy(j, first, axis, side, full, s_full, r_full, at).start()
        else:
            for side in (0, 1):
                full_copy(j, first, axis, side, full, s_full, r_full, at).wait_recv()
            combine(first, half, [(full.at[(*at, side)], 0) for side in (0, 1)])

    stage1 = (relay1, full1, s_relay1, r_relay1, s_full1, r_full1)
    stage2 = (relay2, full2, s_relay2, r_relay2, s_full2, r_full2)
    for j, offsets in enumerate(ORDER):

        @pl.when(step == j)
        def _(j=j, offsets=offsets):
            for h in (0, 1):
                first = h * half
                near, far = offsets[h], offsets[1 - h]
                ring(j, first, h, near, stage1, (h, far))
                if near == 0:
                    ring(j, first, 1 - h, far, stage2, (h,))

    @pl.when(step == len(ORDER) - 1)
    def _():
        hidden_ref[...] = total_ref[...]
        for j, offsets in enumerate(ORDER):
            for h in (0, 1):
                first = h * half
                near, far = offsets[h], offsets[1 - h]
                stages = [(near, h, stage1, (h, far))]
                if near == 0:
                    stages.append((far, 1 - h, stage2, (h,)))
                for offset, axis, bufs, at in stages:
                    relay, full, s_relay, r_relay, s_full, r_full = bufs
                    if offset == 2:
                        for side in (0, 1):
                            relay_copy(j, first, axis, side, relay, s_relay, r_relay, at).wait_send()
                    elif offset in (1, 3):
                        side = 0 if offset == 1 else 1
                        full_copy(j, first, axis, side, full, s_full, r_full, at).wait_send()
        for which in (2, 5, 6, 7):
            query_copy(which).wait_recv()
        for which in range(8):
            query_copy(which).wait_send()


def reduce_parts(picked, counts, live, own, wm, mb, ws, wn, queries):
    peers, cap, negatives = counts.shape
    width = picked.shape[2]
    half, quarter = negatives // 2, negatives // 4
    vmem = pl.BlockSpec(memory_space=pltpu.VMEM)
    hbm = pl.BlockSpec(memory_space=pl.ANY)
    dma = pltpu.SemaphoreType.DMA
    bf16, f32 = jnp.bfloat16, jnp.float32
    return pl.pallas_call(
        reduce_kernel,
        grid=(peers,),
        out_shape=(
            jax.ShapeDtypeStruct((negatives, width), f32),
            jax.ShapeDtypeStruct((8,) + queries.shape, queries.dtype),
        ),
        in_specs=[
            pl.BlockSpec((1, cap, width), lambda j: (j, 0, 0)),
            pl.BlockSpec((1, cap, negatives), lambda j: (j, 0, 0)),
            pl.BlockSpec((1, 1, negatives), lambda j: (j, 0, 0)),
            pl.BlockSpec((1, 1, negatives), lambda j: (j, 0, 0)),
            vmem, vmem, vmem, vmem,
            hbm,
        ],
        out_specs=(vmem, hbm),
        scratch_shapes=[
            pltpu.VMEM((cap, negatives), bf16),
            pltpu.VMEM((cap, width), bf16),
            pltpu.VMEM((2 * cap, width), bf16),
            pltpu.VMEM((negatives, 2 * cap), bf16),
            pltpu.VMEM((negatives, width), f32),
            pltpu.VMEM((peers, negatives, width), bf16),
            pltpu.VMEM((2, SIDE, 2, quarter, width), bf16),
            pltpu.VMEM((2, SIDE, 2, half, width), bf16),
            pltpu.VMEM((2, 2, quarter, width), bf16),
            pltpu.VMEM((2, 2, half, width), bf16),
            dma((2, SIDE, 2)), dma((2, SIDE, 2)), dma((2, SIDE, 2)), dma((2, SIDE, 2)),
            dma((2, 2)), dma((2, 2)), dma((2, 2)), dma((2, 2)),
            dma((8,)), dma((8,)),
        ],
        compiler_params=pltpu.CompilerParams(
            collective_id=1, has_side_effects=True, vmem_limit_bytes=62 << 20
        ),
    )(picked, counts, live, own, wm, mb, ws, wn, queries)


def score_kernel(
    total_negatives, hidden_ref, queries_ref, around_ref, bias_ref, count_ref, live_ref,
    embed_ref, lse_ref,
    log_ref, block_ref, mine_ref, slots_ref, merged_ref, all_ref,
    s_load, s_send1, r_send1, s_send2, r_send2,
):
    x, y, z, core = place()
    others = ORDER[:-1]
    near = [(dz, c) for dz in range(SIDE) for c in (0, 1)][1:]
    greet(
        [device(x, y, z - dz, core if c == 0 else 1 - core) for dz, c in near]
        + [device(x - dx, y - dy, z, core) for dx, dy in others]
    )

    def load(slot):
        buffer = 1 + lax.rem(slot, 2)
        return pltpu.make_async_copy(around_ref.at[slot], block_ref.at[buffer], s_load.at[buffer])

    own_load = pltpu.make_async_copy(queries_ref, block_ref.at[0], s_load.at[0])
    own_load.start()

    load(1).start()
    negatives = hidden_ref.shape[0]

    def column(row_ref):
        row = row_ref[...].astype(jnp.float32)
        return jnp.broadcast_to(row, (LANES, negatives)).T

    mine = pl.ds(pl.multiple_of((2 * z + core) * negatives, negatives), negatives)
    log_ref[...] = LOG2E * jnp.log(column(count_ref.at[:, mine]))
    inverse = 1.0 / column(live_ref)[:, :1]
    hidden = jax.nn.relu(hidden_ref[...] * inverse + bias_ref[...])
    scale = lax.rsqrt(jnp.mean(hidden * hidden, axis=1, keepdims=True) + 0.25)
    embed_ref[...] = (hidden * scale).astype(jnp.bfloat16)
    tile = 256

    def score(slot, ref):
        for t in range(queries_ref.shape[0] // tile):
            span = pl.ds(t * tile, tile)
            product = lax.dot_general(
                embed_ref[...], ref[span, :], NT, preferred_element_type=jnp.float32
            )
            logs = jnp.concatenate([log_ref[...]] * (tile // LANES), axis=1)
            scores = (0.25 * LOG2E) * product - logs
            peak = jnp.max(scores, axis=0, keepdims=True)
            total = jnp.sum(jnp.exp2(scores - peak), axis=0, keepdims=True)
            mine_ref[slot, :, span] = (peak + jnp.log2(total)) * (1 / LOG2E)

    def exchange1(slot):
        dz, c = lax.div(slot, 2), lax.rem(slot, 2)
        return remote(
            mine_ref.at[slot], slots_ref.at[slot], s_send1.at[slot], r_send1.at[slot],
            device(x, y, z + dz, lax.rem(core + c, 2)),
        )

    @pl.loop(0, 8)
    def _(turn):
        slot = lax.rem(turn + 1, 8)

        @pl.when(turn < 6)
        def _():
            load(slot + 1).start()

        @pl.when(turn < 7)
        def _():
            load(slot).wait()

        @pl.when(turn == 7)
        def _():
            own_load.wait()

        score(slot, block_ref.at[lax.select(slot == 0, 0, 1 + lax.rem(slot, 2))])

        @pl.when(turn < 7)
        def _():
            exchange1(slot).start()

    slots_ref[0] = mine_ref[0]
    for slot in range(1, 8):
        exchange1(slot).wait_recv()

    def merge(ref, count):
        values = [ref[i] for i in range(count)]
        top = functools.reduce(jnp.maximum, values)
        return top + jnp.log(sum(jnp.exp(v - top) for v in values))

    merged_ref[...] = merge(slots_ref, 8)

    def exchange2(j):
        dx, dy = others[j]
        return remote(
            merged_ref, all_ref.at[j], s_send2.at[j], r_send2.at[j], device(x - dx, y - dy, z, core)
        )

    for j in range(len(others)):
        exchange2(j).start()
    all_ref[len(others)] = merged_ref[...]
    for j in range(len(others)):
        exchange2(j).wait_recv()
    lse_ref[...] = merge(all_ref, len(others) + 1) - math.log(total_negatives)
    for slot in range(1, 8):
        exchange1(slot).wait_send()
    for j in range(len(others)):
        exchange2(j).wait_send()


def embed_and_score(hidden, queries, around, bias, count, live, total_negatives):
    negatives, width = hidden.shape
    rows = queries.shape[0]
    vmem = pl.BlockSpec(memory_space=pltpu.VMEM)
    hbm = pl.BlockSpec(memory_space=pl.ANY)
    dma = pltpu.SemaphoreType.DMA
    f32 = jnp.float32
    return pl.pallas_call(
        functools.partial(score_kernel, total_negatives),
        out_shape=(
            jax.ShapeDtypeStruct((negatives, width), jnp.bfloat16),
            jax.ShapeDtypeStruct((1, rows), f32),
        ),
        in_specs=[vmem, hbm, hbm, vmem, vmem, vmem],
        out_specs=(vmem, vmem),
        scratch_shapes=[
            pltpu.VMEM((negatives, LANES), f32),
            pltpu.VMEM((3, rows, width), jnp.bfloat16),
            pltpu.VMEM((8, 1, rows), f32),
            pltpu.VMEM((8, 1, rows), f32),
            pltpu.VMEM((1, rows), f32),
            pltpu.VMEM((16, 1, rows), f32),
            dma((3,)), dma((8,)), dma((8,)), dma((15,)), dma((15,)),
        ],
        compiler_params=pltpu.CompilerParams(collective_id=2, has_side_effects=True),
    )(hidden, queries, around, bias, count, live)


def per_device(
    items_table,
    fetch_rows,
    neighbour_slots,
    neighbour_count,
    self_slot,
    negative_count,
    message_weight,
    message_bias,
    self_weight,
    neighbour_weight,
    output_bias,
    queries,
):
    n_neg, n_qry = lax.axis_size("neg"), lax.axis_size("qry")
    own_neg = lax.axis_index("neg")
    cap = fetch_rows.shape[1]
    negatives, neighbours = neighbour_slots.shape

    assert n_neg * cap < DEAD and neighbours % 4 == 0 and n_neg == SIDE * SIDE and n_qry == 8
    live = jnp.arange(neighbours, dtype=jnp.int32)[None, :] < neighbour_count[:, None]
    slots = jnp.where(live, neighbour_slots, DEAD).T
    half = neighbours // 2
    words = slots[:half] | (slots[half:] << 16)
    lists = jnp.concatenate([words.reshape(-1, LANES), self_slot.reshape(-1, LANES)])
    all_lists, all_fetch = exchange_lists(lists, fetch_rows, items_table.shape[1] // LANES)
    base = (own_neg * cap).astype(jnp.int32).reshape(1)
    counts, lives, own, picked = pick_and_count(
        base, all_fetch.reshape(n_neg * cap), all_lists, items_table, neighbours, cap
    )
    hidden, around = reduce_parts(
        picked, counts, lives, own,
        message_weight, message_bias[None, :], self_weight, neighbour_weight, queries,
    )
    negative_embed, query_lse = embed_and_score(
        hidden, queries, around, output_bias[None, :], negative_count[None, :], neighbour_count[None, :],
        negatives * n_neg * n_qry,
    )
    return (negative_embed, query_lse.reshape(-1))


def solution(mesh):
    in_specs = (
        P("neg", None),
        P(("neg", "qry"), None),
        P(("neg", "qry"), None),
        P(("neg", "qry")),
        P(("neg", "qry")),
        P("neg"),
        P(),
        P(),
        P(),
        P(),
        P(),
        P("qry", None),
    )
    out_specs = (P(("neg", "qry"), None), P("qry"))
    return jax.shard_map(
        per_device, mesh=mesh, in_specs=in_specs, out_specs=out_specs, check_vma=False
    )
```

```python
import functools
import math

import jax
import jax.numpy as jnp
from jax import lax
from jax.experimental import pallas as pl
from jax.experimental.pallas import tpu as pltpu
from jax.sharding import PartitionSpec as P


LANES = 128
ROWS = 128
DEAD = 32767
SIDE = 4
NT = (((1,), (1,)), ((), ()))
SURE = 10
LOG2E = math.log2(math.e)
MESH = pl.DeviceIdType.MESH
ORDER = (
    (2, 2), (2, 1), (2, 3), (1, 2), (3, 2), (2, 0), (0, 2), (1, 1),
    (1, 3), (3, 1), (3, 3), (1, 0), (3, 0), (0, 1), (0, 3), (0, 0),
)


def sort_pairs(count):
    full = 1
    while full < count:
        full *= 2
    pairs = []
    p = 1
    while p < full:
        k = p
        while k >= 1:
            for j in range(k % p, full - k, 2 * k):
                for i in range(min(k, full - j - k)):
                    if (i + j) // (2 * p) == (i + j + k) // (2 * p):
                        if i + j + k < count:
                            pairs.append((i + j, i + j + k))
            k //= 2
        p *= 2
    return pairs


def place():
    neg, qry = lax.axis_index("neg"), lax.axis_index("qry")
    return neg // SIDE, neg % SIDE, qry // 2, qry % 2


def device(x, y, z, core):
    wrap = lambda v: lax.rem(v + 2 * SIDE, SIDE)
    return (wrap(x) * SIDE + wrap(y), wrap(z) * 2 + core)


def remote(src, dst, send, recv, target):
    return pltpu.make_async_remote_copy(
        src_ref=src, dst_ref=dst, send_sem=send, recv_sem=recv,
        device_id=target, device_id_type=MESH,
    )


def greet(peers):
    barrier = pltpu.get_barrier_semaphore()
    for peer in peers:
        pl.semaphore_signal(barrier, inc=1, device_id=peer, device_id_type=MESH)
    pl.semaphore_wait(barrier, len(peers))


def exchange_kernel(
    pieces, slots_ref, count_ref, self_ref, fetch_ref, all_lists, all_fetch,
    lists_ref, asked_ref, sends, recvs,
):
    x, y, z, core = place()
    others = ORDER[:-1]
    neighbours, negatives = slots_ref.shape
    groups, half = negatives // LANES, neighbours // 2
    turn = lax.broadcasted_iota(jnp.int32, slots_ref.shape, 0)
    slots = jnp.where(turn < count_ref[...], slots_ref[...], DEAD)
    words = slots[:half] | (slots[half:] << 16)
    for k in range(half):
        for g in range(groups):
            row = k * groups + g
            lists_ref[row : row + 1, :] = words[k : k + 1, g * LANES : (g + 1) * LANES]
    lists_ref[half * groups :, :] = self_ref[...]
    for p in range(SIDE * SIDE):
        asked_ref[p] = fetch_ref[p : p + 1, :] * pieces
    greet([device(x - dx, y - dy, z, core) for dx, dy in others])
    copies = []
    for j, (dx, dy) in enumerate(others):
        target = device(x - dx, y - dy, z, core)
        copies.append(
            remote(asked_ref.at[target[0]], all_fetch.at[j], sends.at[0, j], recvs.at[0, j], target)
        )
        copies.append(remote(lists_ref, all_lists.at[j], sends.at[1, j], recvs.at[1, j], target))
    for copy in copies:
        copy.start()
    last = len(others)
    all_fetch[last] = asked_ref[x * SIDE + y]
    all_lists[last] = lists_ref[...]
    for copy in copies:
        copy.wait()


def exchange_lists(slots, count, own, fetch, pieces):
    peers, cap = fetch.shape
    neighbours, negatives = slots.shape
    lists = ((neighbours // 2 + 1) * negatives // LANES, LANES)
    vmem = pl.BlockSpec(memory_space=pltpu.VMEM)
    return pl.pallas_call(
        functools.partial(exchange_kernel, pieces),
        out_shape=(
            jax.ShapeDtypeStruct((peers,) + lists, jnp.int32),
            jax.ShapeDtypeStruct((peers, 1, cap), fetch.dtype),
        ),
        in_specs=[vmem, vmem, vmem, vmem],
        out_specs=(vmem, vmem),
        scratch_shapes=[
            pltpu.VMEM(lists, jnp.int32),
            pltpu.VMEM((peers, 1, cap), fetch.dtype),
            pltpu.SemaphoreType.DMA((2, peers - 1)),
            pltpu.SemaphoreType.DMA((2, peers - 1)),
        ],
        compiler_params=pltpu.CompilerParams(collective_id=0, has_side_effects=True),
    )(slots, count, own, fetch)


def count_kernel(
    neighbours, cap, base_ref, index_ref, lists_ref, table_ref,
    counts_ref, own_ref, rows_ref,
    order_ref, times_ref, mine_ref, most_ref, alive_ref, self_ref, wide_ref, picked_ref,
    stage_ref, s_stage,
):
    j = pl.program_id(0)
    rows, width = table_ref.shape
    pieces = width // LANES

    loads, share = stage_ref.shape[0], stage_ref.shape[1]

    def load(i):
        return pltpu.make_async_copy(
            table_ref.at[pl.ds(i * share, share)], stage_ref.at[i], s_stage.at[i]
        )

    @pl.when(j == 0)
    def _():
        for i in range(loads):
            load(i).start()

    groups = counts_ref.shape[2] // LANES
    half = neighbours // 2
    packed = 16
    tall = 8
    batch = tall // groups
    big = jnp.int32(DEAD)

    @pl.when(lax.rem(j, batch) == 0)
    def _():
        base = base_ref[0]
        live = jnp.zeros((tall, LANES), jnp.int32)
        mine = jnp.zeros((tall, LANES), jnp.int32)

        def rows_of(k):
            return jnp.concatenate(
                [lists_ref[i, k * groups : (k + 1) * groups, :] for i in range(batch)]
            )

        words = [rows_of(k) for k in range(half)]
        places = []
        for k in range(neighbours):
            slot = words[k] & DEAD if k < half else words[k - half] >> 16
            local = slot - base
            inside = (local >= 0) & (local < cap)
            live = live + jnp.where(slot < DEAD, 1, 0)
            mine = mine + jnp.where(inside, 1, 0)
            places.append(jnp.where(inside, local, big).astype(jnp.float32))
        for a, b in sort_pairs(neighbours):
            low, high = jnp.minimum(places[a], places[b]), jnp.maximum(places[a], places[b])
            places[a], places[b] = low, high
        rows = pl.ds(pl.multiple_of(j * groups, tall), tall)
        run = jnp.ones((tall, LANES), jnp.float32)
        for k in range(neighbours):
            if k:
                run = jnp.where(places[k] == places[k - 1], run + 1.0, 1.0)
            order_ref[k, rows, :] = places[k].astype(jnp.int32)
            times_ref[k, rows, :] = run
        mine_ref[rows, :] = mine
        for i in range(batch):
            most_ref[j + i] = jnp.max(mine[i * groups : (i + 1) * groups])
        alive_ref[rows, :] = live
        own = rows_of(half) - base
        self_ref[rows, :] = jnp.where((own >= 0) & (own < cap), own, big)

    @pl.when(j == 0)
    def _():
        for i in range(loads):
            load(i).wait()

            @pl.loop(0, share // ROWS)
            def _(t):
                span = pl.ds(pl.multiple_of(t * ROWS, ROWS), ROWS)
                for c in range(pieces):
                    wide_ref[
                        pl.ds((i * share + t * ROWS) * pieces + c, ROWS, stride=pieces), :
                    ] = stage_ref[i, span, c * LANES : (c + 1) * LANES].astype(jnp.float32)

    chunk = 320 if cap % 320 == 0 else ROWS
    tiles = chunk // packed
    tile = (packed, LANES)
    iota = lax.broadcasted_iota(jnp.int32, tile, 0)

    def entry(k, row):
        slot = jnp.broadcast_to(order_ref[k, row, :], tile)
        return slot, jnp.broadcast_to(times_ref[k, row, :], tile).astype(jnp.bfloat16)

    def mark(totals, slot, times, first):
        local = (slot - first).astype(jnp.int16)
        return tuple(
            jnp.where((iota + packed * t).astype(jnp.int16) == local, times, totals[t])
            for t in range(tiles)
        )

    def spans(first):
        return [pl.ds(pl.multiple_of(first + packed * t, packed), packed) for t in range(tiles)]

    for g in range(groups):
        lanes = pl.ds(g * LANES, LANES)
        own_ref[0, 0:1, lanes] = self_ref[pl.ds(j * groups + g, 1), :]
        own_ref[0, 1:2, lanes] = alive_ref[pl.ds(j * groups + g, 1), :]

    parts = cap // chunk
    turns = groups * parts
    part = cap // turns

    burst = part // SURE
    casts = [(p, i) for i in range(part // packed) for p in range(pieces)]

    def cast(buffer, target, p, i):
        rows_ref[
            0,
            pl.ds(pl.multiple_of(target + i * packed, packed), packed),
            p * LANES : (p + 1) * LANES,
        ] = picked_ref[
            buffer, i * packed * pieces + p : (i + 1) * packed * pieces : pieces, :
        ].astype(jnp.bfloat16)

    @pl.loop(0, groups)
    def _(g):
        lanes = pl.ds(pl.multiple_of(g * LANES, LANES), LANES)
        row = pl.ds(j * groups + g, 1)
        for c in range(parts):
            turn = g * parts + c
            first = turn * part
            here, there = c % 2, 1 - c % 2
            before = lax.max(turn - 1, 0) * part
            totals = (jnp.zeros(tile, jnp.bfloat16),) * tiles
            for k in range(SURE):
                places = [
                    pl.multiple_of(index_ref[0, 0, first + k * burst + u], pieces) for u in range(burst)
                ]
                for u in range(burst):
                    into = (k * burst + u) * pieces
                    picked_ref[here, into : into + pieces, :] = wide_ref[pl.ds(places[u], pieces), :]
                totals = mark(totals, *entry(k, row), c * chunk)
                for p, i in casts[k * len(casts) // SURE : (k + 1) * len(casts) // SURE]:
                    cast(there, before, p, i)
            for span, total in zip(spans(c * chunk), totals):
                counts_ref[0, span, lanes] = total

    for p, i in casts:
        cast((turns - 1) % 2, (turns - 1) * part, p, i)

    @pl.when(most_ref[j] > SURE)
    def _():
        for g in range(groups):
            lanes = pl.ds(g * LANES, LANES)
            row = pl.ds(j * groups + g, 1)
            most = jnp.max(mine_ref[row, :])

            @pl.when(most > SURE)
            def _():
                @pl.loop(0, cap // chunk)
                def _(c):
                    totals = tuple(counts_ref[0, span, lanes] for span in spans(c * chunk))
                    totals = lax.fori_loop(
                        SURE, most, lambda k, t: mark(t, *entry(k, row), c * chunk), totals
                    )
                    for span, total in zip(spans(c * chunk), totals):
                        counts_ref[0, span, lanes] = total


def pick_and_count(base, index, lists, table, neighbours, cap):
    peers = lists.shape[0]
    groups = lists.shape[1] // (neighbours // 2 + 1)
    negatives = groups * LANES
    rows = peers * groups
    width = table.shape[1]
    pieces = width // LANES
    return pl.pallas_call(
        functools.partial(count_kernel, neighbours, cap),
        grid=(peers,),
        out_shape=(
            jax.ShapeDtypeStruct((peers, cap, negatives), jnp.bfloat16),
            jax.ShapeDtypeStruct((peers, 2, negatives), jnp.int32),
            jax.ShapeDtypeStruct((peers, cap, width), jnp.bfloat16),
        ),
        in_specs=[
            pl.BlockSpec(memory_space=pltpu.SMEM),
            pl.BlockSpec((1, 1, cap), lambda j: (j, 0, 0), memory_space=pltpu.SMEM),
            pl.BlockSpec((2,) + lists.shape[1:], lambda j: (lax.div(j, 2), 0, 0)),
            pl.BlockSpec(memory_space=pl.ANY),
        ],
        out_specs=(
            pl.BlockSpec((1, cap, negatives), lambda j: (j, 0, 0)),
            pl.BlockSpec((1, 2, negatives), lambda j: (j, 0, 0)),
            pl.BlockSpec((1, cap, width), lambda j: (j, 0, 0)),
        ),
        scratch_shapes=[
            pltpu.VMEM((neighbours, rows, LANES), jnp.int32),
            pltpu.VMEM((neighbours, rows, LANES), jnp.float32),
            pltpu.VMEM((rows, LANES), jnp.int32),
            pltpu.SMEM((peers,), jnp.int32),
            pltpu.VMEM((rows, LANES), jnp.int32),
            pltpu.VMEM((rows, LANES), jnp.int32),
            pltpu.VMEM((table.shape[0] * pieces, LANES), jnp.float32),
            pltpu.VMEM((2, cap * pieces // 8, LANES), jnp.float32),
            pltpu.VMEM((8, table.shape[0] // 8, width), table.dtype),
            pltpu.SemaphoreType.DMA((8,)),
        ],
        compiler_params=pltpu.CompilerParams(vmem_limit_bytes=62 << 20),
    )(base, index, lists, table)


def reduce_kernel(
    rows_ref, counts_ref, own_ref, wm_ref, mb_ref, ws_ref, wn_ref,
    queries_ref, hidden_ref, around_ref,
    hot_ref, message_ref, from_ref, into_ref, total_ref, part_ref,
    relay1, full1, relay2, full2,
    s_relay1, r_relay1, s_full1, r_full1, s_relay2, r_relay2, s_full2, r_full2, s_query, r_query,
):
    step = pl.program_id(0)
    x, y, z, core = place()
    _, cap, width = rows_ref.shape
    negatives = counts_ref.shape[2]
    groups = negatives // LANES
    half, quarter = negatives // 2, negatives // 4
    packed = 16

    def neighbour(axis, sign):
        if axis == 0:
            return device(x + sign, y, z, core)
        return device(x, y + sign, z, core)

    up, down, sibling = device(x, y, z + 1, core), device(x, y, z - 1, core), device(x, y, z, 1 - core)
    upper = pl.ds(0, queries_ref.shape[0] // 2)
    lower = pl.ds(queries_ref.shape[0] // 2, queries_ref.shape[0] // 2)

    def query_copy(which):
        sem = (s_query.at[which], r_query.at[which])
        if which == 0:
            return remote(queries_ref, around_ref.at[6], *sem, up)
        if which == 1:
            return remote(queries_ref, around_ref.at[2], *sem, down)
        if which == 2:
            return remote(queries_ref, around_ref.at[1], *sem, sibling)
        if which == 3:
            return remote(around_ref.at[6, upper], around_ref.at[4, upper], *sem, up)
        if which == 4:
            return remote(around_ref.at[2, lower], around_ref.at[4, lower], *sem, down)
        slot = {5: 6, 6: 2, 7: 4}[which]
        return remote(around_ref.at[slot], around_ref.at[slot + 1], *sem, sibling)

    @pl.when(step == 0)
    def _():
        greet(
            [neighbour(0, 1), neighbour(0, -1), neighbour(1, 1), neighbour(1, -1), up, down, sibling]
        )
        for which in range(3):
            query_copy(which).start()

    @pl.when(step == 10)
    def _():
        for which in (0, 1):
            query_copy(which).wait_recv()
        for which in (3, 4, 5, 6):
            query_copy(which).start()

    @pl.when(step == 15)
    def _():
        for which in (3, 4):
            query_copy(which).wait_recv()
        query_copy(7).start()

    tile = (packed, LANES)
    iota = lax.broadcasted_iota(jnp.int32, tile, 0)
    heres = [(iota + i * packed).astype(jnp.int16) for i in range(cap // packed)]
    zero = jnp.zeros(tile, jnp.bfloat16)
    for g in range(groups):
        lanes = pl.ds(g * LANES, LANES)
        own = jnp.broadcast_to(own_ref[0, 0:1, lanes], tile).astype(jnp.int16)
        live = jnp.broadcast_to(own_ref[0, 1:2, lanes].astype(jnp.float32), tile).astype(jnp.bfloat16)
        for i, here in enumerate(heres):
            hot_ref[i * packed : (i + 1) * packed, lanes] = jnp.where(here == own, live, zero)

    columns = [slice(c, c + width // 2) for c in (0, width // 2)]
    into_ref[:, :cap] = counts_ref[0].T
    into_ref[:, cap:] = hot_ref[...].T

    def dot(a, b):
        return jnp.dot(a, b, preferred_element_type=jnp.float32)

    for s in columns:
        message_ref[:, s] = jax.nn.relu(dot(rows_ref[0], wm_ref[:, s]) + mb_ref[:, s]).astype(
            jnp.bfloat16
        )
        from_ref[cap:, s] = dot(rows_ref[0], ws_ref[:, s]).astype(jnp.bfloat16)
    for s in columns:
        from_ref[:cap, s] = dot(message_ref[...], wn_ref[:, s]).astype(jnp.bfloat16)
    for s in columns:
        total_ref[:, s] = dot(into_ref[...], from_ref[:, s])

    block = 32

    def combine(first, count, sources):
        @pl.loop(0, count // block)
        def _(i):
            span = pl.ds(pl.multiple_of(first + i * block, block), block)
            value = total_ref[span, :]
            for source, begin in sources:
                value = value + source[
                    pl.ds(pl.multiple_of(begin + i * block, block), block), :
                ].astype(jnp.float32)
            total_ref[span, :] = value

    def pack(j, first):
        @pl.loop(0, half // block)
        def _(i):
            span = pl.ds(pl.multiple_of(first + i * block, block), block)
            part_ref[j, span, :] = total_ref[span, :].astype(jnp.bfloat16)

    def relay_copy(j, first, axis, side, relay, send, recv, at):
        return remote(
            part_ref.at[j, pl.ds(first + side * quarter, quarter)],
            relay.at[(*at, side)], send.at[(*at, side)], recv.at[(*at, side)],
            neighbour(axis, 1 - 2 * side),
        )

    def full_copy(j, first, axis, side, full, send, recv, at):
        return remote(
            part_ref.at[j, pl.ds(first, half)],
            full.at[(*at, side)], send.at[(*at, side)], recv.at[(*at, side)],
            neighbour(axis, 1 - 2 * side),
        )

    def ring(j, first, axis, offset, bufs, at):
        relay, full, s_relay, r_relay, s_full, r_full = bufs
        if offset == 2:
            pack(j, first)
            for side in (0, 1):
                relay_copy(j, first, axis, side, relay, s_relay, r_relay, at).start()
        elif offset in (1, 3):
            side = 0 if offset == 1 else 1
            relay_copy(j, first, axis, side, relay, s_relay, r_relay, at).wait_recv()
            combine(first + side * quarter, quarter, [(relay.at[(*at, side)], 0)])
            pack(j, first)
            full_copy(j, first, axis, side, full, s_full, r_full, at).start()
        else:
            for side in (0, 1):
                full_copy(j, first, axis, side, full, s_full, r_full, at).wait_recv()
            combine(first, half, [(full.at[(*at, side)], 0) for side in (0, 1)])

    stage1 = (relay1, full1, s_relay1, r_relay1, s_full1, r_full1)
    stage2 = (relay2, full2, s_relay2, r_relay2, s_full2, r_full2)
    for j, offsets in enumerate(ORDER):

        @pl.when(step == j)
        def _(j=j, offsets=offsets):
            for h in sorted((0, 1), key=lambda h: offsets[h] == 0):
                first = h * half
                near, far = offsets[h], offsets[1 - h]
                ring(j, first, h, near, stage1, (h, far))
                if near == 0:
                    ring(j, first, 1 - h, far, stage2, (h,))

    @pl.when(step == len(ORDER) - 1)
    def _():
        hidden_ref[...] = total_ref[...]
        for j, offsets in enumerate(ORDER):
            for h in (0, 1):
                first = h * half
                near, far = offsets[h], offsets[1 - h]
                stages = [(near, h, stage1, (h, far))]
                if near == 0:
                    stages.append((far, 1 - h, stage2, (h,)))
                for offset, axis, bufs, at in stages:
                    relay, full, s_relay, r_relay, s_full, r_full = bufs
                    if offset == 2:
                        for side in (0, 1):
                            relay_copy(j, first, axis, side, relay, s_relay, r_relay, at).wait_send()
                    elif offset in (1, 3):
                        side = 0 if offset == 1 else 1
                        full_copy(j, first, axis, side, full, s_full, r_full, at).wait_send()
        for which in (2, 5, 6, 7):
            query_copy(which).wait_recv()
        for which in range(8):
            query_copy(which).wait_send()


def reduce_parts(picked, counts, own, wm, mb, ws, wn, queries):
    peers, cap, negatives = counts.shape
    width = picked.shape[2]
    half, quarter = negatives // 2, negatives // 4
    vmem = pl.BlockSpec(memory_space=pltpu.VMEM)
    hbm = pl.BlockSpec(memory_space=pl.ANY)
    dma = pltpu.SemaphoreType.DMA
    bf16, f32 = jnp.bfloat16, jnp.float32
    return pl.pallas_call(
        reduce_kernel,
        grid=(peers,),
        out_shape=(
            jax.ShapeDtypeStruct((negatives, width), f32),
            jax.ShapeDtypeStruct((8,) + queries.shape, queries.dtype),
        ),
        in_specs=[
            pl.BlockSpec((1, cap, width), lambda j: (j, 0, 0)),
            pl.BlockSpec((1, cap, negatives), lambda j: (j, 0, 0)),
            pl.BlockSpec((1, 2, negatives), lambda j: (j, 0, 0)),
            vmem, vmem, vmem, vmem,
            hbm,
        ],
        out_specs=(vmem, hbm),
        scratch_shapes=[
            pltpu.VMEM((cap, negatives), bf16),
            pltpu.VMEM((cap, width), bf16),
            pltpu.VMEM((2 * cap, width), bf16),
            pltpu.VMEM((negatives, 2 * cap), bf16),
            pltpu.VMEM((negatives, width), f32),
            pltpu.VMEM((peers, negatives, width), bf16),
            pltpu.VMEM((2, SIDE, 2, quarter, width), bf16),
            pltpu.VMEM((2, SIDE, 2, half, width), bf16),
            pltpu.VMEM((2, 2, quarter, width), bf16),
            pltpu.VMEM((2, 2, half, width), bf16),
            dma((2, SIDE, 2)), dma((2, SIDE, 2)), dma((2, SIDE, 2)), dma((2, SIDE, 2)),
            dma((2, 2)), dma((2, 2)), dma((2, 2)), dma((2, 2)),
            dma((8,)), dma((8,)),
        ],
        compiler_params=pltpu.CompilerParams(
            collective_id=1, has_side_effects=True, vmem_limit_bytes=62 << 20
        ),
    )(picked, counts, own, wm, mb, ws, wn, queries)


def score_kernel(
    total_negatives, hidden_ref, queries_ref, around_ref, bias_ref, count_ref, live_ref,
    embed_ref, lse_ref,
    log_ref, block_ref, mine_ref, slots_ref, merged_ref, all_ref,
    s_load, s_send1, r_send1, s_send2, r_send2,
):
    x, y, z, core = place()
    others = ORDER[:-1]
    near = [(dz, c) for dz in range(SIDE) for c in (0, 1)][1:]
    greet(
        [device(x, y, z - dz, core if c == 0 else 1 - core) for dz, c in near]
        + [device(x - dx, y - dy, z, core) for dx, dy in others]
    )

    def load(slot):
        buffer = 1 + lax.rem(slot, 2)
        return pltpu.make_async_copy(around_ref.at[slot], block_ref.at[buffer], s_load.at[buffer])

    own_load = pltpu.make_async_copy(queries_ref, block_ref.at[0], s_load.at[0])
    own_load.start()

    load(1).start()
    negatives = hidden_ref.shape[0]

    def column(row_ref):
        row = row_ref[...].astype(jnp.float32)
        return jnp.broadcast_to(row, (LANES, negatives)).T

    mine = pl.ds(pl.multiple_of((2 * z + core) * negatives, negatives), negatives)
    log_ref[...] = LOG2E * jnp.log(column(count_ref.at[:, mine]))
    inverse = 1.0 / column(live_ref)[:, :1]
    hidden = jax.nn.relu(hidden_ref[...] * inverse + bias_ref[...])
    scale = lax.rsqrt(jnp.mean(hidden * hidden, axis=1, keepdims=True) + 0.25)
    embed_ref[...] = (hidden * scale).astype(jnp.bfloat16)
    tile = 256

    def score(slot, ref):
        for t in range(queries_ref.shape[0] // tile):
            span = pl.ds(t * tile, tile)
            product = lax.dot_general(
                embed_ref[...], ref[span, :], NT, preferred_element_type=jnp.float32
            )
            logs = jnp.concatenate([log_ref[...]] * (tile // LANES), axis=1)
            scores = (0.25 * LOG2E) * product - logs
            peak = jnp.max(scores, axis=0, keepdims=True)
            total = jnp.sum(jnp.exp2(scores - peak), axis=0, keepdims=True)
            mine_ref[slot, :, span] = (peak + jnp.log2(total)) * (1 / LOG2E)

    def exchange1(slot):
        dz, c = lax.div(slot, 2), lax.rem(slot, 2)
        return remote(
            mine_ref.at[slot], slots_ref.at[slot], s_send1.at[slot], r_send1.at[slot],
            device(x, y, z + dz, lax.rem(core + c, 2)),
        )

    @pl.loop(0, 8)
    def _(turn):
        slot = lax.rem(turn + 1, 8)

        @pl.when(turn < 6)
        def _():
            load(slot + 1).start()

        @pl.when(turn < 7)
        def _():
            load(slot).wait()

        @pl.when(turn == 7)
        def _():
            own_load.wait()

        score(slot, block_ref.at[lax.select(slot == 0, 0, 1 + lax.rem(slot, 2))])

        @pl.when(turn < 7)
        def _():
            exchange1(slot).start()

    slots_ref[0] = mine_ref[0]
    for slot in range(1, 8):
        exchange1(slot).wait_recv()

    def merge(ref, count):
        values = [ref[i] for i in range(count)]
        top = functools.reduce(jnp.maximum, values)
        return top + jnp.log(sum(jnp.exp(v - top) for v in values))

    merged_ref[...] = merge(slots_ref, 8)

    def exchange2(j):
        dx, dy = others[j]
        return remote(
            merged_ref, all_ref.at[j], s_send2.at[j], r_send2.at[j], device(x - dx, y - dy, z, core)
        )

    for j in range(len(others)):
        exchange2(j).start()
    all_ref[len(others)] = merged_ref[...]
    for j in range(len(others)):
        exchange2(j).wait_recv()
    lse_ref[...] = merge(all_ref, len(others) + 1) - math.log(total_negatives)
    for slot in range(1, 8):
        exchange1(slot).wait_send()
    for j in range(len(others)):
        exchange2(j).wait_send()


def embed_and_score(hidden, queries, around, bias, count, live, total_negatives):
    negatives, width = hidden.shape
    rows = queries.shape[0]
    vmem = pl.BlockSpec(memory_space=pltpu.VMEM)
    hbm = pl.BlockSpec(memory_space=pl.ANY)
    dma = pltpu.SemaphoreType.DMA
    f32 = jnp.float32
    return pl.pallas_call(
        functools.partial(score_kernel, total_negatives),
        out_shape=(
            jax.ShapeDtypeStruct((negatives, width), jnp.bfloat16),
            jax.ShapeDtypeStruct((1, rows), f32),
        ),
        in_specs=[vmem, hbm, hbm, vmem, vmem, vmem],
        out_specs=(vmem, vmem),
        scratch_shapes=[
            pltpu.VMEM((negatives, LANES), f32),
            pltpu.VMEM((3, rows, width), jnp.bfloat16),
            pltpu.VMEM((8, 1, rows), f32),
            pltpu.VMEM((8, 1, rows), f32),
            pltpu.VMEM((1, rows), f32),
            pltpu.VMEM((16, 1, rows), f32),
            dma((3,)), dma((8,)), dma((8,)), dma((15,)), dma((15,)),
        ],
        compiler_params=pltpu.CompilerParams(collective_id=2, has_side_effects=True),
    )(hidden, queries, around, bias, count, live)


def per_device(
    items_table,
    fetch_rows,
    neighbour_slots,
    neighbour_count,
    self_slot,
    negative_count,
    message_weight,
    message_bias,
    self_weight,
    neighbour_weight,
    output_bias,
    queries,
):
    n_neg, n_qry = lax.axis_size("neg"), lax.axis_size("qry")
    own_neg = lax.axis_index("neg")
    cap = fetch_rows.shape[1]
    negatives, neighbours = neighbour_slots.shape

    assert n_neg * cap < DEAD and neighbours % 4 == 0 and n_neg == SIDE * SIDE and n_qry == 8
    all_lists, all_fetch = exchange_lists(
        neighbour_slots.T, neighbour_count[None, :], self_slot.reshape(-1, LANES), fetch_rows,
        items_table.shape[1] // LANES,
    )
    base = (own_neg * cap).astype(jnp.int32).reshape(1)
    counts, own, picked = pick_and_count(
        base, all_fetch, all_lists, items_table, neighbours, cap
    )
    hidden, around = reduce_parts(
        picked, counts, own,
        message_weight, message_bias[None, :], self_weight, neighbour_weight, queries,
    )
    negative_embed, query_lse = embed_and_score(
        hidden, queries, around, output_bias[None, :], negative_count[None, :], neighbour_count[None, :],
        negatives * n_neg * n_qry,
    )
    return (negative_embed, query_lse.reshape(-1))


def solution(mesh):
    in_specs = (
        P("neg", None),
        P(("neg", "qry"), None),
        P(("neg", "qry"), None),
        P(("neg", "qry")),
        P(("neg", "qry")),
        P("neg"),
        P(),
        P(),
        P(),
        P(),
        P(),
        P("qry", None),
    )
    out_specs = (P(("neg", "qry"), None), P("qry"))
    return jax.shard_map(
        per_device, mesh=mesh, in_specs=in_specs, out_specs=out_specs, check_vma=False
    )
```

```python
import functools
import math

import jax
import jax.numpy as jnp
from jax import lax
from jax.experimental import pallas as pl
from jax.experimental.pallas import tpu as pltpu
from jax.sharding import PartitionSpec as P


LANES = 128
ROWS = 128
DEAD = 32767
SIDE = 4
NT = (((1,), (1,)), ((), ()))
SURE = 10
LOG2E = math.log2(math.e)
MESH = pl.DeviceIdType.MESH
ORDER = (
    (2, 2), (2, 1), (2, 3), (1, 2), (3, 2), (2, 0), (0, 2), (1, 1),
    (1, 3), (3, 1), (3, 3), (1, 0), (3, 0), (0, 1), (0, 3), (0, 0),
)

NEAR = tuple((dz, c) for dz in range(SIDE) for c in (0, 1))[1:]


def sort_pairs(count):
    full = 1
    while full < count:
        full *= 2
    pairs = []
    p = 1
    while p < full:
        k = p
        while k >= 1:
            for j in range(k % p, full - k, 2 * k):
                for i in range(min(k, full - j - k)):
                    if (i + j) // (2 * p) == (i + j + k) // (2 * p):
                        if i + j + k < count:
                            pairs.append((i + j, i + j + k))
            k //= 2
        p *= 2
    return pairs


def place():
    neg, qry = lax.axis_index("neg"), lax.axis_index("qry")
    return neg // SIDE, neg % SIDE, qry // 2, qry % 2


def device(x, y, z, core):
    wrap = lambda v: lax.rem(v + 2 * SIDE, SIDE)
    return (wrap(x) * SIDE + wrap(y), wrap(z) * 2 + core)


def remote(src, dst, send, recv, target):
    return pltpu.make_async_remote_copy(
        src_ref=src, dst_ref=dst, send_sem=send, recv_sem=recv,
        device_id=target, device_id_type=MESH,
    )


def greet(peers):
    barrier = pltpu.get_barrier_semaphore()
    for peer in peers:
        pl.semaphore_signal(barrier, inc=1, device_id=peer, device_id_type=MESH)
    pl.semaphore_wait(barrier, len(peers))


def exchange_kernel(
    pieces, slots_ref, count_ref, self_ref, fetch_ref, all_lists, all_fetch,
    lists_ref, asked_ref, sends, recvs,
):
    x, y, z, core = place()
    others = ORDER[:-1]
    neighbours, negatives = slots_ref.shape
    groups, half = negatives // LANES, neighbours // 2
    turn = lax.broadcasted_iota(jnp.int32, slots_ref.shape, 0)
    slots = jnp.where(turn < count_ref[...], slots_ref[...], DEAD)
    words = slots[:half] | (slots[half:] << 16)
    for k in range(half):
        for g in range(groups):
            row = k * groups + g
            lists_ref[row : row + 1, :] = words[k : k + 1, g * LANES : (g + 1) * LANES]
    lists_ref[half * groups :, :] = self_ref[...]
    for p in range(SIDE * SIDE):
        asked_ref[p] = fetch_ref[p : p + 1, :] * pieces
    greet([device(x - dx, y - dy, z, core) for dx, dy in others])
    copies = []
    for j, (dx, dy) in enumerate(others):
        target = device(x - dx, y - dy, z, core)
        copies.append(
            remote(asked_ref.at[target[0]], all_fetch.at[j], sends.at[0, j], recvs.at[0, j], target)
        )
        copies.append(remote(lists_ref, all_lists.at[j], sends.at[1, j], recvs.at[1, j], target))
    for copy in copies:
        copy.start()
    last = len(others)
    all_fetch[last] = asked_ref[x * SIDE + y]
    all_lists[last] = lists_ref[...]
    for copy in copies:
        copy.wait()


def exchange_lists(slots, count, own, fetch, pieces):
    peers, cap = fetch.shape
    neighbours, negatives = slots.shape
    lists = ((neighbours // 2 + 1) * negatives // LANES, LANES)
    vmem = pl.BlockSpec(memory_space=pltpu.VMEM)
    return pl.pallas_call(
        functools.partial(exchange_kernel, pieces),
        out_shape=(
            jax.ShapeDtypeStruct((peers,) + lists, jnp.int32),
            jax.ShapeDtypeStruct((peers, 1, cap), fetch.dtype),
        ),
        in_specs=[vmem, vmem, vmem, vmem],
        out_specs=(vmem, vmem),
        scratch_shapes=[
            pltpu.VMEM(lists, jnp.int32),
            pltpu.VMEM((peers, 1, cap), fetch.dtype),
            pltpu.SemaphoreType.DMA((2, peers - 1)),
            pltpu.SemaphoreType.DMA((2, peers - 1)),
        ],
        compiler_params=pltpu.CompilerParams(collective_id=0, has_side_effects=True),
    )(slots, count, own, fetch)


def count_kernel(
    neighbours, cap, base_ref, index_ref, lists_ref, table_ref,
    counts_ref, own_ref, rows_ref,
    order_ref, times_ref, mine_ref, most_ref, alive_ref, self_ref, wide_ref, picked_ref,
    stage_ref, s_stage,
):
    j = pl.program_id(0)
    rows, width = table_ref.shape
    pieces = width // LANES

    loads, share = stage_ref.shape[0], stage_ref.shape[1]

    def load(i):
        return pltpu.make_async_copy(
            table_ref.at[pl.ds(i * share, share)], stage_ref.at[i], s_stage.at[i]
        )

    @pl.when(j == 0)
    def _():
        for i in range(loads):
            load(i).start()

    groups = counts_ref.shape[2] // LANES
    half = neighbours // 2
    packed = 16
    tall = 8
    batch = tall // groups
    big = jnp.int32(DEAD)

    @pl.when(lax.rem(j, batch) == 0)
    def _():
        base = base_ref[0]
        live = jnp.zeros((tall, LANES), jnp.int32)
        mine = jnp.zeros((tall, LANES), jnp.int32)

        def rows_of(k):
            return jnp.concatenate(
                [lists_ref[i, k * groups : (k + 1) * groups, :] for i in range(batch)]
            )

        words = [rows_of(k) for k in range(half)]
        places = []
        for k in range(neighbours):
            slot = words[k] & DEAD if k < half else words[k - half] >> 16
            local = slot - base
            inside = (local >= 0) & (local < cap)
            live = live + jnp.where(slot < DEAD, 1, 0)
            mine = mine + jnp.where(inside, 1, 0)
            places.append(jnp.where(inside, local, big).astype(jnp.float32))
        for a, b in sort_pairs(neighbours):
            low, high = jnp.minimum(places[a], places[b]), jnp.maximum(places[a], places[b])
            places[a], places[b] = low, high
        rows = pl.ds(pl.multiple_of(j * groups, tall), tall)
        run = jnp.ones((tall, LANES), jnp.float32)
        for k in range(neighbours):
            if k:
                run = jnp.where(places[k] == places[k - 1], run + 1.0, 1.0)
            order_ref[k, rows, :] = places[k].astype(jnp.int32)
            times_ref[k, rows, :] = run
        mine_ref[rows, :] = mine
        for i in range(batch):
            most_ref[j + i] = jnp.max(mine[i * groups : (i + 1) * groups])
        alive_ref[rows, :] = live
        own = rows_of(half) - base
        self_ref[rows, :] = jnp.where((own >= 0) & (own < cap), own, big)

    @pl.when(j == 0)
    def _():
        for i in range(loads):
            load(i).wait()

            @pl.loop(0, share // ROWS)
            def _(t):
                span = pl.ds(pl.multiple_of(t * ROWS, ROWS), ROWS)
                for c in range(pieces):
                    wide_ref[
                        pl.ds((i * share + t * ROWS) * pieces + c, ROWS, stride=pieces), :
                    ] = stage_ref[i, span, c * LANES : (c + 1) * LANES].astype(jnp.float32)

    chunk = 320 if cap % 320 == 0 else ROWS
    tiles = chunk // packed
    tile = (packed, LANES)
    iota = lax.broadcasted_iota(jnp.int32, tile, 0)

    def entry(k, row):
        slot = jnp.broadcast_to(order_ref[k, row, :], tile)
        return slot, jnp.broadcast_to(times_ref[k, row, :], tile).astype(jnp.bfloat16)

    def mark(totals, slot, times, first):
        local = (slot - first).astype(jnp.int16)
        return tuple(
            jnp.where((iota + packed * t).astype(jnp.int16) == local, times, totals[t])
            for t in range(tiles)
        )

    def spans(first):
        return [pl.ds(pl.multiple_of(first + packed * t, packed), packed) for t in range(tiles)]

    for g in range(groups):
        lanes = pl.ds(g * LANES, LANES)
        own_ref[0, 0:1, lanes] = self_ref[pl.ds(j * groups + g, 1), :]
        own_ref[0, 1:2, lanes] = alive_ref[pl.ds(j * groups + g, 1), :]

    parts = cap // chunk
    turns = groups * parts
    part = cap // turns

    burst = part // SURE
    casts = [(p, i) for i in range(part // packed) for p in range(pieces)]

    def cast(buffer, target, p, i):
        rows_ref[
            0,
            pl.ds(pl.multiple_of(target + i * packed, packed), packed),
            p * LANES : (p + 1) * LANES,
        ] = picked_ref[
            buffer, i * packed * pieces + p : (i + 1) * packed * pieces : pieces, :
        ].astype(jnp.bfloat16)

    @pl.loop(0, groups)
    def _(g):
        lanes = pl.ds(pl.multiple_of(g * LANES, LANES), LANES)
        row = pl.ds(j * groups + g, 1)
        for c in range(parts):
            turn = g * parts + c
            first = turn * part
            here, there = c % 2, 1 - c % 2
            before = lax.max(turn - 1, 0) * part
            totals = (jnp.zeros(tile, jnp.bfloat16),) * tiles
            for k in range(SURE):
                places = [
                    pl.multiple_of(index_ref[0, 0, first + k * burst + u], pieces) for u in range(burst)
                ]
                for u in range(burst):
                    into = (k * burst + u) * pieces
                    picked_ref[here, into : into + pieces, :] = wide_ref[pl.ds(places[u], pieces), :]
                totals = mark(totals, *entry(k, row), c * chunk)
                for p, i in casts[k * len(casts) // SURE : (k + 1) * len(casts) // SURE]:
                    cast(there, before, p, i)
            for span, total in zip(spans(c * chunk), totals):
                counts_ref[0, span, lanes] = total

    for p, i in casts:
        cast((turns - 1) % 2, (turns - 1) * part, p, i)

    @pl.when(most_ref[j] > SURE)
    def _():
        for g in range(groups):
            lanes = pl.ds(g * LANES, LANES)
            row = pl.ds(j * groups + g, 1)
            most = jnp.max(mine_ref[row, :])

            @pl.when(most > SURE)
            def _():
                @pl.loop(0, cap // chunk)
                def _(c):
                    totals = tuple(counts_ref[0, span, lanes] for span in spans(c * chunk))
                    totals = lax.fori_loop(
                        SURE, most, lambda k, t: mark(t, *entry(k, row), c * chunk), totals
                    )
                    for span, total in zip(spans(c * chunk), totals):
                        counts_ref[0, span, lanes] = total


def pick_and_count(base, index, lists, table, neighbours, cap):
    peers = lists.shape[0]
    groups = lists.shape[1] // (neighbours // 2 + 1)
    negatives = groups * LANES
    rows = peers * groups
    width = table.shape[1]
    pieces = width // LANES
    return pl.pallas_call(
        functools.partial(count_kernel, neighbours, cap),
        grid=(peers,),
        out_shape=(
            jax.ShapeDtypeStruct((peers, cap, negatives), jnp.bfloat16),
            jax.ShapeDtypeStruct((peers, 2, negatives), jnp.int32),
            jax.ShapeDtypeStruct((peers, cap, width), jnp.bfloat16),
        ),
        in_specs=[
            pl.BlockSpec(memory_space=pltpu.SMEM),
            pl.BlockSpec((1, 1, cap), lambda j: (j, 0, 0), memory_space=pltpu.SMEM),
            pl.BlockSpec((2,) + lists.shape[1:], lambda j: (lax.div(j, 2), 0, 0)),
            pl.BlockSpec(memory_space=pl.ANY),
        ],
        out_specs=(
            pl.BlockSpec((1, cap, negatives), lambda j: (j, 0, 0)),
            pl.BlockSpec((1, 2, negatives), lambda j: (j, 0, 0)),
            pl.BlockSpec((1, cap, width), lambda j: (j, 0, 0)),
        ),
        scratch_shapes=[
            pltpu.VMEM((neighbours, rows, LANES), jnp.int32),
            pltpu.VMEM((neighbours, rows, LANES), jnp.float32),
            pltpu.VMEM((rows, LANES), jnp.int32),
            pltpu.SMEM((peers,), jnp.int32),
            pltpu.VMEM((rows, LANES), jnp.int32),
            pltpu.VMEM((rows, LANES), jnp.int32),
            pltpu.VMEM((table.shape[0] * pieces, LANES), jnp.float32),
            pltpu.VMEM((2, cap * pieces // 8, LANES), jnp.float32),
            pltpu.VMEM((8, table.shape[0] // 8, width), table.dtype),
            pltpu.SemaphoreType.DMA((8,)),
        ],
        compiler_params=pltpu.CompilerParams(vmem_limit_bytes=62 << 20),
    )(base, index, lists, table)


def score_all(
    total_negatives, hidden_ref, around_ref, bias_ref, count_ref, live_ref,
    embed_ref, lse_ref,
    log_ref, mine_ref, slots_ref, merged_ref, all_ref,
    s_send1, r_send1, s_send2, r_send2,
):
    x, y, z, core = place()
    others = ORDER[:-1]
    negatives = hidden_ref.shape[0]

    def column(row_ref):
        row = row_ref[...].astype(jnp.float32)
        return jnp.broadcast_to(row, (LANES, negatives)).T

    mine = pl.ds(pl.multiple_of((2 * z + core) * negatives, negatives), negatives)
    log_ref[...] = LOG2E * jnp.log(column(count_ref.at[:, mine]))
    inverse = 1.0 / column(live_ref)[:, :1]
    hidden = jax.nn.relu(hidden_ref[...] * inverse + bias_ref[...])
    scale = lax.rsqrt(jnp.mean(hidden * hidden, axis=1, keepdims=True) + 0.25)
    embed_ref[...] = (hidden * scale).astype(jnp.bfloat16)
    tile = 256

    def score(slot, ref):
        for t in range(around_ref.shape[1] // tile):
            span = pl.ds(t * tile, tile)
            product = lax.dot_general(
                embed_ref[...], ref[span, :], NT, preferred_element_type=jnp.float32
            )
            logs = jnp.concatenate([log_ref[...]] * (tile // LANES), axis=1)
            scores = (0.25 * LOG2E) * product - logs
            peak = jnp.max(scores, axis=0, keepdims=True)
            total = jnp.sum(jnp.exp2(scores - peak), axis=0, keepdims=True)
            mine_ref[slot, :, span] = (peak + jnp.log2(total)) * (1 / LOG2E)

    def exchange1(slot):
        dz, c = lax.div(slot, 2), lax.rem(slot, 2)
        return remote(
            mine_ref.at[slot], slots_ref.at[slot], s_send1.at[slot], r_send1.at[slot],
            device(x, y, z + dz, lax.rem(core + c, 2)),
        )

    @pl.loop(0, 8)
    def _(turn):
        slot = lax.rem(turn + 1, 8)

        score(slot, around_ref.at[slot])

        @pl.when(turn < 7)
        def _():
            exchange1(slot).start()

    slots_ref[0] = mine_ref[0]
    for slot in range(1, 8):
        exchange1(slot).wait_recv()

    def merge(ref, count):
        values = [ref[i] for i in range(count)]
        top = functools.reduce(jnp.maximum, values)
        return top + jnp.log(sum(jnp.exp(v - top) for v in values))

    merged_ref[...] = merge(slots_ref, 8)

    def exchange2(j):
        dx, dy = others[j]
        return remote(
            merged_ref, all_ref.at[j], s_send2.at[j], r_send2.at[j], device(x - dx, y - dy, z, core)
        )

    for j in range(len(others)):
        exchange2(j).start()
    all_ref[len(others)] = merged_ref[...]
    for j in range(len(others)):
        exchange2(j).wait_recv()
    lse_ref[...] = merge(all_ref, len(others) + 1) - math.log(total_negatives)
    for slot in range(1, 8):
        exchange1(slot).wait_send()
    for j in range(len(others)):
        exchange2(j).wait_send()


def reduce_kernel(
    total_negatives,
    rows_ref, counts_ref, own_ref, wm_ref, mb_ref, ws_ref, wn_ref,
    queries_ref, bias_ref, count_ref, live_ref, embed_ref, lse_ref,
    around_ref, hot_ref, message_ref, from_ref, into_ref, total_ref, part_ref,
    relay1, full1, relay2, full2,
    s_relay1, r_relay1, s_full1, r_full1, s_relay2, r_relay2, s_full2, r_full2,
    s_query, r_query, s_own,
    *score_refs,
):
    step = pl.program_id(0)
    x, y, z, core = place()
    _, cap, width = rows_ref.shape
    negatives = counts_ref.shape[2]
    groups = negatives // LANES
    half, quarter = negatives // 2, negatives // 4
    packed = 16

    def neighbour(axis, sign):
        if axis == 0:
            return device(x + sign, y, z, core)
        return device(x, y + sign, z, core)

    up, down, sibling = device(x, y, z + 1, core), device(x, y, z - 1, core), device(x, y, z, 1 - core)
    upper = pl.ds(0, queries_ref.shape[0] // 2)
    lower = pl.ds(queries_ref.shape[0] // 2, queries_ref.shape[0] // 2)

    def query_copy(which):
        sem = (s_query.at[which], r_query.at[which])
        if which == 0:
            return remote(queries_ref, around_ref.at[6], *sem, up)
        if which == 1:
            return remote(queries_ref, around_ref.at[2], *sem, down)
        if which == 2:
            return remote(queries_ref, around_ref.at[1], *sem, sibling)
        if which == 3:
            return remote(around_ref.at[6, upper], around_ref.at[4, upper], *sem, up)
        if which == 4:
            return remote(around_ref.at[2, lower], around_ref.at[4, lower], *sem, down)
        slot = {5: 6, 6: 2, 7: 4}[which]
        return remote(around_ref.at[slot], around_ref.at[slot + 1], *sem, sibling)

    @pl.when(step == 0)
    def _():
        greet(
            [device(x, y, z - dz, lax.rem(core + c, 2)) for dz, c in NEAR]
            + [device(x - dx, y - dy, z, core) for dx, dy in ORDER[:-1]]
        )
        for which in range(3):
            query_copy(which).start()
        pltpu.make_async_copy(queries_ref, around_ref.at[0], s_own).start()

    @pl.when(step == 10)
    def _():
        for which in (0, 1):
            query_copy(which).wait_recv()
        for which in (3, 4, 5, 6):
            query_copy(which).start()

    @pl.when(step == 15)
    def _():
        for which in (3, 4):
            query_copy(which).wait_recv()
        query_copy(7).start()

    tile = (packed, LANES)
    iota = lax.broadcasted_iota(jnp.int32, tile, 0)
    heres = [(iota + i * packed).astype(jnp.int16) for i in range(cap // packed)]
    zero = jnp.zeros(tile, jnp.bfloat16)
    for g in range(groups):
        lanes = pl.ds(g * LANES, LANES)
        own = jnp.broadcast_to(own_ref[0, 0:1, lanes], tile).astype(jnp.int16)
        live = jnp.broadcast_to(own_ref[0, 1:2, lanes].astype(jnp.float32), tile).astype(jnp.bfloat16)
        for i, here in enumerate(heres):
            hot_ref[i * packed : (i + 1) * packed, lanes] = jnp.where(here == own, live, zero)

    columns = [slice(c, c + width // 2) for c in (0, width // 2)]
    into_ref[:, :cap] = counts_ref[0].T
    into_ref[:, cap:] = hot_ref[...].T

    def dot(a, b):
        return jnp.dot(a, b, preferred_element_type=jnp.float32)

    for s in columns:
        message_ref[:, s] = jax.nn.relu(dot(rows_ref[0], wm_ref[:, s]) + mb_ref[:, s]).astype(
            jnp.bfloat16
        )
        from_ref[cap:, s] = dot(rows_ref[0], ws_ref[:, s]).astype(jnp.bfloat16)
    for s in columns:
        from_ref[:cap, s] = dot(message_ref[...], wn_ref[:, s]).astype(jnp.bfloat16)
    for s in columns:
        total_ref[:, s] = dot(into_ref[...], from_ref[:, s])

    block = 32

    def combine(first, count, sources):
        @pl.loop(0, count // block)
        def _(i):
            span = pl.ds(pl.multiple_of(first + i * block, block), block)
            value = total_ref[span, :]
            for source, begin in sources:
                value = value + source[
                    pl.ds(pl.multiple_of(begin + i * block, block), block), :
                ].astype(jnp.float32)
            total_ref[span, :] = value

    def pack(j, first):
        @pl.loop(0, half // block)
        def _(i):
            span = pl.ds(pl.multiple_of(first + i * block, block), block)
            part_ref[j, span, :] = total_ref[span, :].astype(jnp.bfloat16)

    def relay_copy(j, first, axis, side, relay, send, recv, at):
        return remote(
            part_ref.at[j, pl.ds(first + side * quarter, quarter)],
            relay.at[(*at, side)], send.at[(*at, side)], recv.at[(*at, side)],
            neighbour(axis, 1 - 2 * side),
        )

    def full_copy(j, first, axis, side, full, send, recv, at):
        return remote(
            part_ref.at[j, pl.ds(first, half)],
            full.at[(*at, side)], send.at[(*at, side)], recv.at[(*at, side)],
            neighbour(axis, 1 - 2 * side),
        )

    def ring(j, first, axis, offset, bufs, at):
        relay, full, s_relay, r_relay, s_full, r_full = bufs
        if offset == 2:
            pack(j, first)
            for side in (0, 1):
                relay_copy(j, first, axis, side, relay, s_relay, r_relay, at).start()
        elif offset in (1, 3):
            side = 0 if offset == 1 else 1
            relay_copy(j, first, axis, side, relay, s_relay, r_relay, at).wait_recv()
            combine(first + side * quarter, quarter, [(relay.at[(*at, side)], 0)])
            pack(j, first)
            full_copy(j, first, axis, side, full, s_full, r_full, at).start()
        else:
            for side in (0, 1):
                full_copy(j, first, axis, side, full, s_full, r_full, at).wait_recv()
            combine(first, half, [(full.at[(*at, side)], 0) for side in (0, 1)])

    stage1 = (relay1, full1, s_relay1, r_relay1, s_full1, r_full1)
    stage2 = (relay2, full2, s_relay2, r_relay2, s_full2, r_full2)
    for j, offsets in enumerate(ORDER):

        @pl.when(step == j)
        def _(j=j, offsets=offsets):
            for h in sorted((0, 1), key=lambda h: offsets[h] == 0):
                first = h * half
                near, far = offsets[h], offsets[1 - h]
                ring(j, first, h, near, stage1, (h, far))
                if near == 0:
                    ring(j, first, 1 - h, far, stage2, (h,))

    @pl.when(step == len(ORDER) - 1)
    def _():
        for which in (2, 5, 6, 7):
            query_copy(which).wait_recv()
        pltpu.make_async_copy(queries_ref, around_ref.at[0], s_own).wait()
        score_all(
            total_negatives, total_ref, around_ref, bias_ref, count_ref, live_ref,
            embed_ref, lse_ref, *score_refs,
        )
        for j, offsets in enumerate(ORDER):
            for h in (0, 1):
                first = h * half
                near, far = offsets[h], offsets[1 - h]
                stages = [(near, h, stage1, (h, far))]
                if near == 0:
                    stages.append((far, 1 - h, stage2, (h,)))
                for offset, axis, bufs, at in stages:
                    relay, full, s_relay, r_relay, s_full, r_full = bufs
                    if offset == 2:
                        for side in (0, 1):
                            relay_copy(j, first, axis, side, relay, s_relay, r_relay, at).wait_send()
                    elif offset in (1, 3):
                        side = 0 if offset == 1 else 1
                        full_copy(j, first, axis, side, full, s_full, r_full, at).wait_send()
        for which in range(8):
            query_copy(which).wait_send()


def reduce_and_score(
    picked, counts, own, wm, mb, ws, wn, queries, bias, count, live, total_negatives
):
    peers, cap, negatives = counts.shape
    width = picked.shape[2]
    half, quarter = negatives // 2, negatives // 4
    vmem = pl.BlockSpec(memory_space=pltpu.VMEM)
    hbm = pl.BlockSpec(memory_space=pl.ANY)
    dma = pltpu.SemaphoreType.DMA
    bf16, f32 = jnp.bfloat16, jnp.float32
    return pl.pallas_call(
        functools.partial(reduce_kernel, total_negatives),
        grid=(peers,),
        out_shape=(
            jax.ShapeDtypeStruct((negatives, width), bf16),
            jax.ShapeDtypeStruct((1, queries.shape[0]), f32),
        ),
        in_specs=[
            pl.BlockSpec((1, cap, width), lambda j: (j, 0, 0)),
            pl.BlockSpec((1, cap, negatives), lambda j: (j, 0, 0)),
            pl.BlockSpec((1, 2, negatives), lambda j: (j, 0, 0)),
            vmem, vmem, vmem, vmem,
            hbm, vmem, vmem, vmem,
        ],
        out_specs=(vmem, vmem),
        scratch_shapes=[
            pltpu.VMEM((8,) + queries.shape, bf16),
            pltpu.VMEM((cap, negatives), bf16),
            pltpu.VMEM((cap, width), bf16),
            pltpu.VMEM((2 * cap, width), bf16),
            pltpu.VMEM((negatives, 2 * cap), bf16),
            pltpu.VMEM((negatives, width), f32),
            pltpu.VMEM((peers, negatives, width), bf16),
            pltpu.VMEM((2, SIDE, 2, quarter, width), bf16),
            pltpu.VMEM((2, SIDE, 2, half, width), bf16),
            pltpu.VMEM((2, 2, quarter, width), bf16),
            pltpu.VMEM((2, 2, half, width), bf16),
            dma((2, SIDE, 2)), dma((2, SIDE, 2)), dma((2, SIDE, 2)), dma((2, SIDE, 2)),
            dma((2, 2)), dma((2, 2)), dma((2, 2)), dma((2, 2)),
            dma((8,)), dma((8,)), dma,
            pltpu.VMEM((negatives, LANES), f32),
            pltpu.VMEM((8, 1, queries.shape[0]), f32),
            pltpu.VMEM((8, 1, queries.shape[0]), f32),
            pltpu.VMEM((1, queries.shape[0]), f32),
            pltpu.VMEM((peers, 1, queries.shape[0]), f32),
            dma((8,)), dma((8,)), dma((15,)), dma((15,)),
        ],
        compiler_params=pltpu.CompilerParams(
            collective_id=1, has_side_effects=True, vmem_limit_bytes=62 << 20
        ),
    )(picked, counts, own, wm, mb, ws, wn, queries, bias, count, live)


def per_device(
    items_table,
    fetch_rows,
    neighbour_slots,
    neighbour_count,
    self_slot,
    negative_count,
    message_weight,
    message_bias,
    self_weight,
    neighbour_weight,
    output_bias,
    queries,
):
    n_neg, n_qry = lax.axis_size("neg"), lax.axis_size("qry")
    own_neg = lax.axis_index("neg")
    cap = fetch_rows.shape[1]
    negatives, neighbours = neighbour_slots.shape

    assert n_neg * cap < DEAD and neighbours % 4 == 0 and n_neg == SIDE * SIDE and n_qry == 8
    all_lists, all_fetch = exchange_lists(
        neighbour_slots.T, neighbour_count[None, :], self_slot.reshape(-1, LANES), fetch_rows,
        items_table.shape[1] // LANES,
    )
    base = (own_neg * cap).astype(jnp.int32).reshape(1)
    counts, own, picked = pick_and_count(
        base, all_fetch, all_lists, items_table, neighbours, cap
    )
    negative_embed, query_lse = reduce_and_score(
        picked, counts, own,
        message_weight, message_bias[None, :], self_weight, neighbour_weight, queries,
        output_bias[None, :], negative_count[None, :], neighbour_count[None, :],
        negatives * n_neg * n_qry,
    )
    return (negative_embed, query_lse.reshape(-1))


def solution(mesh):
    in_specs = (
        P("neg", None),
        P(("neg", "qry"), None),
        P(("neg", "qry"), None),
        P(("neg", "qry")),
        P(("neg", "qry")),
        P("neg"),
        P(),
        P(),
        P(),
        P(),
        P(),
        P("qry", None),
    )
    out_specs = (P(("neg", "qry"), None), P("qry"))
    return jax.shard_map(
        per_device, mesh=mesh, in_specs=in_specs, out_specs=out_specs, check_vma=False
    )
```

```python
import functools
import math

import jax
import jax.numpy as jnp
from jax import lax
from jax.experimental import pallas as pl
from jax.experimental.pallas import tpu as pltpu
from jax.sharding import PartitionSpec as P


LANES = 128
ROWS = 128
DEAD = 32767
SIDE = 4
NT = (((1,), (1,)), ((), ()))
SURE = 10
LOG2E = math.log2(math.e)
MESH = pl.DeviceIdType.MESH
ORDER = (
    (2, 2), (2, 1), (2, 3), (1, 2), (3, 2), (2, 0), (0, 2), (1, 1),
    (1, 3), (3, 1), (3, 3), (1, 0), (3, 0), (0, 1), (0, 3), (0, 0),
)

NEAR = tuple((dz, c) for dz in range(SIDE) for c in (0, 1))[1:]


def sort_pairs(count):
    full = 1
    while full < count:
        full *= 2
    pairs = []
    p = 1
    while p < full:
        k = p
        while k >= 1:
            for j in range(k % p, full - k, 2 * k):
                for i in range(min(k, full - j - k)):
                    if (i + j) // (2 * p) == (i + j + k) // (2 * p):
                        if i + j + k < count:
                            pairs.append((i + j, i + j + k))
            k //= 2
        p *= 2
    return pairs


def place():
    neg, qry = lax.axis_index("neg"), lax.axis_index("qry")
    return neg // SIDE, neg % SIDE, qry // 2, qry % 2


def device(x, y, z, core):
    wrap = lambda v: lax.rem(v + 2 * SIDE, SIDE)
    return (wrap(x) * SIDE + wrap(y), wrap(z) * 2 + core)


def remote(src, dst, send, recv, target):
    return pltpu.make_async_remote_copy(
        src_ref=src, dst_ref=dst, send_sem=send, recv_sem=recv,
        device_id=target, device_id_type=MESH,
    )


def greet(peers):
    barrier = pltpu.get_barrier_semaphore()
    for peer in peers:
        pl.semaphore_signal(barrier, inc=1, device_id=peer, device_id_type=MESH)
    pl.semaphore_wait(barrier, len(peers))


def exchange_kernel(
    pieces, slots_ref, count_ref, self_ref, fetch_ref, all_lists, all_fetch,
    lists_ref, asked_ref, sends, recvs,
):
    x, y, z, core = place()
    others = ORDER[:-1]
    neighbours, negatives = slots_ref.shape
    groups, half = negatives // LANES, neighbours // 2
    turn = lax.broadcasted_iota(jnp.int32, slots_ref.shape, 0)
    slots = jnp.where(turn < count_ref[...], slots_ref[...], DEAD)
    words = slots[:half] | (slots[half:] << 16)
    for k in range(half):
        for g in range(groups):
            row = k * groups + g
            lists_ref[row : row + 1, :] = words[k : k + 1, g * LANES : (g + 1) * LANES]
    lists_ref[half * groups :, :] = self_ref[...]
    for p in range(SIDE * SIDE):
        asked_ref[p] = fetch_ref[p : p + 1, :] * pieces
    greet([device(x - dx, y - dy, z, core) for dx, dy in others])
    copies = []
    for j, (dx, dy) in enumerate(others):
        target = device(x - dx, y - dy, z, core)
        copies.append(
            remote(asked_ref.at[target[0]], all_fetch.at[j], sends.at[0, j], recvs.at[0, j], target)
        )
        copies.append(remote(lists_ref, all_lists.at[j], sends.at[1, j], recvs.at[1, j], target))
    for copy in copies:
        copy.start()
    last = len(others)
    all_fetch[last] = asked_ref[x * SIDE + y]
    all_lists[last] = lists_ref[...]
    for copy in copies:
        copy.wait()


def exchange_lists(slots, count, own, fetch, pieces):
    peers, cap = fetch.shape
    neighbours, negatives = slots.shape
    lists = ((neighbours // 2 + 1) * negatives // LANES, LANES)
    vmem = pl.BlockSpec(memory_space=pltpu.VMEM)
    return pl.pallas_call(
        functools.partial(exchange_kernel, pieces),
        out_shape=(
            jax.ShapeDtypeStruct((peers,) + lists, jnp.int32),
            jax.ShapeDtypeStruct((peers, 1, cap), fetch.dtype),
        ),
        in_specs=[vmem, vmem, vmem, vmem],
        out_specs=(vmem, vmem),
        scratch_shapes=[
            pltpu.VMEM(lists, jnp.int32),
            pltpu.VMEM((peers, 1, cap), fetch.dtype),
            pltpu.SemaphoreType.DMA((2, peers - 1)),
            pltpu.SemaphoreType.DMA((2, peers - 1)),
        ],
        compiler_params=pltpu.CompilerParams(collective_id=0, has_side_effects=True),
    )(slots, count, own, fetch)


def count_kernel(
    neighbours, cap, base_ref, index_ref, lists_ref, table_ref,
    counts_ref, own_ref, rows_ref,
    order_ref, times_ref, mine_ref, most_ref, alive_ref, self_ref, wide_ref, picked_ref,
    stage_ref, s_stage,
):
    j = pl.program_id(0)
    rows, width = table_ref.shape
    pieces = width // LANES

    loads, share = stage_ref.shape[0], stage_ref.shape[1]

    def load(i):
        return pltpu.make_async_copy(
            table_ref.at[pl.ds(i * share, share)], stage_ref.at[i], s_stage.at[i]
        )

    @pl.when(j == 0)
    def _():
        for i in range(loads):
            load(i).start()

    groups = counts_ref.shape[2] // LANES
    half = neighbours // 2
    packed = 16
    tall = 8
    batch = tall // groups
    big = jnp.int32(DEAD)

    @pl.when(lax.rem(j, batch) == 0)
    def _():
        base = base_ref[0]
        live = jnp.zeros((tall, LANES), jnp.int32)
        mine = jnp.zeros((tall, LANES), jnp.int32)

        def rows_of(k):
            return jnp.concatenate(
                [lists_ref[i, k * groups : (k + 1) * groups, :] for i in range(batch)]
            )

        words = [rows_of(k) for k in range(half)]
        places = []
        for k in range(neighbours):
            slot = words[k] & DEAD if k < half else words[k - half] >> 16
            local = slot - base
            inside = (local >= 0) & (local < cap)
            live = live + jnp.where(slot < DEAD, 1, 0)
            mine = mine + jnp.where(inside, 1, 0)
            places.append(jnp.where(inside, local, big).astype(jnp.float32))
        for a, b in sort_pairs(neighbours):
            low, high = jnp.minimum(places[a], places[b]), jnp.maximum(places[a], places[b])
            places[a], places[b] = low, high
        rows = pl.ds(pl.multiple_of(j * groups, tall), tall)
        run = jnp.ones((tall, LANES), jnp.float32)
        for k in range(neighbours):
            if k:
                run = jnp.where(places[k] == places[k - 1], run + 1.0, 1.0)
            order_ref[k, rows, :] = places[k].astype(jnp.int32)
            times_ref[k, rows, :] = run
        mine_ref[rows, :] = mine
        for i in range(batch):
            most_ref[j + i] = jnp.max(mine[i * groups : (i + 1) * groups])
        alive_ref[rows, :] = live
        own = rows_of(half) - base
        self_ref[rows, :] = jnp.where((own >= 0) & (own < cap), own, big)

    @pl.when(j == 0)
    def _():
        for i in range(loads):
            load(i).wait()

            @pl.loop(0, share // ROWS)
            def _(t):
                span = pl.ds(pl.multiple_of(t * ROWS, ROWS), ROWS)
                for c in range(pieces):
                    wide_ref[
                        pl.ds((i * share + t * ROWS) * pieces + c, ROWS, stride=pieces), :
                    ] = stage_ref[i, span, c * LANES : (c + 1) * LANES].astype(jnp.float32)

    chunk = 320 if cap % 320 == 0 else ROWS
    tiles = chunk // packed
    tile = (packed, LANES)
    iota = lax.broadcasted_iota(jnp.int32, tile, 0)

    def entry(k, row):
        slot = jnp.broadcast_to(order_ref[k, row, :], tile)
        return slot, jnp.broadcast_to(times_ref[k, row, :], tile).astype(jnp.bfloat16)

    def mark(totals, slot, times, first):
        local = (slot - first).astype(jnp.int16)
        return tuple(
            jnp.where((iota + packed * t).astype(jnp.int16) == local, times, totals[t])
            for t in range(tiles)
        )

    def spans(first):
        return [pl.ds(pl.multiple_of(first + packed * t, packed), packed) for t in range(tiles)]

    for g in range(groups):
        lanes = pl.ds(g * LANES, LANES)
        own_ref[0, 0:1, lanes] = self_ref[pl.ds(j * groups + g, 1), :]
        own_ref[0, 1:2, lanes] = alive_ref[pl.ds(j * groups + g, 1), :]

    parts = cap // chunk
    turns = groups * parts
    part = cap // turns

    burst = part // SURE
    casts = [(p, i) for i in range(part // packed) for p in range(pieces)]

    def cast(buffer, target, p, i):
        rows_ref[
            0,
            pl.ds(pl.multiple_of(target + i * packed, packed), packed),
            p * LANES : (p + 1) * LANES,
        ] = picked_ref[
            buffer, i * packed * pieces + p : (i + 1) * packed * pieces : pieces, :
        ].astype(jnp.bfloat16)

    @pl.loop(0, groups)
    def _(g):
        lanes = pl.ds(pl.multiple_of(g * LANES, LANES), LANES)
        row = pl.ds(j * groups + g, 1)
        for c in range(parts):
            turn = g * parts + c
            first = turn * part
            here, there = c % 2, 1 - c % 2
            before = lax.max(turn - 1, 0) * part
            totals = (jnp.zeros(tile, jnp.bfloat16),) * tiles
            for k in range(SURE):
                places = [
                    pl.multiple_of(index_ref[0, 0, first + k * burst + u], pieces) for u in range(burst)
                ]
                for u in range(burst):
                    into = (k * burst + u) * pieces
                    picked_ref[here, into : into + pieces, :] = wide_ref[pl.ds(places[u], pieces), :]
                totals = mark(totals, *entry(k, row), c * chunk)
                for p, i in casts[k * len(casts) // SURE : (k + 1) * len(casts) // SURE]:
                    cast(there, before, p, i)
            for span, total in zip(spans(c * chunk), totals):
                counts_ref[0, span, lanes] = total

    for p, i in casts:
        cast((turns - 1) % 2, (turns - 1) * part, p, i)

    @pl.when(most_ref[j] > SURE)
    def _():
        for g in range(groups):
            lanes = pl.ds(g * LANES, LANES)
            row = pl.ds(j * groups + g, 1)
            most = jnp.max(mine_ref[row, :])

            @pl.when(most > SURE)
            def _():
                @pl.loop(0, cap // chunk)
                def _(c):
                    totals = tuple(counts_ref[0, span, lanes] for span in spans(c * chunk))
                    totals = lax.fori_loop(
                        SURE, most, lambda k, t: mark(t, *entry(k, row), c * chunk), totals
                    )
                    for span, total in zip(spans(c * chunk), totals):
                        counts_ref[0, span, lanes] = total


def pick_and_count(base, index, lists, table, neighbours, cap):
    peers = lists.shape[0]
    groups = lists.shape[1] // (neighbours // 2 + 1)
    negatives = groups * LANES
    rows = peers * groups
    width = table.shape[1]
    pieces = width // LANES
    return pl.pallas_call(
        functools.partial(count_kernel, neighbours, cap),
        grid=(peers,),
        out_shape=(
            jax.ShapeDtypeStruct((peers, cap, negatives), jnp.bfloat16),
            jax.ShapeDtypeStruct((peers, 2, negatives), jnp.int32),
            jax.ShapeDtypeStruct((peers, cap, width), jnp.bfloat16),
        ),
        in_specs=[
            pl.BlockSpec(memory_space=pltpu.SMEM),
            pl.BlockSpec((1, 1, cap), lambda j: (j, 0, 0), memory_space=pltpu.SMEM),
            pl.BlockSpec((2,) + lists.shape[1:], lambda j: (lax.div(j, 2), 0, 0)),
            pl.BlockSpec(memory_space=pl.ANY),
        ],
        out_specs=(
            pl.BlockSpec((1, cap, negatives), lambda j: (j, 0, 0)),
            pl.BlockSpec((1, 2, negatives), lambda j: (j, 0, 0)),
            pl.BlockSpec((1, cap, width), lambda j: (j, 0, 0)),
        ),
        scratch_shapes=[
            pltpu.VMEM((neighbours, rows, LANES), jnp.int32),
            pltpu.VMEM((neighbours, rows, LANES), jnp.float32),
            pltpu.VMEM((rows, LANES), jnp.int32),
            pltpu.SMEM((peers,), jnp.int32),
            pltpu.VMEM((rows, LANES), jnp.int32),
            pltpu.VMEM((rows, LANES), jnp.int32),
            pltpu.VMEM((table.shape[0] * pieces, LANES), jnp.float32),
            pltpu.VMEM((2, cap * pieces // 8, LANES), jnp.float32),
            pltpu.VMEM((8, table.shape[0] // 8, width), table.dtype),
            pltpu.SemaphoreType.DMA((8,)),
        ],
        compiler_params=pltpu.CompilerParams(vmem_limit_bytes=62 << 20),
    )(base, index, lists, table)


def score_all(
    total_negatives, hidden_ref, around_ref, bias_ref, count_ref, live_ref,
    embed_ref, lse_ref,
    log_ref, mine_ref, slots_ref, merged_ref, all_ref,
    s_send1, r_send1, s_send2, r_send2,
):
    x, y, z, core = place()
    others = ORDER[:-1]
    negatives = hidden_ref.shape[0]

    def column(row_ref):
        row = row_ref[...].astype(jnp.float32)
        return jnp.broadcast_to(row, (LANES, negatives)).T

    mine = pl.ds(pl.multiple_of((2 * z + core) * negatives, negatives), negatives)
    log_ref[...] = LOG2E * jnp.log(column(count_ref.at[:, mine]))
    inverse = 1.0 / column(live_ref)[:, :1]
    hidden = jax.nn.relu(hidden_ref[...] * inverse + bias_ref[...])
    scale = lax.rsqrt(jnp.mean(hidden * hidden, axis=1, keepdims=True) + 0.25)
    embed_ref[...] = (hidden * scale).astype(jnp.bfloat16)
    tile = 256

    def score(slot, ref):
        for t in range(around_ref.shape[1] // tile):
            span = pl.ds(t * tile, tile)
            product = lax.dot_general(
                embed_ref[...], ref[span, :], NT, preferred_element_type=jnp.float32
            )
            logs = jnp.concatenate([log_ref[...]] * (tile // LANES), axis=1)
            scores = (0.25 * LOG2E) * product - logs
            peak = jnp.max(scores, axis=0, keepdims=True)
            total = jnp.sum(jnp.exp2(scores - peak), axis=0, keepdims=True)
            mine_ref[slot, :, span] = (peak + jnp.log2(total)) * (1 / LOG2E)

    def exchange1(slot):
        dz, c = lax.div(slot, 2), lax.rem(slot, 2)
        return remote(
            mine_ref.at[slot], slots_ref.at[slot], s_send1.at[slot], r_send1.at[slot],
            device(x, y, z + dz, lax.rem(core + c, 2)),
        )

    @pl.loop(0, 8)
    def _(turn):
        slot = jnp.int32(0)
        for i, chosen in enumerate((4, 5, 2, 3, 6, 7, 1)):
            slot = lax.select(turn == i, jnp.int32(chosen), slot)

        score(slot, around_ref.at[slot])

        @pl.when(turn < 7)
        def _():
            exchange1(slot).start()

    slots_ref[0] = mine_ref[0]
    for slot in range(1, 8):
        exchange1(slot).wait_recv()

    def merge(ref, count):
        values = [ref[i] for i in range(count)]
        top = functools.reduce(jnp.maximum, values)
        return top + jnp.log(sum(jnp.exp(v - top) for v in values))

    merged_ref[...] = merge(slots_ref, 8)

    def exchange2(j):
        dx, dy = others[j]
        return remote(
            merged_ref, all_ref.at[j], s_send2.at[j], r_send2.at[j], device(x - dx, y - dy, z, core)
        )

    for j in range(len(others)):
        exchange2(j).start()
    all_ref[len(others)] = merged_ref[...]
    for j in range(len(others)):
        exchange2(j).wait_recv()
    lse_ref[...] = merge(all_ref, len(others) + 1) - math.log(total_negatives)
    for slot in range(1, 8):
        exchange1(slot).wait_send()
    for j in range(len(others)):
        exchange2(j).wait_send()


def reduce_kernel(
    total_negatives,
    rows_ref, counts_ref, own_ref, wm_ref, mb_ref, ws_ref, wn_ref,
    queries_ref, bias_ref, count_ref, live_ref, embed_ref, lse_ref,
    around_ref, hot_ref, message_ref, from_ref, into_ref, total_ref, part_ref,
    relay1, full1, relay2, full2,
    s_relay1, r_relay1, s_full1, r_full1, s_relay2, r_relay2, s_full2, r_full2,
    s_query, r_query, s_own,
    *score_refs,
):
    step = pl.program_id(0)
    x, y, z, core = place()
    _, cap, width = rows_ref.shape
    negatives = counts_ref.shape[2]
    groups = negatives // LANES
    half, quarter = negatives // 2, negatives // 4
    packed = 16

    def neighbour(axis, sign):
        if axis == 0:
            return device(x + sign, y, z, core)
        return device(x, y + sign, z, core)

    up, down, sibling = device(x, y, z + 1, core), device(x, y, z - 1, core), device(x, y, z, 1 - core)
    upper = pl.ds(0, queries_ref.shape[0] // 2)
    lower = pl.ds(queries_ref.shape[0] // 2, queries_ref.shape[0] // 2)

    def query_copy(which):
        sem = (s_query.at[which], r_query.at[which])
        if which == 0:
            return remote(queries_ref, around_ref.at[6], *sem, up)
        if which == 1:
            return remote(queries_ref, around_ref.at[2], *sem, down)
        if which == 2:
            return remote(queries_ref, around_ref.at[1], *sem, sibling)
        if which == 3:
            return remote(around_ref.at[6, upper], around_ref.at[4, upper], *sem, up)
        if which == 4:
            return remote(around_ref.at[2, lower], around_ref.at[4, lower], *sem, down)
        slot = {5: 6, 6: 2, 7: 4}[which]
        return remote(around_ref.at[slot], around_ref.at[slot + 1], *sem, sibling)

    @pl.when(step == 0)
    def _():
        greet(
            [device(x, y, z - dz, lax.rem(core + c, 2)) for dz, c in NEAR]
            + [device(x - dx, y - dy, z, core) for dx, dy in ORDER[:-1]]
        )
        for which in range(3):
            query_copy(which).start()
        pltpu.make_async_copy(queries_ref, around_ref.at[0], s_own).start()

    @pl.when(step == 10)
    def _():
        for which in (0, 1):
            query_copy(which).wait_recv()
        for which in (3, 4, 5, 6):
            query_copy(which).start()

    @pl.when(step == 15)
    def _():
        for which in (3, 4):
            query_copy(which).wait_recv()
        query_copy(7).start()

    tile = (packed, LANES)
    iota = lax.broadcasted_iota(jnp.int32, tile, 0)
    heres = [(iota + i * packed).astype(jnp.int16) for i in range(cap // packed)]
    zero = jnp.zeros(tile, jnp.bfloat16)
    for g in range(groups):
        lanes = pl.ds(g * LANES, LANES)
        own = jnp.broadcast_to(own_ref[0, 0:1, lanes], tile).astype(jnp.int16)
        live = jnp.broadcast_to(own_ref[0, 1:2, lanes].astype(jnp.float32), tile).astype(jnp.bfloat16)
        for i, here in enumerate(heres):
            hot_ref[i * packed : (i + 1) * packed, lanes] = jnp.where(here == own, live, zero)

    columns = [slice(c, c + width // 2) for c in (0, width // 2)]
    into_ref[:, :cap] = counts_ref[0].T
    into_ref[:, cap:] = hot_ref[...].T

    def dot(a, b):
        return jnp.dot(a, b, preferred_element_type=jnp.float32)

    for s in columns:
        message_ref[:, s] = jax.nn.relu(dot(rows_ref[0], wm_ref[:, s]) + mb_ref[:, s]).astype(
            jnp.bfloat16
        )
        from_ref[cap:, s] = dot(rows_ref[0], ws_ref[:, s]).astype(jnp.bfloat16)
    for s in columns:
        from_ref[:cap, s] = dot(message_ref[...], wn_ref[:, s]).astype(jnp.bfloat16)
    for s in columns:
        part_ref[step, :, s] = dot(into_ref[...], from_ref[:, s]).astype(jnp.bfloat16)

    block = 64
    last = len(ORDER) - 1

    def combine(j, first, count, sources):
        @pl.loop(0, count // block)
        def _(i):
            span = pl.ds(pl.multiple_of(first + i * block, block), block)
            value = part_ref[j, span, :].astype(jnp.float32)
            for source, begin in sources:
                value = value + source[
                    pl.ds(pl.multiple_of(begin + i * block, block), block), :
                ].astype(jnp.float32)
            if j == last:
                total_ref[span, :] = value
            else:
                part_ref[j, span, :] = value.astype(jnp.bfloat16)

    def relay_copy(j, first, axis, side, relay, send, recv, at):
        return remote(
            part_ref.at[j, pl.ds(first + side * quarter, quarter)],
            relay.at[(*at, side)], send.at[(*at, side)], recv.at[(*at, side)],
            neighbour(axis, 1 - 2 * side),
        )

    def full_copy(j, first, axis, side, full, send, recv, at):
        return remote(
            part_ref.at[j, pl.ds(first, half)],
            full.at[(*at, side)], send.at[(*at, side)], recv.at[(*at, side)],
            neighbour(axis, 1 - 2 * side),
        )

    def arrive(j, first, axis, offset, bufs, at):
        relay, full, s_relay, r_relay, s_full, r_full = bufs
        into = [[], []]
        if offset in (1, 3):
            side = 0 if offset == 1 else 1
            relay_copy(j, first, axis, side, relay, s_relay, r_relay, at).wait_recv()
            into[side].append((relay.at[(*at, side)], 0))
        elif offset == 0:
            for side in (0, 1):
                full_copy(j, first, axis, side, full, s_full, r_full, at).wait_recv()
                for q in (0, 1):
                    into[q].append((full.at[(*at, side)], q * quarter))
        return into

    def leave(j, first, axis, offset, bufs, at):
        relay, full, s_relay, r_relay, s_full, r_full = bufs
        if offset == 2:
            for side in (0, 1):
                relay_copy(j, first, axis, side, relay, s_relay, r_relay, at).start()
        elif offset in (1, 3):
            side = 0 if offset == 1 else 1
            full_copy(j, first, axis, side, full, s_full, r_full, at).start()

    stage1 = (relay1, full1, s_relay1, r_relay1, s_full1, r_full1)
    stage2 = (relay2, full2, s_relay2, r_relay2, s_full2, r_full2)
    for j, offsets in enumerate(ORDER):

        @pl.when(step == j)
        def _(j=j, offsets=offsets):
            for h in sorted((0, 1), key=lambda h: offsets[h] == 0):
                first = h * half
                near, far = offsets[h], offsets[1 - h]
                into = arrive(j, first, h, near, stage1, (h, far))
                out = (j, first, h, near, stage1, (h, far))
                if near == 0:
                    out = (j, first, 1 - h, far, stage2, (h,))
                    into = [a + b for a, b in zip(into, arrive(*out))]
                for q in (0, 1):
                    if into[q]:
                        combine(j, first + q * quarter, quarter, into[q])
                leave(*out)

    @pl.when(step == len(ORDER) - 1)
    def _():
        for which in (2, 5, 6, 7):
            query_copy(which).wait_recv()
        pltpu.make_async_copy(queries_ref, around_ref.at[0], s_own).wait()
        score_all(
            total_negatives, total_ref, around_ref, bias_ref, count_ref, live_ref,
            embed_ref, lse_ref, *score_refs,
        )
        for j, offsets in enumerate(ORDER):
            for h in (0, 1):
                first = h * half
                near, far = offsets[h], offsets[1 - h]
                stages = [(near, h, stage1, (h, far))]
                if near == 0:
                    stages.append((far, 1 - h, stage2, (h,)))
                for offset, axis, bufs, at in stages:
                    relay, full, s_relay, r_relay, s_full, r_full = bufs
                    if offset == 2:
                        for side in (0, 1):
                            relay_copy(j, first, axis, side, relay, s_relay, r_relay, at).wait_send()
                    elif offset in (1, 3):
                        side = 0 if offset == 1 else 1
                        full_copy(j, first, axis, side, full, s_full, r_full, at).wait_send()
        for which in range(8):
            query_copy(which).wait_send()


def reduce_and_score(
    picked, counts, own, wm, mb, ws, wn, queries, bias, count, live, total_negatives
):
    peers, cap, negatives = counts.shape
    width = picked.shape[2]
    half, quarter = negatives // 2, negatives // 4
    vmem = pl.BlockSpec(memory_space=pltpu.VMEM)
    hbm = pl.BlockSpec(memory_space=pl.ANY)
    dma = pltpu.SemaphoreType.DMA
    bf16, f32 = jnp.bfloat16, jnp.float32
    return pl.pallas_call(
        functools.partial(reduce_kernel, total_negatives),
        grid=(peers,),
        out_shape=(
            jax.ShapeDtypeStruct((negatives, width), bf16),
            jax.ShapeDtypeStruct((1, queries.shape[0]), f32),
        ),
        in_specs=[
            pl.BlockSpec((1, cap, width), lambda j: (j, 0, 0)),
            pl.BlockSpec((1, cap, negatives), lambda j: (j, 0, 0)),
            pl.BlockSpec((1, 2, negatives), lambda j: (j, 0, 0)),
            vmem, vmem, vmem, vmem,
            hbm, vmem, vmem, vmem,
        ],
        out_specs=(vmem, vmem),
        scratch_shapes=[
            pltpu.VMEM((8,) + queries.shape, bf16),
            pltpu.VMEM((cap, negatives), bf16),
            pltpu.VMEM((cap, width), bf16),
            pltpu.VMEM((2 * cap, width), bf16),
            pltpu.VMEM((negatives, 2 * cap), bf16),
            pltpu.VMEM((negatives, width), f32),
            pltpu.VMEM((peers, negatives, width), bf16),
            pltpu.VMEM((2, SIDE, 2, quarter, width), bf16),
            pltpu.VMEM((2, SIDE, 2, half, width), bf16),
            pltpu.VMEM((2, 2, quarter, width), bf16),
            pltpu.VMEM((2, 2, half, width), bf16),
            dma((2, SIDE, 2)), dma((2, SIDE, 2)), dma((2, SIDE, 2)), dma((2, SIDE, 2)),
            dma((2, 2)), dma((2, 2)), dma((2, 2)), dma((2, 2)),
            dma((8,)), dma((8,)), dma,
            pltpu.VMEM((negatives, LANES), f32),
            pltpu.VMEM((8, 1, queries.shape[0]), f32),
            pltpu.VMEM((8, 1, queries.shape[0]), f32),
            pltpu.VMEM((1, queries.shape[0]), f32),
            pltpu.VMEM((peers, 1, queries.shape[0]), f32),
            dma((8,)), dma((8,)), dma((15,)), dma((15,)),
        ],
        compiler_params=pltpu.CompilerParams(
            collective_id=1, has_side_effects=True, vmem_limit_bytes=62 << 20
        ),
    )(picked, counts, own, wm, mb, ws, wn, queries, bias, count, live)


def per_device(
    items_table,
    fetch_rows,
    neighbour_slots,
    neighbour_count,
    self_slot,
    negative_count,
    message_weight,
    message_bias,
    self_weight,
    neighbour_weight,
    output_bias,
    queries,
):
    n_neg, n_qry = lax.axis_size("neg"), lax.axis_size("qry")
    own_neg = lax.axis_index("neg")
    cap = fetch_rows.shape[1]
    negatives, neighbours = neighbour_slots.shape

    assert n_neg * cap < DEAD and neighbours % 4 == 0 and n_neg == SIDE * SIDE and n_qry == 8
    all_lists, all_fetch = exchange_lists(
        neighbour_slots.T, neighbour_count[None, :], self_slot.reshape(-1, LANES), fetch_rows,
        items_table.shape[1] // LANES,
    )
    base = (own_neg * cap).astype(jnp.int32).reshape(1)
    counts, own, picked = pick_and_count(
        base, all_fetch, all_lists, items_table, neighbours, cap
    )
    negative_embed, query_lse = reduce_and_score(
        picked, counts, own,
        message_weight, message_bias[None, :], self_weight, neighbour_weight, queries,
        output_bias[None, :], negative_count[None, :], neighbour_count[None, :],
        negatives * n_neg * n_qry,
    )
    return (negative_embed, query_lse.reshape(-1))


def solution(mesh):
    in_specs = (
        P("neg", None),
        P(("neg", "qry"), None),
        P(("neg", "qry"), None),
        P(("neg", "qry")),
        P(("neg", "qry")),
        P("neg"),
        P(),
        P(),
        P(),
        P(),
        P(),
        P("qry", None),
    )
    out_specs = (P(("neg", "qry"), None), P("qry"))
    return jax.shard_map(
        per_device, mesh=mesh, in_specs=in_specs, out_specs=out_specs, check_vma=False
    )
```

```python
import functools
import math

import jax
import jax.numpy as jnp
from jax import lax
from jax.experimental import pallas as pl
from jax.experimental.pallas import tpu as pltpu
from jax.sharding import PartitionSpec as P


LANES = 128
ROWS = 128
DEAD = 32767
SIDE = 4
NT = (((1,), (1,)), ((), ()))
SURE = 10
LOG2E = math.log2(math.e)
MESH = pl.DeviceIdType.MESH
ORDER = (
    (2, 2), (2, 1), (2, 3), (1, 2), (3, 2), (2, 0), (0, 2), (1, 1),
    (1, 3), (3, 1), (3, 3), (1, 0), (3, 0), (0, 1), (0, 3), (0, 0),
)

NEAR = tuple((dz, c) for dz in range(SIDE) for c in (0, 1))[1:]


def sort_pairs(count):
    full = 1
    while full < count:
        full *= 2
    pairs = []
    p = 1
    while p < full:
        k = p
        while k >= 1:
            for j in range(k % p, full - k, 2 * k):
                for i in range(min(k, full - j - k)):
                    if (i + j) // (2 * p) == (i + j + k) // (2 * p):
                        if i + j + k < count:
                            pairs.append((i + j, i + j + k))
            k //= 2
        p *= 2
    return pairs


def place():
    neg, qry = lax.axis_index("neg"), lax.axis_index("qry")
    return neg // SIDE, neg % SIDE, qry // 2, qry % 2


def device(x, y, z, core):
    wrap = lambda v: lax.rem(v + 2 * SIDE, SIDE)
    return (wrap(x) * SIDE + wrap(y), wrap(z) * 2 + core)


def remote(src, dst, send, recv, target):
    return pltpu.make_async_remote_copy(
        src_ref=src, dst_ref=dst, send_sem=send, recv_sem=recv,
        device_id=target, device_id_type=MESH,
    )


def greet(peers):
    barrier = pltpu.get_barrier_semaphore()
    for peer in peers:
        pl.semaphore_signal(barrier, inc=1, device_id=peer, device_id_type=MESH)
    pl.semaphore_wait(barrier, len(peers))


def exchange_kernel(
    pieces, slots_ref, count_ref, self_ref, fetch_ref, all_lists, all_fetch,
    lists_ref, asked_ref, sends, recvs,
):
    x, y, z, core = place()
    others = ORDER[:-1]
    neighbours, negatives = slots_ref.shape
    groups, half = negatives // LANES, neighbours // 2
    turn = lax.broadcasted_iota(jnp.int32, slots_ref.shape, 0)
    slots = jnp.where(turn < count_ref[...], slots_ref[...], DEAD)
    words = slots[:half] | (slots[half:] << 16)
    for k in range(half):
        for g in range(groups):
            row = k * groups + g
            lists_ref[row : row + 1, :] = words[k : k + 1, g * LANES : (g + 1) * LANES]
    lists_ref[half * groups :, :] = self_ref[...]
    for p in range(SIDE * SIDE):
        asked_ref[p] = fetch_ref[p : p + 1, :] * pieces
    greet([device(x - dx, y - dy, z, core) for dx, dy in others])
    copies = []
    for j, (dx, dy) in enumerate(others):
        target = device(x - dx, y - dy, z, core)
        copies.append(
            remote(asked_ref.at[target[0]], all_fetch.at[j], sends.at[0, j], recvs.at[0, j], target)
        )
        copies.append(remote(lists_ref, all_lists.at[j], sends.at[1, j], recvs.at[1, j], target))
    for copy in copies:
        copy.start()
    last = len(others)
    all_fetch[last] = asked_ref[x * SIDE + y]
    all_lists[last] = lists_ref[...]
    for copy in copies:
        copy.wait()


def exchange_lists(slots, count, own, fetch, pieces):
    peers, cap = fetch.shape
    neighbours, negatives = slots.shape
    lists = ((neighbours // 2 + 1) * negatives // LANES, LANES)
    vmem = pl.BlockSpec(memory_space=pltpu.VMEM)
    return pl.pallas_call(
        functools.partial(exchange_kernel, pieces),
        out_shape=(
            jax.ShapeDtypeStruct((peers,) + lists, jnp.int32),
            jax.ShapeDtypeStruct((peers, 1, cap), fetch.dtype),
        ),
        in_specs=[vmem, vmem, vmem, vmem],
        out_specs=(vmem, vmem),
        scratch_shapes=[
            pltpu.VMEM(lists, jnp.int32),
            pltpu.VMEM((peers, 1, cap), fetch.dtype),
            pltpu.SemaphoreType.DMA((2, peers - 1)),
            pltpu.SemaphoreType.DMA((2, peers - 1)),
        ],
        compiler_params=pltpu.CompilerParams(collective_id=0, has_side_effects=True),
    )(slots, count, own, fetch)


def count_kernel(
    neighbours, cap, base_ref, index_ref, lists_ref, table_ref,
    counts_ref, own_ref, rows_ref,
    order_ref, times_ref, mine_ref, most_ref, alive_ref, self_ref, wide_ref, picked_ref,
    stage_ref, s_stage,
):
    j = pl.program_id(0)
    rows, width = table_ref.shape
    pieces = width // LANES

    loads, share = stage_ref.shape[0], stage_ref.shape[1]

    def load(i):
        return pltpu.make_async_copy(
            table_ref.at[pl.ds(i * share, share)], stage_ref.at[i], s_stage.at[i]
        )

    @pl.when(j == 0)
    def _():
        for i in range(loads):
            load(i).start()

    groups = counts_ref.shape[2] // LANES
    half = neighbours // 2
    packed = 16
    tall = 8
    batch = tall // groups
    big = jnp.int32(DEAD)

    @pl.when(lax.rem(j, batch) == 0)
    def _():
        base = base_ref[0]
        live = jnp.zeros((tall, LANES), jnp.int32)
        mine = jnp.zeros((tall, LANES), jnp.int32)

        def rows_of(k):
            return jnp.concatenate(
                [lists_ref[i, k * groups : (k + 1) * groups, :] for i in range(batch)]
            )

        words = [rows_of(k) for k in range(half)]
        places = []
        for k in range(neighbours):
            slot = words[k] & DEAD if k < half else words[k - half] >> 16
            local = slot - base
            inside = (local >= 0) & (local < cap)
            live = live + jnp.where(slot < DEAD, 1, 0)
            mine = mine + jnp.where(inside, 1, 0)
            places.append(jnp.where(inside, local, big).astype(jnp.float32))
        for a, b in sort_pairs(neighbours):
            low, high = jnp.minimum(places[a], places[b]), jnp.maximum(places[a], places[b])
            places[a], places[b] = low, high
        rows = pl.ds(pl.multiple_of(j * groups, tall), tall)
        run = jnp.ones((tall, LANES), jnp.float32)
        for k in range(neighbours):
            if k:
                run = jnp.where(places[k] == places[k - 1], run + 1.0, 1.0)
            order_ref[k, rows, :] = places[k].astype(jnp.int32)
            times_ref[k, rows, :] = run
        mine_ref[rows, :] = mine
        for i in range(batch):
            most_ref[j + i] = jnp.max(mine[i * groups : (i + 1) * groups])
        alive_ref[rows, :] = live
        own = rows_of(half) - base
        self_ref[rows, :] = jnp.where((own >= 0) & (own < cap), own, big)

    @pl.when(j == 0)
    def _():
        for i in range(loads):
            load(i).wait()

            @pl.loop(0, share // ROWS)
            def _(t):
                span = pl.ds(pl.multiple_of(t * ROWS, ROWS), ROWS)
                for c in range(pieces):
                    wide_ref[
                        pl.ds((i * share + t * ROWS) * pieces + c, ROWS, stride=pieces), :
                    ] = stage_ref[i, span, c * LANES : (c + 1) * LANES].astype(jnp.float32)

    chunk = 320 if cap % 320 == 0 else ROWS
    tiles = chunk // packed
    tile = (packed, LANES)
    iota = lax.broadcasted_iota(jnp.int32, tile, 0)

    def entry(k, row):
        slot = jnp.broadcast_to(order_ref[k, row, :], tile)
        return slot, jnp.broadcast_to(times_ref[k, row, :], tile).astype(jnp.bfloat16)

    def mark(totals, slot, times, first):
        local = (slot - first).astype(jnp.int16)
        return tuple(
            jnp.where((iota + packed * t).astype(jnp.int16) == local, times, totals[t])
            for t in range(tiles)
        )

    def spans(first):
        return [pl.ds(pl.multiple_of(first + packed * t, packed), packed) for t in range(tiles)]

    for g in range(groups):
        lanes = pl.ds(g * LANES, LANES)
        own_ref[0, 0:1, lanes] = self_ref[pl.ds(j * groups + g, 1), :]
        own_ref[0, 1:2, lanes] = alive_ref[pl.ds(j * groups + g, 1), :]

    parts = cap // chunk
    turns = groups * parts
    part = cap // turns

    burst = part // SURE
    casts = [(p, i) for i in range(part // packed) for p in range(pieces)]

    def cast(buffer, target, p, i):
        rows_ref[
            0,
            pl.ds(pl.multiple_of(target + i * packed, packed), packed),
            p * LANES : (p + 1) * LANES,
        ] = picked_ref[
            buffer, i * packed * pieces + p : (i + 1) * packed * pieces : pieces, :
        ].astype(jnp.bfloat16)

    @pl.loop(0, groups)
    def _(g):
        lanes = pl.ds(pl.multiple_of(g * LANES, LANES), LANES)
        row = pl.ds(j * groups + g, 1)
        for c in range(parts):
            turn = g * parts + c
            first = turn * part
            here, there = c % 2, 1 - c % 2
            before = lax.max(turn - 1, 0) * part
            totals = (jnp.zeros(tile, jnp.bfloat16),) * tiles
            for k in range(SURE):
                places = [
                    pl.multiple_of(index_ref[0, 0, first + k * burst + u], pieces) for u in range(burst)
                ]
                for u in range(burst):
                    into = (k * burst + u) * pieces
                    picked_ref[here, into : into + pieces, :] = wide_ref[pl.ds(places[u], pieces), :]
                totals = mark(totals, *entry(k, row), c * chunk)
                for p, i in casts[k * len(casts) // SURE : (k + 1) * len(casts) // SURE]:
                    cast(there, before, p, i)
            for span, total in zip(spans(c * chunk), totals):
                counts_ref[0, span, lanes] = total

    for p, i in casts:
        cast((turns - 1) % 2, (turns - 1) * part, p, i)

    @pl.when(most_ref[j] > SURE)
    def _():
        for g in range(groups):
            lanes = pl.ds(g * LANES, LANES)
            row = pl.ds(j * groups + g, 1)
            most = jnp.max(mine_ref[row, :])

            @pl.when(most > SURE)
            def _():
                @pl.loop(0, cap // chunk)
                def _(c):
                    totals = tuple(counts_ref[0, span, lanes] for span in spans(c * chunk))
                    totals = lax.fori_loop(
                        SURE, most, lambda k, t: mark(t, *entry(k, row), c * chunk), totals
                    )
                    for span, total in zip(spans(c * chunk), totals):
                        counts_ref[0, span, lanes] = total


def pick_and_count(base, index, lists, table, neighbours, cap):
    peers = lists.shape[0]
    groups = lists.shape[1] // (neighbours // 2 + 1)
    negatives = groups * LANES
    rows = peers * groups
    width = table.shape[1]
    pieces = width // LANES
    return pl.pallas_call(
        functools.partial(count_kernel, neighbours, cap),
        grid=(peers,),
        out_shape=(
            jax.ShapeDtypeStruct((peers, cap, negatives), jnp.bfloat16),
            jax.ShapeDtypeStruct((peers, 2, negatives), jnp.int32),
            jax.ShapeDtypeStruct((peers, cap, width), jnp.bfloat16),
        ),
        in_specs=[
            pl.BlockSpec(memory_space=pltpu.SMEM),
            pl.BlockSpec((1, 1, cap), lambda j: (j, 0, 0), memory_space=pltpu.SMEM),
            pl.BlockSpec((2,) + lists.shape[1:], lambda j: (lax.div(j, 2), 0, 0)),
            pl.BlockSpec(memory_space=pl.ANY),
        ],
        out_specs=(
            pl.BlockSpec((1, cap, negatives), lambda j: (j, 0, 0)),
            pl.BlockSpec((1, 2, negatives), lambda j: (j, 0, 0)),
            pl.BlockSpec((1, cap, width), lambda j: (j, 0, 0)),
        ),
        scratch_shapes=[
            pltpu.VMEM((neighbours, rows, LANES), jnp.int32),
            pltpu.VMEM((neighbours, rows, LANES), jnp.float32),
            pltpu.VMEM((rows, LANES), jnp.int32),
            pltpu.SMEM((peers,), jnp.int32),
            pltpu.VMEM((rows, LANES), jnp.int32),
            pltpu.VMEM((rows, LANES), jnp.int32),
            pltpu.VMEM((table.shape[0] * pieces, LANES), jnp.float32),
            pltpu.VMEM((2, cap * pieces // 8, LANES), jnp.float32),
            pltpu.VMEM((8, table.shape[0] // 8, width), table.dtype),
            pltpu.SemaphoreType.DMA((8,)),
        ],
        compiler_params=pltpu.CompilerParams(vmem_limit_bytes=62 << 20),
    )(base, index, lists, table)


def score_all(
    total_negatives, hidden_ref, around_ref, bias_ref, count_ref, live_ref,
    embed_out, lse_ref,
    embed_ref, s_embed, log_ref, mine_ref, slots_ref, merged_ref, all_ref,
    s_send1, r_send1, s_send2, r_send2,
):
    x, y, z, core = place()
    others = ORDER[:-1]
    negatives = hidden_ref.shape[0]

    def column(row_ref):
        row = row_ref[...].astype(jnp.float32)
        return jnp.broadcast_to(row, (LANES, negatives)).T

    mine = pl.ds(pl.multiple_of((2 * z + core) * negatives, negatives), negatives)
    log_ref[...] = LOG2E * jnp.log(column(count_ref.at[:, mine]))
    inverse = 1.0 / column(live_ref)[:, :1]
    hidden = jax.nn.relu(hidden_ref[...] * inverse + bias_ref[...])
    scale = lax.rsqrt(jnp.mean(hidden * hidden, axis=1, keepdims=True) + 0.25)
    embed_ref[...] = (hidden * scale).astype(jnp.bfloat16)
    tile = 256

    def score(slot, ref):
        for t in range(around_ref.shape[1] // tile):
            span = pl.ds(t * tile, tile)
            product = lax.dot_general(
                embed_ref[...], ref[span, :], NT, preferred_element_type=jnp.float32
            )
            logs = jnp.concatenate([log_ref[...]] * (tile // LANES), axis=1)
            scores = (0.25 * LOG2E) * product - logs
            peak = jnp.max(scores, axis=0, keepdims=True)
            total = jnp.sum(jnp.exp2(scores - peak), axis=0, keepdims=True)
            mine_ref[slot, :, span] = (peak + jnp.log2(total)) * (1 / LOG2E)

    def exchange1(slot):
        dz, c = lax.div(slot, 2), lax.rem(slot, 2)
        return remote(
            mine_ref.at[slot], slots_ref.at[slot], s_send1.at[slot], r_send1.at[slot],
            device(x, y, z + dz, lax.rem(core + c, 2)),
        )

    @pl.loop(0, 8)
    def _(turn):
        slot = jnp.int32(0)
        for i, chosen in enumerate((4, 5, 2, 3, 6, 7, 1)):
            slot = lax.select(turn == i, jnp.int32(chosen), slot)

        score(slot, around_ref.at[slot])

        @pl.when(turn < 7)
        def _():
            exchange1(slot).start()

    embed_copy = pltpu.make_async_copy(embed_ref, embed_out, s_embed)
    embed_copy.start()
    slots_ref[0] = mine_ref[0]
    for slot in range(1, 8):
        exchange1(slot).wait_recv()

    def merge(ref, count):
        values = [ref[i] for i in range(count)]
        top = functools.reduce(jnp.maximum, values)
        return top + jnp.log(sum(jnp.exp(v - top) for v in values))

    merged_ref[...] = merge(slots_ref, 8)

    def exchange2(j):
        dx, dy = others[j]
        return remote(
            merged_ref, all_ref.at[j], s_send2.at[j], r_send2.at[j], device(x - dx, y - dy, z, core)
        )

    for j in range(len(others)):
        exchange2(j).start()
    all_ref[len(others)] = merged_ref[...]
    for j in range(len(others)):
        exchange2(j).wait_recv()
    lse_ref[...] = merge(all_ref, len(others) + 1) - math.log(total_negatives)
    embed_copy.wait()
    for slot in range(1, 8):
        exchange1(slot).wait_send()
    for j in range(len(others)):
        exchange2(j).wait_send()


def reduce_kernel(
    total_negatives,
    rows_ref, counts_ref, own_ref, wm_ref, mb_ref, ws_ref, wn_ref,
    queries_ref, bias_ref, count_ref, live_ref, embed_out, lse_ref,
    around_ref, hot_ref, message_ref, from_ref, into_ref, total_ref, part_ref,
    relay1, full1, relay2, full2,
    s_relay1, r_relay1, s_full1, r_full1, s_relay2, r_relay2, s_full2, r_full2,
    s_query, r_query, s_own,
    *score_refs,
):
    step = pl.program_id(0)
    x, y, z, core = place()
    _, cap, width = rows_ref.shape
    negatives = counts_ref.shape[2]
    groups = negatives // LANES
    half, quarter = negatives // 2, negatives // 4
    packed = 16

    def neighbour(axis, sign):
        if axis == 0:
            return device(x + sign, y, z, core)
        return device(x, y + sign, z, core)

    up, down, sibling = device(x, y, z + 1, core), device(x, y, z - 1, core), device(x, y, z, 1 - core)
    upper = pl.ds(0, queries_ref.shape[0] // 2)
    lower = pl.ds(queries_ref.shape[0] // 2, queries_ref.shape[0] // 2)

    def query_copy(which):
        sem = (s_query.at[which], r_query.at[which])
        if which == 0:
            return remote(queries_ref, around_ref.at[6], *sem, up)
        if which == 1:
            return remote(queries_ref, around_ref.at[2], *sem, down)
        if which == 2:
            return remote(queries_ref, around_ref.at[1], *sem, sibling)
        if which == 3:
            return remote(around_ref.at[6, upper], around_ref.at[4, upper], *sem, up)
        if which == 4:
            return remote(around_ref.at[2, lower], around_ref.at[4, lower], *sem, down)
        slot = {5: 6, 6: 2, 7: 4}[which]
        return remote(around_ref.at[slot], around_ref.at[slot + 1], *sem, sibling)

    @pl.when(step == 0)
    def _():
        greet(
            [device(x, y, z - dz, lax.rem(core + c, 2)) for dz, c in NEAR]
            + [device(x - dx, y - dy, z, core) for dx, dy in ORDER[:-1]]
        )
        for which in range(3):
            query_copy(which).start()
        pltpu.make_async_copy(queries_ref, around_ref.at[0], s_own).start()

    @pl.when(step == 10)
    def _():
        for which in (0, 1):
            query_copy(which).wait_recv()
        for which in (3, 4, 5, 6):
            query_copy(which).start()

    @pl.when(step == 15)
    def _():
        for which in (3, 4):
            query_copy(which).wait_recv()
        query_copy(7).start()

    tile = (packed, LANES)
    iota = lax.broadcasted_iota(jnp.int32, tile, 0)
    heres = [(iota + i * packed).astype(jnp.int16) for i in range(cap // packed)]
    zero = jnp.zeros(tile, jnp.bfloat16)
    for g in range(groups):
        lanes = pl.ds(g * LANES, LANES)
        own = jnp.broadcast_to(own_ref[0, 0:1, lanes], tile).astype(jnp.int16)
        live = jnp.broadcast_to(own_ref[0, 1:2, lanes].astype(jnp.float32), tile).astype(jnp.bfloat16)
        for i, here in enumerate(heres):
            hot_ref[i * packed : (i + 1) * packed, lanes] = jnp.where(here == own, live, zero)

    columns = [slice(c, c + width // 2) for c in (0, width // 2)]
    into_ref[:, :cap] = counts_ref[0].T
    into_ref[:, cap:] = hot_ref[...].T

    def dot(a, b):
        return jnp.dot(a, b, preferred_element_type=jnp.float32)

    for s in columns:
        message_ref[:, s] = jax.nn.relu(dot(rows_ref[0], wm_ref[:, s]) + mb_ref[:, s]).astype(
            jnp.bfloat16
        )
        from_ref[cap:, s] = dot(rows_ref[0], ws_ref[:, s]).astype(jnp.bfloat16)
    for s in columns:
        from_ref[:cap, s] = dot(message_ref[...], wn_ref[:, s]).astype(jnp.bfloat16)
    for s in columns:
        part_ref[step, :, s] = dot(into_ref[...], from_ref[:, s]).astype(jnp.bfloat16)

    block = 64
    last = len(ORDER) - 1

    def combine(j, first, count, sources):
        @pl.loop(0, count // block)
        def _(i):
            span = pl.ds(pl.multiple_of(first + i * block, block), block)
            value = part_ref[j, span, :].astype(jnp.float32)
            for source, begin in sources:
                value = value + source[
                    pl.ds(pl.multiple_of(begin + i * block, block), block), :
                ].astype(jnp.float32)
            if j == last:
                total_ref[span, :] = value
            else:
                part_ref[j, span, :] = value.astype(jnp.bfloat16)

    def relay_copy(j, first, axis, side, relay, send, recv, at):
        return remote(
            part_ref.at[j, pl.ds(first + side * quarter, quarter)],
            relay.at[(*at, side)], send.at[(*at, side)], recv.at[(*at, side)],
            neighbour(axis, 1 - 2 * side),
        )

    def full_copy(j, first, axis, side, full, send, recv, at):
        return remote(
            part_ref.at[j, pl.ds(first, half)],
            full.at[(*at, side)], send.at[(*at, side)], recv.at[(*at, side)],
            neighbour(axis, 1 - 2 * side),
        )

    def arrive(j, first, axis, offset, bufs, at):
        relay, full, s_relay, r_relay, s_full, r_full = bufs
        into = [[], []]
        if offset in (1, 3):
            side = 0 if offset == 1 else 1
            relay_copy(j, first, axis, side, relay, s_relay, r_relay, at).wait_recv()
            into[side].append((relay.at[(*at, side)], 0))
        elif offset == 0:
            for side in (0, 1):
                full_copy(j, first, axis, side, full, s_full, r_full, at).wait_recv()
                for q in (0, 1):
                    into[q].append((full.at[(*at, side)], q * quarter))
        return into

    def leave(j, first, axis, offset, bufs, at):
        relay, full, s_relay, r_relay, s_full, r_full = bufs
        if offset == 2:
            for side in (0, 1):
                relay_copy(j, first, axis, side, relay, s_relay, r_relay, at).start()
        elif offset in (1, 3):
            side = 0 if offset == 1 else 1
            full_copy(j, first, axis, side, full, s_full, r_full, at).start()

    stage1 = (relay1, full1, s_relay1, r_relay1, s_full1, r_full1)
    stage2 = (relay2, full2, s_relay2, r_relay2, s_full2, r_full2)
    for j, offsets in enumerate(ORDER):

        @pl.when(step == j)
        def _(j=j, offsets=offsets):
            for h in sorted((0, 1), key=lambda h: offsets[h] == 0):
                first = h * half
                near, far = offsets[h], offsets[1 - h]
                into = arrive(j, first, h, near, stage1, (h, far))
                out = (j, first, h, near, stage1, (h, far))
                if near == 0:
                    out = (j, first, 1 - h, far, stage2, (h,))
                    into = [a + b for a, b in zip(into, arrive(*out))]
                for q in (0, 1):
                    if into[q]:
                        combine(j, first + q * quarter, quarter, into[q])
                leave(*out)

    @pl.when(step == len(ORDER) - 1)
    def _():
        for which in (2, 5, 6, 7):
            query_copy(which).wait_recv()
        pltpu.make_async_copy(queries_ref, around_ref.at[0], s_own).wait()
        score_all(
            total_negatives, total_ref, around_ref, bias_ref, count_ref, live_ref,
            embed_out, lse_ref, *score_refs,
        )
        for j, offsets in enumerate(ORDER):
            for h in (0, 1):
                first = h * half
                near, far = offsets[h], offsets[1 - h]
                stages = [(near, h, stage1, (h, far))]
                if near == 0:
                    stages.append((far, 1 - h, stage2, (h,)))
                for offset, axis, bufs, at in stages:
                    relay, full, s_relay, r_relay, s_full, r_full = bufs
                    if offset == 2:
                        for side in (0, 1):
                            relay_copy(j, first, axis, side, relay, s_relay, r_relay, at).wait_send()
                    elif offset in (1, 3):
                        side = 0 if offset == 1 else 1
                        full_copy(j, first, axis, side, full, s_full, r_full, at).wait_send()
        for which in range(8):
            query_copy(which).wait_send()


def reduce_and_score(
    picked, counts, own, wm, mb, ws, wn, queries, bias, count, live, total_negatives
):
    peers, cap, negatives = counts.shape
    width = picked.shape[2]
    half, quarter = negatives // 2, negatives // 4
    vmem = pl.BlockSpec(memory_space=pltpu.VMEM)
    hbm = pl.BlockSpec(memory_space=pl.ANY)
    dma = pltpu.SemaphoreType.DMA
    bf16, f32 = jnp.bfloat16, jnp.float32
    return pl.pallas_call(
        functools.partial(reduce_kernel, total_negatives),
        grid=(peers,),
        out_shape=(
            jax.ShapeDtypeStruct((negatives, width), bf16),
            jax.ShapeDtypeStruct((1, queries.shape[0]), f32),
        ),
        in_specs=[
            pl.BlockSpec((1, cap, width), lambda j: (j, 0, 0)),
            pl.BlockSpec((1, cap, negatives), lambda j: (j, 0, 0)),
            pl.BlockSpec((1, 2, negatives), lambda j: (j, 0, 0)),
            vmem, vmem, vmem, vmem,
            hbm, vmem, vmem, vmem,
        ],
        out_specs=(hbm, vmem),
        scratch_shapes=[
            pltpu.VMEM((8,) + queries.shape, bf16),
            pltpu.VMEM((cap, negatives), bf16),
            pltpu.VMEM((cap, width), bf16),
            pltpu.VMEM((2 * cap, width), bf16),
            pltpu.VMEM((negatives, 2 * cap), bf16),
            pltpu.VMEM((negatives, width), f32),
            pltpu.VMEM((peers, negatives, width), bf16),
            pltpu.VMEM((2, SIDE, 2, quarter, width), bf16),
            pltpu.VMEM((2, SIDE, 2, half, width), bf16),
            pltpu.VMEM((2, 2, quarter, width), bf16),
            pltpu.VMEM((2, 2, half, width), bf16),
            dma((2, SIDE, 2)), dma((2, SIDE, 2)), dma((2, SIDE, 2)), dma((2, SIDE, 2)),
            dma((2, 2)), dma((2, 2)), dma((2, 2)), dma((2, 2)),
            dma((8,)), dma((8,)), dma,
            pltpu.VMEM((negatives, width), bf16),
            dma,
            pltpu.VMEM((negatives, LANES), f32),
            pltpu.VMEM((8, 1, queries.shape[0]), f32),
            pltpu.VMEM((8, 1, queries.shape[0]), f32),
            pltpu.VMEM((1, queries.shape[0]), f32),
            pltpu.VMEM((peers, 1, queries.shape[0]), f32),
            dma((8,)), dma((8,)), dma((15,)), dma((15,)),
        ],
        compiler_params=pltpu.CompilerParams(
            collective_id=1, has_side_effects=True, vmem_limit_bytes=62 << 20
        ),
    )(picked, counts, own, wm, mb, ws, wn, queries, bias, count, live)


def hand_out_kernel(embed_ref, lse_ref, embed_out, lse_out):
    embed_out[...] = embed_ref[...]
    lse_out[...] = lse_ref[...]


def hand_out(embed, lse):
    vmem = pl.BlockSpec(memory_space=pltpu.VMEM)
    return pl.pallas_call(
        hand_out_kernel,
        out_shape=[jax.ShapeDtypeStruct(a.shape, a.dtype) for a in (embed, lse)],
        in_specs=[vmem, vmem],
        out_specs=[vmem, vmem],
    )(embed, lse)


def per_device(
    items_table,
    fetch_rows,
    neighbour_slots,
    neighbour_count,
    self_slot,
    negative_count,
    message_weight,
    message_bias,
    self_weight,
    neighbour_weight,
    output_bias,
    queries,
):
    n_neg, n_qry = lax.axis_size("neg"), lax.axis_size("qry")
    own_neg = lax.axis_index("neg")
    cap = fetch_rows.shape[1]
    negatives, neighbours = neighbour_slots.shape

    assert n_neg * cap < DEAD and neighbours % 4 == 0 and n_neg == SIDE * SIDE and n_qry == 8
    all_lists, all_fetch = exchange_lists(
        neighbour_slots.T, neighbour_count[None, :], self_slot.reshape(-1, LANES), fetch_rows,
        items_table.shape[1] // LANES,
    )
    base = (own_neg * cap).astype(jnp.int32).reshape(1)
    counts, own, picked = pick_and_count(
        base, all_fetch, all_lists, items_table, neighbours, cap
    )
    negative_embed, query_lse = reduce_and_score(
        picked, counts, own,
        message_weight, message_bias[None, :], self_weight, neighbour_weight, queries,
        output_bias[None, :], negative_count[None, :], neighbour_count[None, :],
        negatives * n_neg * n_qry,
    )
    negative_embed, query_lse = hand_out(negative_embed, query_lse)
    return (negative_embed, query_lse.reshape(-1))


def solution(mesh):
    in_specs = (
        P("neg", None),
        P(("neg", "qry"), None),
        P(("neg", "qry"), None),
        P(("neg", "qry")),
        P(("neg", "qry")),
        P("neg"),
        P(),
        P(),
        P(),
        P(),
        P(),
        P("qry", None),
    )
    out_specs = (P(("neg", "qry"), None), P("qry"))
    return jax.shard_map(
        per_device, mesh=mesh, in_specs=in_specs, out_specs=out_specs, check_vma=False
    )
```

```python
import functools
import math

import jax
import jax.numpy as jnp
from jax import lax
from jax.experimental import pallas as pl
from jax.experimental.pallas import tpu as pltpu
from jax.sharding import PartitionSpec as P


LANES = 128
ROWS = 128
DEAD = 32767
SIDE = 4
NT = (((1,), (1,)), ((), ()))
SURE = 10
LOG2E = math.log2(math.e)
MESH = pl.DeviceIdType.MESH
ORDER = (
    (2, 2), (2, 1), (2, 3), (1, 2), (3, 2), (2, 0), (0, 2), (1, 1),
    (1, 3), (3, 1), (3, 3), (1, 0), (3, 0), (0, 1), (0, 3), (0, 0),
)

NEAR = tuple((dz, c) for dz in range(SIDE) for c in (0, 1))[1:]


def sort_pairs(count):
    full = 1
    while full < count:
        full *= 2
    pairs = []
    p = 1
    while p < full:
        k = p
        while k >= 1:
            for j in range(k % p, full - k, 2 * k):
                for i in range(min(k, full - j - k)):
                    if (i + j) // (2 * p) == (i + j + k) // (2 * p):
                        if i + j + k < count:
                            pairs.append((i + j, i + j + k))
            k //= 2
        p *= 2
    return pairs


def place():
    neg, qry = lax.axis_index("neg"), lax.axis_index("qry")
    return neg // SIDE, neg % SIDE, qry // 2, qry % 2


def device(x, y, z, core):
    wrap = lambda v: lax.rem(v + 2 * SIDE, SIDE)
    return (wrap(x) * SIDE + wrap(y), wrap(z) * 2 + core)


def remote(src, dst, send, recv, target):
    return pltpu.make_async_remote_copy(
        src_ref=src, dst_ref=dst, send_sem=send, recv_sem=recv,
        device_id=target, device_id_type=MESH,
    )


def greet(peers):
    barrier = pltpu.get_barrier_semaphore()
    for peer in peers:
        pl.semaphore_signal(barrier, inc=1, device_id=peer, device_id_type=MESH)


def meet(peers):
    pl.semaphore_wait(pltpu.get_barrier_semaphore(), len(peers))


def exchange_kernel(
    pieces, slots_ref, count_ref, self_ref, fetch_ref, all_lists, all_fetch,
    lists_ref, asked_ref, sends, recvs,
):
    x, y, z, core = place()
    others = ORDER[:-1]
    greet([device(x - dx, y - dy, z, core) for dx, dy in others])
    neighbours, negatives = slots_ref.shape
    groups, half = negatives // LANES, neighbours // 2
    turn = lax.broadcasted_iota(jnp.int32, slots_ref.shape, 0)
    slots = jnp.where(turn < count_ref[...], slots_ref[...], DEAD)
    words = slots[:half] | (slots[half:] << 16)
    for k in range(half):
        for g in range(groups):
            row = k * groups + g
            lists_ref[row : row + 1, :] = words[k : k + 1, g * LANES : (g + 1) * LANES]
    lists_ref[half * groups :, :] = self_ref[...]
    for p in range(SIDE * SIDE):
        asked_ref[p] = fetch_ref[p : p + 1, :] * pieces
    meet(others)
    copies = []
    for j, (dx, dy) in enumerate(others):
        target = device(x - dx, y - dy, z, core)
        copies.append(
            remote(asked_ref.at[target[0]], all_fetch.at[j], sends.at[0, j], recvs.at[0, j], target)
        )
        copies.append(remote(lists_ref, all_lists.at[j], sends.at[1, j], recvs.at[1, j], target))
    for copy in copies:
        copy.start()
    last = len(others)
    all_fetch[last] = asked_ref[x * SIDE + y]
    all_lists[last] = lists_ref[...]
    for copy in copies:
        copy.wait()


def exchange_lists(slots, count, own, fetch, pieces):
    peers, cap = fetch.shape
    neighbours, negatives = slots.shape
    lists = ((neighbours // 2 + 1) * negatives // LANES, LANES)
    vmem = pl.BlockSpec(memory_space=pltpu.VMEM)
    return pl.pallas_call(
        functools.partial(exchange_kernel, pieces),
        out_shape=(
            jax.ShapeDtypeStruct((peers,) + lists, jnp.int32),
            jax.ShapeDtypeStruct((peers, 1, cap), fetch.dtype),
        ),
        in_specs=[vmem, vmem, vmem, vmem],
        out_specs=(vmem, vmem),
        scratch_shapes=[
            pltpu.VMEM(lists, jnp.int32),
            pltpu.VMEM((peers, 1, cap), fetch.dtype),
            pltpu.SemaphoreType.DMA((2, peers - 1)),
            pltpu.SemaphoreType.DMA((2, peers - 1)),
        ],
        compiler_params=pltpu.CompilerParams(collective_id=0, has_side_effects=True),
    )(slots, count, own, fetch)


def count_kernel(
    neighbours, cap, base_ref, index_ref, lists_ref, table_ref,
    counts_ref, own_ref, rows_ref,
    order_ref, times_ref, mine_ref, most_ref, alive_ref, self_ref, wide_ref, picked_ref,
    stage_ref, s_stage,
):
    j = pl.program_id(0)
    rows, width = table_ref.shape
    pieces = width // LANES

    loads, share = stage_ref.shape[0], stage_ref.shape[1]

    def load(i):
        return pltpu.make_async_copy(
            table_ref.at[pl.ds(i * share, share)], stage_ref.at[i], s_stage.at[i]
        )

    @pl.when(j == 0)
    def _():
        for i in range(loads):
            load(i).start()

    groups = counts_ref.shape[2] // LANES
    half = neighbours // 2
    packed = 16
    tall = 8
    batch = tall // groups
    big = jnp.int32(DEAD)

    @pl.when(lax.rem(j, batch) == 0)
    def _():
        base = base_ref[0]
        live = jnp.zeros((tall, LANES), jnp.int32)
        mine = jnp.zeros((tall, LANES), jnp.int32)

        def rows_of(k):
            return jnp.concatenate(
                [lists_ref[i, k * groups : (k + 1) * groups, :] for i in range(batch)]
            )

        words = [rows_of(k) for k in range(half)]
        places = []
        for k in range(neighbours):
            slot = words[k] & DEAD if k < half else words[k - half] >> 16
            local = slot - base
            inside = (local >= 0) & (local < cap)
            live = live + jnp.where(slot < DEAD, 1, 0)
            mine = mine + jnp.where(inside, 1, 0)
            places.append(jnp.where(inside, local, big).astype(jnp.float32))
        for a, b in sort_pairs(neighbours):
            low, high = jnp.minimum(places[a], places[b]), jnp.maximum(places[a], places[b])
            places[a], places[b] = low, high
        rows = pl.ds(pl.multiple_of(j * groups, tall), tall)
        run = jnp.ones((tall, LANES), jnp.float32)
        for k in range(neighbours):
            if k:
                run = jnp.where(places[k] == places[k - 1], run + 1.0, 1.0)
            order_ref[k, rows, :] = places[k].astype(jnp.int32)
            times_ref[k, rows, :] = run
        mine_ref[rows, :] = mine
        for i in range(batch):
            most_ref[j + i] = jnp.max(mine[i * groups : (i + 1) * groups])
        alive_ref[rows, :] = live
        own = rows_of(half) - base
        self_ref[rows, :] = jnp.where((own >= 0) & (own < cap), own, big)

    @pl.when(j == 0)
    def _():
        for i in range(loads):
            load(i).wait()

            @pl.loop(0, share // ROWS)
            def _(t):
                span = pl.ds(pl.multiple_of(t * ROWS, ROWS), ROWS)
                for c in range(pieces):
                    wide_ref[
                        pl.ds((i * share + t * ROWS) * pieces + c, ROWS, stride=pieces), :
                    ] = stage_ref[i, span, c * LANES : (c + 1) * LANES].astype(jnp.float32)

    chunk = 320 if cap % 320 == 0 else ROWS
    tiles = chunk // packed
    tile = (packed, LANES)
    iota = lax.broadcasted_iota(jnp.int32, tile, 0)

    def entry(k, row):
        slot = jnp.broadcast_to(order_ref[k, row, :], tile)
        return slot, jnp.broadcast_to(times_ref[k, row, :], tile).astype(jnp.bfloat16)

    def mark(totals, slot, times, first):
        local = (slot - first).astype(jnp.int16)
        return tuple(
            jnp.where((iota + packed * t).astype(jnp.int16) == local, times, totals[t])
            for t in range(tiles)
        )

    def spans(first):
        return [pl.ds(pl.multiple_of(first + packed * t, packed), packed) for t in range(tiles)]

    for g in range(groups):
        lanes = pl.ds(g * LANES, LANES)
        own_ref[0, 0:1, lanes] = self_ref[pl.ds(j * groups + g, 1), :]
        own_ref[0, 1:2, lanes] = alive_ref[pl.ds(j * groups + g, 1), :]

    parts = cap // chunk
    turns = groups * parts
    part = cap // turns

    burst = part // SURE
    casts = [(p, i) for i in range(part // packed) for p in range(pieces)]

    def cast(buffer, target, p, i):
        rows_ref[
            0,
            pl.ds(pl.multiple_of(target + i * packed, packed), packed),
            p * LANES : (p + 1) * LANES,
        ] = picked_ref[
            buffer, i * packed * pieces + p : (i + 1) * packed * pieces : pieces, :
        ].astype(jnp.bfloat16)

    @pl.loop(0, groups)
    def _(g):
        lanes = pl.ds(pl.multiple_of(g * LANES, LANES), LANES)
        row = pl.ds(j * groups + g, 1)
        for c in range(parts):
            turn = g * parts + c
            first = turn * part
            here, there = c % 2, 1 - c % 2
            before = lax.max(turn - 1, 0) * part
            totals = (jnp.zeros(tile, jnp.bfloat16),) * tiles
            for k in range(SURE):
                places = [
                    pl.multiple_of(index_ref[0, 0, first + k * burst + u], pieces) for u in range(burst)
                ]
                for u in range(burst):
                    into = (k * burst + u) * pieces
                    picked_ref[here, into : into + pieces, :] = wide_ref[pl.ds(places[u], pieces), :]
                totals = mark(totals, *entry(k, row), c * chunk)
                for p, i in casts[k * len(casts) // SURE : (k + 1) * len(casts) // SURE]:
                    cast(there, before, p, i)
            for span, total in zip(spans(c * chunk), totals):
                counts_ref[0, span, lanes] = total

    for p, i in casts:
        cast((turns - 1) % 2, (turns - 1) * part, p, i)

    @pl.when(most_ref[j] > SURE)
    def _():
        for g in range(groups):
            lanes = pl.ds(g * LANES, LANES)
            row = pl.ds(j * groups + g, 1)
            most = jnp.max(mine_ref[row, :])

            @pl.when(most > SURE)
            def _():
                @pl.loop(0, cap // chunk)
                def _(c):
                    totals = tuple(counts_ref[0, span, lanes] for span in spans(c * chunk))
                    totals = lax.fori_loop(
                        SURE, most, lambda k, t: mark(t, *entry(k, row), c * chunk), totals
                    )
                    for span, total in zip(spans(c * chunk), totals):
                        counts_ref[0, span, lanes] = total


def pick_and_count(base, index, lists, table, neighbours, cap):
    peers = lists.shape[0]
    groups = lists.shape[1] // (neighbours // 2 + 1)
    negatives = groups * LANES
    rows = peers * groups
    width = table.shape[1]
    pieces = width // LANES
    return pl.pallas_call(
        functools.partial(count_kernel, neighbours, cap),
        grid=(peers,),
        out_shape=(
            jax.ShapeDtypeStruct((peers, cap, negatives), jnp.bfloat16),
            jax.ShapeDtypeStruct((peers, 2, negatives), jnp.int32),
            jax.ShapeDtypeStruct((peers, cap, width), jnp.bfloat16),
        ),
        in_specs=[
            pl.BlockSpec(memory_space=pltpu.SMEM),
            pl.BlockSpec((1, 1, cap), lambda j: (j, 0, 0), memory_space=pltpu.SMEM),
            pl.BlockSpec((2,) + lists.shape[1:], lambda j: (lax.div(j, 2), 0, 0)),
            pl.BlockSpec(memory_space=pl.ANY),
        ],
        out_specs=(
            pl.BlockSpec((1, cap, negatives), lambda j: (j, 0, 0)),
            pl.BlockSpec((1, 2, negatives), lambda j: (j, 0, 0)),
            pl.BlockSpec((1, cap, width), lambda j: (j, 0, 0)),
        ),
        scratch_shapes=[
            pltpu.VMEM((neighbours, rows, LANES), jnp.int32),
            pltpu.VMEM((neighbours, rows, LANES), jnp.float32),
            pltpu.VMEM((rows, LANES), jnp.int32),
            pltpu.SMEM((peers,), jnp.int32),
            pltpu.VMEM((rows, LANES), jnp.int32),
            pltpu.VMEM((rows, LANES), jnp.int32),
            pltpu.VMEM((table.shape[0] * pieces, LANES), jnp.float32),
            pltpu.VMEM((2, cap * pieces // 8, LANES), jnp.float32),
            pltpu.VMEM((8, table.shape[0] // 8, width), table.dtype),
            pltpu.SemaphoreType.DMA((8,)),
        ],
        compiler_params=pltpu.CompilerParams(vmem_limit_bytes=62 << 20),
    )(base, index, lists, table)


def score_all(
    total_negatives, hidden_ref, around_ref, bias_ref, count_ref, live_ref,
    embed_out, lse_ref,
    embed_ref, s_embed, log_ref, mine_ref, slots_ref, merged_ref, all_ref,
    s_send1, r_send1, s_send2, r_send2,
):
    x, y, z, core = place()
    others = ORDER[:-1]
    negatives = hidden_ref.shape[0]

    def column(row_ref):
        row = row_ref[...].astype(jnp.float32)
        return jnp.broadcast_to(row, (LANES, negatives)).T

    mine = pl.ds(pl.multiple_of((2 * z + core) * negatives, negatives), negatives)
    log_ref[...] = LOG2E * jnp.log(column(count_ref.at[:, mine]))
    inverse = 1.0 / column(live_ref)[:, :1]
    hidden = jax.nn.relu(hidden_ref[...] * inverse + bias_ref[...])
    scale = lax.rsqrt(jnp.mean(hidden * hidden, axis=1, keepdims=True) + 0.25)
    embed_ref[...] = (hidden * scale).astype(jnp.bfloat16)
    tile = 256

    def score(slot, ref):
        for t in range(around_ref.shape[1] // tile):
            span = pl.ds(t * tile, tile)
            product = lax.dot_general(
                embed_ref[...], ref[span, :], NT, preferred_element_type=jnp.float32
            )
            logs = jnp.concatenate([log_ref[...]] * (tile // LANES), axis=1)
            scores = (0.25 * LOG2E) * product - logs
            peak = jnp.max(scores, axis=0, keepdims=True)
            total = jnp.sum(jnp.exp2(scores - peak), axis=0, keepdims=True)
            mine_ref[slot, :, span] = (peak + jnp.log2(total)) * (1 / LOG2E)

    def exchange1(slot):
        dz, c = lax.div(slot, 2), lax.rem(slot, 2)
        return remote(
            mine_ref.at[slot], slots_ref.at[slot], s_send1.at[slot], r_send1.at[slot],
            device(x, y, z + dz, lax.rem(core + c, 2)),
        )

    @pl.loop(0, 8)
    def _(turn):
        slot = jnp.int32(0)
        for i, chosen in enumerate((4, 5, 2, 3, 6, 7, 1)):
            slot = lax.select(turn == i, jnp.int32(chosen), slot)

        score(slot, around_ref.at[slot])

        @pl.when(turn < 7)
        def _():
            exchange1(slot).start()

    embed_copy = pltpu.make_async_copy(embed_ref, embed_out, s_embed)
    embed_copy.start()
    slots_ref[0] = mine_ref[0]
    for slot in range(1, 8):
        exchange1(slot).wait_recv()

    def merge(ref, count):
        values = [ref[i] for i in range(count)]
        top = functools.reduce(jnp.maximum, values)
        return top + jnp.log(sum(jnp.exp(v - top) for v in values))

    merged_ref[...] = merge(slots_ref, 8)

    def exchange2(j):
        dx, dy = others[j]
        return remote(
            merged_ref, all_ref.at[j], s_send2.at[j], r_send2.at[j], device(x - dx, y - dy, z, core)
        )

    for j in range(len(others)):
        exchange2(j).start()
    all_ref[len(others)] = merged_ref[...]
    for j in range(len(others)):
        exchange2(j).wait_recv()
    lse_ref[...] = merge(all_ref, len(others) + 1) - math.log(total_negatives)
    embed_copy.wait()
    for slot in range(1, 8):
        exchange1(slot).wait_send()
    for j in range(len(others)):
        exchange2(j).wait_send()


def reduce_kernel(
    total_negatives,
    rows_ref, counts_ref, own_ref, wm_ref, mb_ref, ws_ref, wn_ref,
    queries_ref, bias_ref, count_ref, live_ref, embed_out, lse_ref,
    around_ref, hot_ref, message_ref, from_ref, into_ref, total_ref, part_ref,
    relay1, full1, relay2, full2,
    s_relay1, r_relay1, s_full1, r_full1, s_relay2, r_relay2, s_full2, r_full2,
    s_query, r_query, s_own,
    *score_refs,
):
    step = pl.program_id(0)
    x, y, z, core = place()
    _, cap, width = rows_ref.shape
    negatives = counts_ref.shape[2]
    groups = negatives // LANES
    half, quarter = negatives // 2, negatives // 4
    packed = 16

    def neighbour(axis, sign):
        if axis == 0:
            return device(x + sign, y, z, core)
        return device(x, y + sign, z, core)

    up, down, sibling = device(x, y, z + 1, core), device(x, y, z - 1, core), device(x, y, z, 1 - core)
    upper = pl.ds(0, queries_ref.shape[0] // 2)
    lower = pl.ds(queries_ref.shape[0] // 2, queries_ref.shape[0] // 2)

    def query_copy(which):
        sem = (s_query.at[which], r_query.at[which])
        if which == 0:
            return remote(queries_ref, around_ref.at[6], *sem, up)
        if which == 1:
            return remote(queries_ref, around_ref.at[2], *sem, down)
        if which == 2:
            return remote(queries_ref, around_ref.at[1], *sem, sibling)
        if which == 3:
            return remote(around_ref.at[6, upper], around_ref.at[4, upper], *sem, up)
        if which == 4:
            return remote(around_ref.at[2, lower], around_ref.at[4, lower], *sem, down)
        slot = {5: 6, 6: 2, 7: 4}[which]
        return remote(around_ref.at[slot], around_ref.at[slot + 1], *sem, sibling)

    @pl.when(step == 0)
    def _():
        greet(
            [device(x, y, z - dz, lax.rem(core + c, 2)) for dz, c in NEAR]
            + [device(x - dx, y - dy, z, core) for dx, dy in ORDER[:-1]]
        )
        pltpu.make_async_copy(queries_ref, around_ref.at[0], s_own).start()

    tile = (packed, LANES)
    iota = lax.broadcasted_iota(jnp.int32, tile, 0)
    heres = [(iota + i * packed).astype(jnp.int16) for i in range(cap // packed)]
    zero = jnp.zeros(tile, jnp.bfloat16)
    for g in range(groups):
        lanes = pl.ds(g * LANES, LANES)
        own = jnp.broadcast_to(own_ref[0, 0:1, lanes], tile).astype(jnp.int16)
        live = jnp.broadcast_to(own_ref[0, 1:2, lanes].astype(jnp.float32), tile).astype(jnp.bfloat16)
        for i, here in enumerate(heres):
            hot_ref[i * packed : (i + 1) * packed, lanes] = jnp.where(here == own, live, zero)

    columns = [slice(c, c + width // 2) for c in (0, width // 2)]
    into_ref[:, :cap] = counts_ref[0].T
    into_ref[:, cap:] = hot_ref[...].T

    def dot(a, b):
        return jnp.dot(a, b, preferred_element_type=jnp.float32)

    for s in columns:
        message_ref[:, s] = jax.nn.relu(dot(rows_ref[0], wm_ref[:, s]) + mb_ref[:, s]).astype(
            jnp.bfloat16
        )
        from_ref[cap:, s] = dot(rows_ref[0], ws_ref[:, s]).astype(jnp.bfloat16)
    for s in columns:
        from_ref[:cap, s] = dot(message_ref[...], wn_ref[:, s]).astype(jnp.bfloat16)
    for s in columns:
        part_ref[step, :, s] = dot(into_ref[...], from_ref[:, s]).astype(jnp.bfloat16)

    @pl.when(step == 0)
    def _():
        meet(NEAR + ORDER[:-1])
        for which in range(3):
            query_copy(which).start()

    @pl.when(step == 9)
    def _():
        for which in (0, 1):
            query_copy(which).wait_recv()
        for which in (3, 4, 5, 6):
            query_copy(which).start()

    @pl.when(step == 14)
    def _():
        for which in (3, 4):
            query_copy(which).wait_recv()
        query_copy(7).start()

    block = 64
    last = len(ORDER) - 1

    def combine(j, first, count, sources):
        @pl.loop(0, count // block)
        def _(i):
            span = pl.ds(pl.multiple_of(first + i * block, block), block)
            value = part_ref[j, span, :].astype(jnp.float32)
            for source, begin in sources:
                value = value + source[
                    pl.ds(pl.multiple_of(begin + i * block, block), block), :
                ].astype(jnp.float32)
            if j == last:
                total_ref[span, :] = value
            else:
                part_ref[j, span, :] = value.astype(jnp.bfloat16)

    def relay_copy(j, first, axis, side, relay, send, recv, at):
        return remote(
            part_ref.at[j, pl.ds(first + side * quarter, quarter)],
            relay.at[(*at, side)], send.at[(*at, side)], recv.at[(*at, side)],
            neighbour(axis, 1 - 2 * side),
        )

    def full_copy(j, first, axis, side, full, send, recv, at):
        return remote(
            part_ref.at[j, pl.ds(first, half)],
            full.at[(*at, side)], send.at[(*at, side)], recv.at[(*at, side)],
            neighbour(axis, 1 - 2 * side),
        )

    def arrive(j, first, axis, offset, bufs, at):
        relay, full, s_relay, r_relay, s_full, r_full = bufs
        into = [[], []]
        if offset in (1, 3):
            side = 0 if offset == 1 else 1
            relay_copy(j, first, axis, side, relay, s_relay, r_relay, at).wait_recv()
            into[side].append((relay.at[(*at, side)], 0))
        elif offset == 0:
            for side in (0, 1):
                full_copy(j, first, axis, side, full, s_full, r_full, at).wait_recv()
                for q in (0, 1):
                    into[q].append((full.at[(*at, side)], q * quarter))
        return into

    def leave(j, first, axis, offset, bufs, at):
        relay, full, s_relay, r_relay, s_full, r_full = bufs
        if offset == 2:
            for side in (0, 1):
                relay_copy(j, first, axis, side, relay, s_relay, r_relay, at).start()
        elif offset in (1, 3):
            side = 0 if offset == 1 else 1
            full_copy(j, first, axis, side, full, s_full, r_full, at).start()

    stage1 = (relay1, full1, s_relay1, r_relay1, s_full1, r_full1)
    stage2 = (relay2, full2, s_relay2, r_relay2, s_full2, r_full2)
    for j, offsets in enumerate(ORDER):

        @pl.when(step == j)
        def _(j=j, offsets=offsets):
            for h in sorted((0, 1), key=lambda h: offsets[h] == 0):
                first = h * half
                near, far = offsets[h], offsets[1 - h]
                into = arrive(j, first, h, near, stage1, (h, far))
                out = (j, first, h, near, stage1, (h, far))
                if near == 0:
                    out = (j, first, 1 - h, far, stage2, (h,))
                    into = [a + b for a, b in zip(into, arrive(*out))]
                for q in (0, 1):
                    if into[q]:
                        combine(j, first + q * quarter, quarter, into[q])
                leave(*out)

    @pl.when(step == len(ORDER) - 1)
    def _():
        for which in (2, 5, 6, 7):
            query_copy(which).wait_recv()
        pltpu.make_async_copy(queries_ref, around_ref.at[0], s_own).wait()
        score_all(
            total_negatives, total_ref, around_ref, bias_ref, count_ref, live_ref,
            embed_out, lse_ref, *score_refs,
        )
        for j, offsets in enumerate(ORDER):
            for h in (0, 1):
                first = h * half
                near, far = offsets[h], offsets[1 - h]
                stages = [(near, h, stage1, (h, far))]
                if near == 0:
                    stages.append((far, 1 - h, stage2, (h,)))
                for offset, axis, bufs, at in stages:
                    relay, full, s_relay, r_relay, s_full, r_full = bufs
                    if offset == 2:
                        for side in (0, 1):
                            relay_copy(j, first, axis, side, relay, s_relay, r_relay, at).wait_send()
                    elif offset in (1, 3):
                        side = 0 if offset == 1 else 1
                        full_copy(j, first, axis, side, full, s_full, r_full, at).wait_send()
        for which in range(8):
            query_copy(which).wait_send()


def reduce_and_score(
    picked, counts, own, wm, mb, ws, wn, queries, bias, count, live, total_negatives
):
    peers, cap, negatives = counts.shape
    width = picked.shape[2]
    half, quarter = negatives // 2, negatives // 4
    vmem = pl.BlockSpec(memory_space=pltpu.VMEM)
    hbm = pl.BlockSpec(memory_space=pl.ANY)
    dma = pltpu.SemaphoreType.DMA
    bf16, f32 = jnp.bfloat16, jnp.float32
    return pl.pallas_call(
        functools.partial(reduce_kernel, total_negatives),
        grid=(peers,),
        out_shape=(
            jax.ShapeDtypeStruct((negatives, width), bf16),
            jax.ShapeDtypeStruct((1, queries.shape[0]), f32),
        ),
        in_specs=[
            pl.BlockSpec((1, cap, width), lambda j: (j, 0, 0)),
            pl.BlockSpec((1, cap, negatives), lambda j: (j, 0, 0)),
            pl.BlockSpec((1, 2, negatives), lambda j: (j, 0, 0)),
            vmem, vmem, vmem, vmem,
            hbm, vmem, vmem, vmem,
        ],
        out_specs=(hbm, vmem),
        scratch_shapes=[
            pltpu.VMEM((8,) + queries.shape, bf16),
            pltpu.VMEM((cap, negatives), bf16),
            pltpu.VMEM((cap, width), bf16),
            pltpu.VMEM((2 * cap, width), bf16),
            pltpu.VMEM((negatives, 2 * cap), bf16),
            pltpu.VMEM((negatives, width), f32),
            pltpu.VMEM((peers, negatives, width), bf16),
            pltpu.VMEM((2, SIDE, 2, quarter, width), bf16),
            pltpu.VMEM((2, SIDE, 2, half, width), bf16),
            pltpu.VMEM((2, 2, quarter, width), bf16),
            pltpu.VMEM((2, 2, half, width), bf16),
            dma((2, SIDE, 2)), dma((2, SIDE, 2)), dma((2, SIDE, 2)), dma((2, SIDE, 2)),
            dma((2, 2)), dma((2, 2)), dma((2, 2)), dma((2, 2)),
            dma((8,)), dma((8,)), dma,
            pltpu.VMEM((negatives, width), bf16),
            dma,
            pltpu.VMEM((negatives, LANES), f32),
            pltpu.VMEM((8, 1, queries.shape[0]), f32),
            pltpu.VMEM((8, 1, queries.shape[0]), f32),
            pltpu.VMEM((1, queries.shape[0]), f32),
            pltpu.VMEM((peers, 1, queries.shape[0]), f32),
            dma((8,)), dma((8,)), dma((15,)), dma((15,)),
        ],
        compiler_params=pltpu.CompilerParams(
            collective_id=1, has_side_effects=True, vmem_limit_bytes=62 << 20
        ),
    )(picked, counts, own, wm, mb, ws, wn, queries, bias, count, live)


def hand_out_kernel(embed_ref, lse_ref, embed_out, lse_out):
    embed_out[...] = embed_ref[...]
    lse_out[...] = lse_ref[...]


def hand_out(embed, lse):
    vmem = pl.BlockSpec(memory_space=pltpu.VMEM)
    return pl.pallas_call(
        hand_out_kernel,
        out_shape=[jax.ShapeDtypeStruct(a.shape, a.dtype) for a in (embed, lse)],
        in_specs=[vmem, vmem],
        out_specs=[vmem, vmem],
    )(embed, lse)


def per_device(
    items_table,
    fetch_rows,
    neighbour_slots,
    neighbour_count,
    self_slot,
    negative_count,
    message_weight,
    message_bias,
    self_weight,
    neighbour_weight,
    output_bias,
    queries,
):
    n_neg, n_qry = lax.axis_size("neg"), lax.axis_size("qry")
    own_neg = lax.axis_index("neg")
    cap = fetch_rows.shape[1]
    negatives, neighbours = neighbour_slots.shape

    assert n_neg * cap < DEAD and neighbours % 4 == 0 and n_neg == SIDE * SIDE and n_qry == 8
    all_lists, all_fetch = exchange_lists(
        neighbour_slots.T, neighbour_count[None, :], self_slot.reshape(-1, LANES), fetch_rows,
        items_table.shape[1] // LANES,
    )
    base = (own_neg * cap).astype(jnp.int32).reshape(1)
    counts, own, picked = pick_and_count(
        base, all_fetch, all_lists, items_table, neighbours, cap
    )
    negative_embed, query_lse = reduce_and_score(
        picked, counts, own,
        message_weight, message_bias[None, :], self_weight, neighbour_weight, queries,
        output_bias[None, :], negative_count[None, :], neighbour_count[None, :],
        negatives * n_neg * n_qry,
    )
    negative_embed, query_lse = hand_out(negative_embed, query_lse)
    return (negative_embed, query_lse.reshape(-1))


def solution(mesh):
    in_specs = (
        P("neg", None),
        P(("neg", "qry"), None),
        P(("neg", "qry"), None),
        P(("neg", "qry")),
        P(("neg", "qry")),
        P("neg"),
        P(),
        P(),
        P(),
        P(),
        P(),
        P("qry", None),
    )
    out_specs = (P(("neg", "qry"), None), P("qry"))
    return jax.shard_map(
        per_device, mesh=mesh, in_specs=in_specs, out_specs=out_specs, check_vma=False
    )
```

```python
import functools
import math

import jax
import jax.numpy as jnp
from jax import lax
from jax.experimental import pallas as pl
from jax.experimental.pallas import tpu as pltpu
from jax.sharding import PartitionSpec as P


LANES = 128
ROWS = 128
DEAD = 32767
SIDE = 4
NT = (((1,), (1,)), ((), ()))
SURE = 10
LOG2E = math.log2(math.e)
MESH = pl.DeviceIdType.MESH
ORDER = (
    (2, 2), (2, 1), (2, 3), (1, 2), (3, 2), (2, 0), (0, 2), (1, 1),
    (1, 3), (3, 1), (3, 3), (1, 0), (3, 0), (0, 1), (0, 3), (0, 0),
)

NEAR = tuple((dz, c) for dz in range(SIDE) for c in (0, 1))[1:]


def sort_pairs(count):
    full = 1
    while full < count:
        full *= 2
    pairs = []
    p = 1
    while p < full:
        k = p
        while k >= 1:
            for j in range(k % p, full - k, 2 * k):
                for i in range(min(k, full - j - k)):
                    if (i + j) // (2 * p) == (i + j + k) // (2 * p):
                        if i + j + k < count:
                            pairs.append((i + j, i + j + k))
            k //= 2
        p *= 2
    return pairs


def place():
    neg, qry = lax.axis_index("neg"), lax.axis_index("qry")
    return neg // SIDE, neg % SIDE, qry // 2, qry % 2


def device(x, y, z, core):
    wrap = lambda v: lax.rem(v + 2 * SIDE, SIDE)
    return (wrap(x) * SIDE + wrap(y), wrap(z) * 2 + core)


def remote(src, dst, send, recv, target):
    return pltpu.make_async_remote_copy(
        src_ref=src, dst_ref=dst, send_sem=send, recv_sem=recv,
        device_id=target, device_id_type=MESH,
    )


def greet(peers):
    barrier = pltpu.get_barrier_semaphore()
    for peer in peers:
        pl.semaphore_signal(barrier, inc=1, device_id=peer, device_id_type=MESH)


def meet(peers):
    pl.semaphore_wait(pltpu.get_barrier_semaphore(), len(peers))


def exchange_kernel(
    pieces, slots_ref, count_ref, self_ref, fetch_ref, all_lists, all_fetch,
    lists_ref, asked_ref, sends, recvs,
):
    x, y, z, core = place()
    others = ORDER[:-1]
    greet([device(x - dx, y - dy, z, core) for dx, dy in others])
    neighbours, negatives = slots_ref.shape
    groups, half = negatives // LANES, neighbours // 2
    turn = lax.broadcasted_iota(jnp.int32, slots_ref.shape, 0)
    slots = jnp.where(turn < count_ref[...], slots_ref[...], DEAD)
    words = slots[:half] | (slots[half:] << 16)
    for k in range(half):
        for g in range(groups):
            row = k * groups + g
            lists_ref[row : row + 1, :] = words[k : k + 1, g * LANES : (g + 1) * LANES]
    lists_ref[half * groups :, :] = self_ref[...]
    for p in range(SIDE * SIDE):
        asked_ref[p] = fetch_ref[p : p + 1, :] * pieces
    meet(others)
    copies = []
    for j, (dx, dy) in enumerate(others):
        target = device(x - dx, y - dy, z, core)
        copies.append(
            remote(asked_ref.at[target[0]], all_fetch.at[j], sends.at[0, j], recvs.at[0, j], target)
        )
        copies.append(remote(lists_ref, all_lists.at[j], sends.at[1, j], recvs.at[1, j], target))
    for copy in copies:
        copy.start()
    last = len(others)
    all_fetch[last] = asked_ref[x * SIDE + y]
    all_lists[last] = lists_ref[...]
    for copy in copies:
        copy.wait()


def exchange_lists(slots, count, own, fetch, pieces):
    peers, cap = fetch.shape
    neighbours, negatives = slots.shape
    lists = ((neighbours // 2 + 1) * negatives // LANES, LANES)
    vmem = pl.BlockSpec(memory_space=pltpu.VMEM)
    return pl.pallas_call(
        functools.partial(exchange_kernel, pieces),
        out_shape=(
            jax.ShapeDtypeStruct((peers,) + lists, jnp.int32),
            jax.ShapeDtypeStruct((peers, 1, cap), fetch.dtype),
        ),
        in_specs=[vmem, vmem, vmem, vmem],
        out_specs=(vmem, vmem),
        scratch_shapes=[
            pltpu.VMEM(lists, jnp.int32),
            pltpu.VMEM((peers, 1, cap), fetch.dtype),
            pltpu.SemaphoreType.DMA((2, peers - 1)),
            pltpu.SemaphoreType.DMA((2, peers - 1)),
        ],
        compiler_params=pltpu.CompilerParams(collective_id=0, has_side_effects=True),
    )(slots, count, own, fetch)


def count_kernel(
    neighbours, cap, base_ref, index_ref, lists_ref, table_ref,
    counts_ref, own_ref, rows_ref,
    order_ref, times_ref, mine_ref, most_ref, alive_ref, self_ref, wide_ref, picked_ref,
    stage_ref, s_stage,
):
    j = pl.program_id(0)
    rows, width = table_ref.shape
    pieces = width // LANES

    loads, share = stage_ref.shape[0], stage_ref.shape[1]

    def load(i):
        return pltpu.make_async_copy(
            table_ref.at[pl.ds(i * share, share)], stage_ref.at[i], s_stage.at[i]
        )

    @pl.when(j == 0)
    def _():
        for i in range(loads):
            load(i).start()

    groups = counts_ref.shape[2] // LANES
    half = neighbours // 2
    packed = 16
    tall = 8
    batch = tall // groups
    big = jnp.int32(DEAD)

    @pl.when(lax.rem(j, batch) == 0)
    def _():
        base = base_ref[0]
        live = jnp.zeros((tall, LANES), jnp.int32)
        mine = jnp.zeros((tall, LANES), jnp.int32)

        def rows_of(k):
            return jnp.concatenate(
                [lists_ref[i, k * groups : (k + 1) * groups, :] for i in range(batch)]
            )

        words = [rows_of(k) for k in range(half)]
        places = []
        for k in range(neighbours):
            slot = words[k] & DEAD if k < half else words[k - half] >> 16
            local = slot - base
            inside = (local >= 0) & (local < cap)
            live = live + jnp.where(slot < DEAD, 1, 0)
            mine = mine + jnp.where(inside, 1, 0)
            places.append(jnp.where(inside, local, big).astype(jnp.float32))
        for a, b in sort_pairs(neighbours):
            low, high = jnp.minimum(places[a], places[b]), jnp.maximum(places[a], places[b])
            places[a], places[b] = low, high
        rows = pl.ds(pl.multiple_of(j * groups, tall), tall)
        run = jnp.ones((tall, LANES), jnp.float32)
        for k in range(neighbours):
            if k:
                run = jnp.where(places[k] == places[k - 1], run + 1.0, 1.0)
            order_ref[k, rows, :] = places[k].astype(jnp.int32)
            times_ref[k, rows, :] = run
        mine_ref[rows, :] = mine
        for i in range(batch):
            most_ref[j + i] = jnp.max(mine[i * groups : (i + 1) * groups])
        alive_ref[rows, :] = live
        own = rows_of(half) - base
        self_ref[rows, :] = jnp.where((own >= 0) & (own < cap), own, big)

    @pl.when(j == 0)
    def _():
        for i in range(loads):
            load(i).wait()

            @pl.loop(0, share // ROWS)
            def _(t):
                span = pl.ds(pl.multiple_of(t * ROWS, ROWS), ROWS)
                for c in range(pieces):
                    wide_ref[
                        pl.ds((i * share + t * ROWS) * pieces + c, ROWS, stride=pieces), :
                    ] = stage_ref[i, span, c * LANES : (c + 1) * LANES].astype(jnp.float32)

    chunk = 320 if cap % 320 == 0 else ROWS
    tiles = chunk // packed
    tile = (packed, LANES)
    iota = lax.broadcasted_iota(jnp.int32, tile, 0)

    def entry(k, row):
        slot = jnp.broadcast_to(order_ref[k, row, :], tile)
        return slot, jnp.broadcast_to(times_ref[k, row, :], tile).astype(jnp.bfloat16)

    def mark(totals, slot, times, first):
        local = (slot - first).astype(jnp.int16)
        return tuple(
            jnp.where((iota + packed * t).astype(jnp.int16) == local, times, totals[t])
            for t in range(tiles)
        )

    def spans(first):
        return [pl.ds(pl.multiple_of(first + packed * t, packed), packed) for t in range(tiles)]

    for g in range(groups):
        lanes = pl.ds(g * LANES, LANES)
        own_ref[0, 0:1, lanes] = self_ref[pl.ds(j * groups + g, 1), :]
        own_ref[0, 1:2, lanes] = alive_ref[pl.ds(j * groups + g, 1), :]

    parts = cap // chunk
    turns = groups * parts
    part = cap // turns

    burst = part // SURE
    casts = [(p, i) for i in range(part // packed) for p in range(pieces)]

    def cast(buffer, target, p, i):
        rows_ref[
            0,
            pl.ds(pl.multiple_of(target + i * packed, packed), packed),
            p * LANES : (p + 1) * LANES,
        ] = picked_ref[
            buffer, i * packed * pieces + p : (i + 1) * packed * pieces : pieces, :
        ].astype(jnp.bfloat16)

    @pl.loop(0, groups)
    def _(g):
        lanes = pl.ds(pl.multiple_of(g * LANES, LANES), LANES)
        row = pl.ds(j * groups + g, 1)
        for c in range(parts):
            turn = g * parts + c
            first = turn * part
            here, there = c % 2, 1 - c % 2
            before = lax.max(turn - 1, 0) * part
            totals = (jnp.zeros(tile, jnp.bfloat16),) * tiles
            for k in range(SURE):
                places = [
                    pl.multiple_of(index_ref[0, 0, first + k * burst + u], pieces) for u in range(burst)
                ]
                for u in range(burst):
                    into = (k * burst + u) * pieces
                    picked_ref[here, into : into + pieces, :] = wide_ref[pl.ds(places[u], pieces), :]
                totals = mark(totals, *entry(k, row), c * chunk)
                for p, i in casts[k * len(casts) // SURE : (k + 1) * len(casts) // SURE]:
                    cast(there, before, p, i)
            for span, total in zip(spans(c * chunk), totals):
                counts_ref[0, span, lanes] = total

    for p, i in casts:
        cast((turns - 1) % 2, (turns - 1) * part, p, i)

    @pl.when(most_ref[j] > SURE)
    def _():
        for g in range(groups):
            lanes = pl.ds(g * LANES, LANES)
            row = pl.ds(j * groups + g, 1)
            most = jnp.max(mine_ref[row, :])

            @pl.when(most > SURE)
            def _():
                @pl.loop(0, cap // chunk)
                def _(c):
                    totals = tuple(counts_ref[0, span, lanes] for span in spans(c * chunk))
                    totals = lax.fori_loop(
                        SURE, most, lambda k, t: mark(t, *entry(k, row), c * chunk), totals
                    )
                    for span, total in zip(spans(c * chunk), totals):
                        counts_ref[0, span, lanes] = total


def pick_and_count(base, index, lists, table, neighbours, cap):
    peers = lists.shape[0]
    groups = lists.shape[1] // (neighbours // 2 + 1)
    negatives = groups * LANES
    rows = peers * groups
    width = table.shape[1]
    pieces = width // LANES
    return pl.pallas_call(
        functools.partial(count_kernel, neighbours, cap),
        grid=(peers,),
        out_shape=(
            jax.ShapeDtypeStruct((peers, cap, negatives), jnp.bfloat16),
            jax.ShapeDtypeStruct((peers, 2, negatives), jnp.int32),
            jax.ShapeDtypeStruct((peers, cap, width), jnp.bfloat16),
        ),
        in_specs=[
            pl.BlockSpec(memory_space=pltpu.SMEM),
            pl.BlockSpec((1, 1, cap), lambda j: (j, 0, 0), memory_space=pltpu.SMEM),
            pl.BlockSpec((2,) + lists.shape[1:], lambda j: (lax.div(j, 2), 0, 0)),
            pl.BlockSpec(memory_space=pl.ANY),
        ],
        out_specs=(
            pl.BlockSpec((1, cap, negatives), lambda j: (j, 0, 0)),
            pl.BlockSpec((1, 2, negatives), lambda j: (j, 0, 0)),
            pl.BlockSpec((1, cap, width), lambda j: (j, 0, 0)),
        ),
        scratch_shapes=[
            pltpu.VMEM((neighbours, rows, LANES), jnp.int32),
            pltpu.VMEM((neighbours, rows, LANES), jnp.float32),
            pltpu.VMEM((rows, LANES), jnp.int32),
            pltpu.SMEM((peers,), jnp.int32),
            pltpu.VMEM((rows, LANES), jnp.int32),
            pltpu.VMEM((rows, LANES), jnp.int32),
            pltpu.VMEM((table.shape[0] * pieces, LANES), jnp.float32),
            pltpu.VMEM((2, cap * pieces // 8, LANES), jnp.float32),
            pltpu.VMEM((8, table.shape[0] // 8, width), table.dtype),
            pltpu.SemaphoreType.DMA((8,)),
        ],
        compiler_params=pltpu.CompilerParams(vmem_limit_bytes=62 << 20),
    )(base, index, lists, table)


def score_all(
    total_negatives, hidden_ref, around_ref, bias_ref, count_ref, live_ref,
    embed_out, lse_ref,
    embed_ref, s_embed, log_ref, mine_ref, slots_ref, merged_ref, all_ref,
    s_send1, r_send1, s_send2, r_send2,
):
    x, y, z, core = place()
    others = ORDER[:-1]
    negatives = hidden_ref.shape[0]

    def column(row_ref):
        row = row_ref[...].astype(jnp.float32)
        return jnp.broadcast_to(row, (LANES, negatives)).T

    mine = pl.ds(pl.multiple_of((2 * z + core) * negatives, negatives), negatives)
    log_ref[...] = LOG2E * jnp.log(column(count_ref.at[:, mine]))
    inverse = 1.0 / column(live_ref)[:, :1]
    hidden = jax.nn.relu(hidden_ref[...] * inverse + bias_ref[...])
    scale = lax.rsqrt(jnp.mean(hidden * hidden, axis=1, keepdims=True) + 0.25)
    embed_ref[...] = (hidden * scale).astype(jnp.bfloat16)
    tile = 256

    def score(slot, ref):
        for t in range(around_ref.shape[1] // tile):
            span = pl.ds(t * tile, tile)
            product = lax.dot_general(
                embed_ref[...], ref[span, :], NT, preferred_element_type=jnp.float32
            )
            logs = jnp.concatenate([log_ref[...]] * (tile // LANES), axis=1)
            scores = (0.25 * LOG2E) * product - logs
            peak = jnp.max(scores, axis=0, keepdims=True)
            total = jnp.sum(jnp.exp2(scores - peak), axis=0, keepdims=True)
            mine_ref[slot, :, span] = (peak + jnp.log2(total)) * (1 / LOG2E)

    def exchange1(slot):
        dz, c = lax.div(slot, 2), lax.rem(slot, 2)
        return remote(
            mine_ref.at[slot], slots_ref.at[slot], s_send1.at[slot], r_send1.at[slot],
            device(x, y, z + dz, lax.rem(core + c, 2)),
        )

    @pl.loop(0, 8)
    def _(turn):
        slot = jnp.int32(0)
        for i, chosen in enumerate((4, 5, 2, 3, 6, 7, 1)):
            slot = lax.select(turn == i, jnp.int32(chosen), slot)

        score(slot, around_ref.at[slot])

        @pl.when(turn < 7)
        def _():
            exchange1(slot).start()

    embed_copy = pltpu.make_async_copy(embed_ref, embed_out, s_embed)
    embed_copy.start()
    slots_ref[0] = mine_ref[0]
    for slot in range(1, 8):
        exchange1(slot).wait_recv()

    def merge(ref, count):
        values = [ref[i] for i in range(count)]
        top = functools.reduce(jnp.maximum, values)
        return top + jnp.log(sum(jnp.exp(v - top) for v in values))

    merged_ref[...] = merge(slots_ref, 8)

    def exchange2(j):
        dx, dy = others[j]
        return remote(
            merged_ref, all_ref.at[j], s_send2.at[j], r_send2.at[j], device(x - dx, y - dy, z, core)
        )

    for j in range(len(others)):
        exchange2(j).start()
    all_ref[len(others)] = merged_ref[...]
    for j in range(len(others)):
        exchange2(j).wait_recv()
    lse_ref[...] = merge(all_ref, len(others) + 1) - math.log(total_negatives)
    embed_copy.wait()
    for slot in range(1, 8):
        exchange1(slot).wait_send()
    for j in range(len(others)):
        exchange2(j).wait_send()


def reduce_kernel(
    total_negatives,
    rows_ref, counts_ref, own_ref, wm_ref, mb_ref, ws_ref, wn_ref,
    queries_ref, bias_ref, count_ref, live_ref, embed_out, lse_ref,
    around_ref, hot_ref, message_ref, from_ref, into_ref, total_ref, part_ref,
    relay1, full1, relay2, full2,
    s_relay1, r_relay1, s_full1, r_full1, s_relay2, r_relay2, s_full2, r_full2,
    s_query, r_query, s_own,
    *score_refs,
):
    step = pl.program_id(0)
    x, y, z, core = place()
    _, cap, width = rows_ref.shape
    negatives = counts_ref.shape[2]
    groups = negatives // LANES
    half, quarter = negatives // 2, negatives // 4
    packed = 16

    def neighbour(axis, sign):
        if axis == 0:
            return device(x + sign, y, z, core)
        return device(x, y + sign, z, core)

    up, down, sibling = device(x, y, z + 1, core), device(x, y, z - 1, core), device(x, y, z, 1 - core)
    upper = pl.ds(0, queries_ref.shape[0] // 2)
    lower = pl.ds(queries_ref.shape[0] // 2, queries_ref.shape[0] // 2)

    def query_copy(which):
        sem = (s_query.at[which], r_query.at[which])
        if which == 0:
            return remote(queries_ref, around_ref.at[6], *sem, up)
        if which == 1:
            return remote(queries_ref, around_ref.at[2], *sem, down)
        if which == 2:
            return remote(queries_ref, around_ref.at[1], *sem, sibling)
        if which == 3:
            return remote(around_ref.at[6, upper], around_ref.at[4, upper], *sem, up)
        if which == 4:
            return remote(around_ref.at[2, lower], around_ref.at[4, lower], *sem, down)
        slot = {5: 6, 6: 2, 7: 4}[which]
        return remote(around_ref.at[slot], around_ref.at[slot + 1], *sem, sibling)

    @pl.when(step == 0)
    def _():
        greet(
            [device(x, y, z - dz, lax.rem(core + c, 2)) for dz, c in NEAR]
            + [device(x - dx, y - dy, z, core) for dx, dy in ORDER[:-1]]
        )
        pltpu.make_async_copy(queries_ref, around_ref.at[0], s_own).start()

    tile = (packed, LANES)
    iota = lax.broadcasted_iota(jnp.int32, tile, 0)
    heres = [(iota + i * packed).astype(jnp.int16) for i in range(cap // packed)]
    zero = jnp.zeros(tile, jnp.bfloat16)
    for g in range(groups):
        lanes = pl.ds(g * LANES, LANES)
        own = jnp.broadcast_to(own_ref[0, 0:1, lanes], tile).astype(jnp.int16)
        live = jnp.broadcast_to(own_ref[0, 1:2, lanes].astype(jnp.float32), tile).astype(jnp.bfloat16)
        for i, here in enumerate(heres):
            hot_ref[i * packed : (i + 1) * packed, lanes] = jnp.where(here == own, live, zero)

    columns = [slice(c, c + width // 2) for c in (0, width // 2)]
    into_ref[:, :cap] = counts_ref[0].T
    into_ref[:, cap:] = hot_ref[...].T

    def dot(a, b):
        return jnp.dot(a, b, preferred_element_type=jnp.float32)

    for s in columns:
        message_ref[:, s] = jax.nn.relu(dot(rows_ref[0], wm_ref[:, s]) + mb_ref[:, s]).astype(
            jnp.bfloat16
        )
        from_ref[cap:, s] = dot(rows_ref[0], ws_ref[:, s]).astype(jnp.bfloat16)
    for s in columns:
        from_ref[:cap, s] = dot(message_ref[...], wn_ref[:, s]).astype(jnp.bfloat16)
    for s in columns:
        part_ref[step, :, s] = dot(into_ref[...], from_ref[:, s]).astype(jnp.bfloat16)

    @pl.when(step == 0)
    def _():
        meet(NEAR + ORDER[:-1])
        for which in range(3):
            query_copy(which).start()

    @pl.when(step == 9)
    def _():
        for which in (0, 1):
            query_copy(which).wait_recv()
        for which in (3, 4, 5, 6):
            query_copy(which).start()

    @pl.when(step == 14)
    def _():
        for which in (3, 4):
            query_copy(which).wait_recv()
        query_copy(7).start()

    block = 128
    last = len(ORDER) - 1

    def combine(j, first, count, sources):
        @pl.loop(0, count // block)
        def _(i):
            span = pl.ds(pl.multiple_of(first + i * block, block), block)
            value = part_ref[j, span, :].astype(jnp.float32)
            for source, begin in sources:
                value = value + source[
                    pl.ds(pl.multiple_of(begin + i * block, block), block), :
                ].astype(jnp.float32)
            if j == last:
                total_ref[span, :] = value
            else:
                part_ref[j, span, :] = value.astype(jnp.bfloat16)

    def relay_copy(j, first, axis, side, relay, send, recv, at):
        return remote(
            part_ref.at[j, pl.ds(first + side * quarter, quarter)],
            relay.at[(*at, side)], send.at[(*at, side)], recv.at[(*at, side)],
            neighbour(axis, 1 - 2 * side),
        )

    def full_copy(j, first, axis, side, full, send, recv, at):
        return remote(
            part_ref.at[j, pl.ds(first, half)],
            full.at[(*at, side)], send.at[(*at, side)], recv.at[(*at, side)],
            neighbour(axis, 1 - 2 * side),
        )

    def arrive(j, first, axis, offset, bufs, at):
        relay, full, s_relay, r_relay, s_full, r_full = bufs
        into = [[], []]
        if offset in (1, 3):
            side = 0 if offset == 1 else 1
            relay_copy(j, first, axis, side, relay, s_relay, r_relay, at).wait_recv()
            into[side].append((relay.at[(*at, side)], 0))
        elif offset == 0:
            for side in (0, 1):
                full_copy(j, first, axis, side, full, s_full, r_full, at).wait_recv()
                for q in (0, 1):
                    into[q].append((full.at[(*at, side)], q * quarter))
        return into

    def leave(j, first, axis, offset, bufs, at):
        relay, full, s_relay, r_relay, s_full, r_full = bufs
        if offset == 2:
            for side in (0, 1):
                relay_copy(j, first, axis, side, relay, s_relay, r_relay, at).start()
        elif offset in (1, 3):
            side = 0 if offset == 1 else 1
            full_copy(j, first, axis, side, full, s_full, r_full, at).start()

    stage1 = (relay1, full1, s_relay1, r_relay1, s_full1, r_full1)
    stage2 = (relay2, full2, s_relay2, r_relay2, s_full2, r_full2)
    for j, offsets in enumerate(ORDER):

        @pl.when(step == j)
        def _(j=j, offsets=offsets):
            for h in sorted((0, 1), key=lambda h: offsets[h] == 0):
                first = h * half
                near, far = offsets[h], offsets[1 - h]
                into = arrive(j, first, h, near, stage1, (h, far))
                out = (j, first, h, near, stage1, (h, far))
                if near == 0:
                    out = (j, first, 1 - h, far, stage2, (h,))
                    into = [a + b for a, b in zip(into, arrive(*out))]
                for q in (0, 1):
                    if into[q]:
                        combine(j, first + q * quarter, quarter, into[q])
                leave(*out)

    @pl.when(step == len(ORDER) - 1)
    def _():
        for which in (2, 5, 6, 7):
            query_copy(which).wait_recv()
        pltpu.make_async_copy(queries_ref, around_ref.at[0], s_own).wait()
        score_all(
            total_negatives, total_ref, around_ref, bias_ref, count_ref, live_ref,
            embed_out, lse_ref, *score_refs,
        )
        for j, offsets in enumerate(ORDER):
            for h in (0, 1):
                first = h * half
                near, far = offsets[h], offsets[1 - h]
                stages = [(near, h, stage1, (h, far))]
                if near == 0:
                    stages.append((far, 1 - h, stage2, (h,)))
                for offset, axis, bufs, at in stages:
                    relay, full, s_relay, r_relay, s_full, r_full = bufs
                    if offset == 2:
                        for side in (0, 1):
                            relay_copy(j, first, axis, side, relay, s_relay, r_relay, at).wait_send()
                    elif offset in (1, 3):
                        side = 0 if offset == 1 else 1
                        full_copy(j, first, axis, side, full, s_full, r_full, at).wait_send()
        for which in range(8):
            query_copy(which).wait_send()


def reduce_and_score(
    picked, counts, own, wm, mb, ws, wn, queries, bias, count, live, total_negatives
):
    peers, cap, negatives = counts.shape
    width = picked.shape[2]
    half, quarter = negatives // 2, negatives // 4
    vmem = pl.BlockSpec(memory_space=pltpu.VMEM)
    hbm = pl.BlockSpec(memory_space=pl.ANY)
    dma = pltpu.SemaphoreType.DMA
    bf16, f32 = jnp.bfloat16, jnp.float32
    return pl.pallas_call(
        functools.partial(reduce_kernel, total_negatives),
        grid=(peers,),
        out_shape=(
            jax.ShapeDtypeStruct((negatives, width), bf16),
            jax.ShapeDtypeStruct((1, queries.shape[0]), f32),
        ),
        in_specs=[
            pl.BlockSpec((1, cap, width), lambda j: (j, 0, 0)),
            pl.BlockSpec((1, cap, negatives), lambda j: (j, 0, 0)),
            pl.BlockSpec((1, 2, negatives), lambda j: (j, 0, 0)),
            vmem, vmem, vmem, vmem,
            hbm, vmem, vmem, vmem,
        ],
        out_specs=(hbm, vmem),
        scratch_shapes=[
            pltpu.VMEM((8,) + queries.shape, bf16),
            pltpu.VMEM((cap, negatives), bf16),
            pltpu.VMEM((cap, width), bf16),
            pltpu.VMEM((2 * cap, width), bf16),
            pltpu.VMEM((negatives, 2 * cap), bf16),
            pltpu.VMEM((negatives, width), f32),
            pltpu.VMEM((peers, negatives, width), bf16),
            pltpu.VMEM((2, SIDE, 2, quarter, width), bf16),
            pltpu.VMEM((2, SIDE, 2, half, width), bf16),
            pltpu.VMEM((2, 2, quarter, width), bf16),
            pltpu.VMEM((2, 2, half, width), bf16),
            dma((2, SIDE, 2)), dma((2, SIDE, 2)), dma((2, SIDE, 2)), dma((2, SIDE, 2)),
            dma((2, 2)), dma((2, 2)), dma((2, 2)), dma((2, 2)),
            dma((8,)), dma((8,)), dma,
            pltpu.VMEM((negatives, width), bf16),
            dma,
            pltpu.VMEM((negatives, LANES), f32),
            pltpu.VMEM((8, 1, queries.shape[0]), f32),
            pltpu.VMEM((8, 1, queries.shape[0]), f32),
            pltpu.VMEM((1, queries.shape[0]), f32),
            pltpu.VMEM((peers, 1, queries.shape[0]), f32),
            dma((8,)), dma((8,)), dma((15,)), dma((15,)),
        ],
        compiler_params=pltpu.CompilerParams(
            collective_id=1, has_side_effects=True, vmem_limit_bytes=62 << 20
        ),
    )(picked, counts, own, wm, mb, ws, wn, queries, bias, count, live)


def hand_out_kernel(embed_ref, lse_ref, embed_out, lse_out):
    embed_out[...] = embed_ref[...]
    lse_out[...] = lse_ref[...]


def hand_out(embed, lse):
    vmem = pl.BlockSpec(memory_space=pltpu.VMEM)
    return pl.pallas_call(
        hand_out_kernel,
        out_shape=[jax.ShapeDtypeStruct(a.shape, a.dtype) for a in (embed, lse)],
        in_specs=[vmem, vmem],
        out_specs=[vmem, vmem],
    )(embed, lse)


def per_device(
    items_table,
    fetch_rows,
    neighbour_slots,
    neighbour_count,
    self_slot,
    negative_count,
    message_weight,
    message_bias,
    self_weight,
    neighbour_weight,
    output_bias,
    queries,
):
    n_neg, n_qry = lax.axis_size("neg"), lax.axis_size("qry")
    own_neg = lax.axis_index("neg")
    cap = fetch_rows.shape[1]
    negatives, neighbours = neighbour_slots.shape

    assert n_neg * cap < DEAD and neighbours % 4 == 0 and n_neg == SIDE * SIDE and n_qry == 8
    all_lists, all_fetch = exchange_lists(
        neighbour_slots.T, neighbour_count[None, :], self_slot.reshape(-1, LANES), fetch_rows,
        items_table.shape[1] // LANES,
    )
    base = (own_neg * cap).astype(jnp.int32).reshape(1)
    counts, own, picked = pick_and_count(
        base, all_fetch, all_lists, items_table, neighbours, cap
    )
    negative_embed, query_lse = reduce_and_score(
        picked, counts, own,
        message_weight, message_bias[None, :], self_weight, neighbour_weight, queries,
        output_bias[None, :], negative_count[None, :], neighbour_count[None, :],
        negatives * n_neg * n_qry,
    )
    negative_embed, query_lse = hand_out(negative_embed, query_lse)
    return (negative_embed, query_lse.reshape(-1))


def solution(mesh):
    in_specs = (
        P("neg", None),
        P(("neg", "qry"), None),
        P(("neg", "qry"), None),
        P(("neg", "qry")),
        P(("neg", "qry")),
        P("neg"),
        P(),
        P(),
        P(),
        P(),
        P(),
        P("qry", None),
    )
    out_specs = (P(("neg", "qry"), None), P("qry"))
    return jax.shard_map(
        per_device, mesh=mesh, in_specs=in_specs, out_specs=out_specs, check_vma=False
    )
```
